16 devices in a mesh: emb: 2 (over z), col: 2 (over y), row: 4 (over x, core).
Axes of the slice: x: 2, y: 2, z: 2, core: 2. Of those that a mesh axis runs over, the one named last changes fastest.
Arguments:
- inter_mask: int32 [4096, 32768], P('row', 'col')
- emb_user: bfloat16 [4096, 256], P(('row', 'col'), 'emb')
- emb_item: bfloat16 [32768, 256], P(('col', 'row'), 'emb')
- triples: int32 [4096, 3], replicated
Outputs:
- output 1: bfloat16 [4096, 256], P(('row', 'col'), 'emb')
- output 2: bfloat16 [32768, 256], P(('col', 'row'), 'emb')
- output 3: float32 [4096], replicated
All inputs are finite; a program needn't handle non-finite values.
Results may differ from the reference program's by a relative error of at most 0.0133009.
Values are sent between devices in bfloat16 or wider.
A program may use at most 1 GiB of HBM per device.

```python
import jax
import jax.numpy as jnp
from jax import lax

NUM_USERS = 4096
NUM_ITEMS = 32768
EMB_DIM = 256
NUM_TRIPLES = 4096
NUM_LAYERS = 3
SPARSITY = 8
NUM_GROUPS = 8


def setup_inputs(seed: int = 0) -> dict:
    key = jax.random.key(seed)
    key_list = jax.random.split(key, 10)
    inter_mask = (jax.random.randint(key_list[0], (NUM_USERS, NUM_ITEMS), 0, SPARSITY) == 0).astype(jnp.int32)
    mean_user = jax.random.normal(key_list[1], (EMB_DIM,), jnp.float32)
    mean_item = jax.random.normal(key_list[2], (EMB_DIM,), jnp.float32)
    noise_user = jax.random.normal(key_list[3], (NUM_USERS, EMB_DIM), jnp.float32)
    noise_item = jax.random.normal(key_list[4], (NUM_ITEMS, EMB_DIM), jnp.float32)
    group_user = jax.random.normal(key_list[8], (NUM_GROUPS, EMB_DIM), jnp.float32)
    group_item = jax.random.normal(key_list[9], (NUM_GROUPS, EMB_DIM), jnp.float32)
    user_group = (jnp.arange(NUM_USERS) * NUM_GROUPS) // NUM_USERS
    item_group = (jnp.arange(NUM_ITEMS) * NUM_GROUPS) // NUM_ITEMS
    emb_user = (0.5 * (mean_user[None, :] + 1.5 * group_user[user_group] + noise_user)).astype(jnp.bfloat16)
    emb_item = (0.5 * (mean_item[None, :] + 1.5 * group_item[item_group] + noise_item)).astype(jnp.bfloat16)
    users = jax.random.randint(key_list[5], (NUM_TRIPLES,), 0, NUM_USERS).at[0].set(NUM_USERS - 1)
    pos_items = jax.random.randint(key_list[6], (NUM_TRIPLES,), 0, NUM_ITEMS).at[0].set(NUM_ITEMS - 1)
    neg_items = jax.random.randint(key_list[7], (NUM_TRIPLES,), 0, NUM_ITEMS).at[1].set(0)
    triples = jnp.stack([users, pos_items, neg_items], axis=1).astype(jnp.int32)
    return {"inter_mask": inter_mask, "emb_user": emb_user, "emb_item": emb_item, "triples": triples}


def reference(inter_mask, emb_user, emb_item, triples):
    deg_user = jnp.maximum(jnp.sum(inter_mask, axis=1), 1).astype(jnp.float32)
    deg_item = jnp.maximum(jnp.sum(inter_mask, axis=0), 1).astype(jnp.float32)
    adj_norm = ((lax.rsqrt(deg_user)[:, None] * inter_mask.astype(jnp.float32)) * lax.rsqrt(deg_item)[None, :]).astype(jnp.bfloat16)

    def layer_step(carry, unused):
        user_cur, item_cur, user_acc, item_acc = carry
        user_next = jnp.dot(adj_norm, item_cur, preferred_element_type=jnp.float32).astype(jnp.bfloat16)
        item_next = jnp.dot(adj_norm.T, user_cur, preferred_element_type=jnp.float32).astype(jnp.bfloat16)
        new_carry = (user_next, item_next, user_acc + user_next.astype(jnp.float32), item_acc + item_next.astype(jnp.float32))
        return new_carry, None

    init_state = (emb_user, emb_item, emb_user.astype(jnp.float32), emb_item.astype(jnp.float32))
    carry_out, scan_ys = lax.scan(layer_step, init_state, None, length=NUM_LAYERS)
    final_user = (carry_out[2] / (NUM_LAYERS + 1)).astype(jnp.bfloat16)
    final_item = (carry_out[3] / (NUM_LAYERS + 1)).astype(jnp.bfloat16)
    e_user = jnp.take(final_user, triples[:, 0], axis=0).astype(jnp.float32)
    e_pos = jnp.take(final_item, triples[:, 1], axis=0).astype(jnp.float32)
    e_neg = jnp.take(final_item, triples[:, 2], axis=0).astype(jnp.float32)
    score = jnp.sum(e_user * (e_pos - e_neg), axis=1)
    bpr_loss = jax.nn.softplus(-score)
    return final_user, final_item, bpr_loss
```

```python
import functools

import jax
import jax.numpy as jnp
from jax import lax
from jax.experimental import pallas as pl
from jax.experimental.pallas import tpu as pltpu
from jax.sharding import PartitionSpec as P

NUM_LAYERS = 3
F32 = jnp.float32
BF16 = jnp.bfloat16
MESH = pl.DeviceIdType.MESH

CHUNK = 512
MASK_COLS = 512
MASK_SLOTS = 3
SCALE_ROWS = 256
FOLD = 1024


def prop_kernel(mask_hbm, eu_ref, ei_ref, outu_ref, outi_ref,
                adj, mbuf, panel, xsend, xrecv, near, stage, drecv, upanel, upart, yrecv,
                rsum, rscale, csum, ccore, cchip, cfar, rdeg, rdfar,
                msem, ag0_s, ag0_r, deg_s, deg_r, u_s, u_r, y_s, y_r,
                d_s, d_r, x_s, x_r, agx_s, agx_r, agd_s, agd_r, agf_s, agf_r):
    users, items = adj.shape
    own_u = eu_ref.shape[0]
    own_i = ei_ref.shape[0]
    n_chunk = own_i // CHUNK
    row = lax.axis_index("row")
    col = lax.axis_index("col")
    mate = row + 1 - 2 * (row % 2)
    far = (row + 2) % 4
    far_mate = (mate + 2) % 4
    other_col = 1 - col
    to_mate = {"row": mate}
    to_far = {"row": far}
    to_col = {"col": other_col}

    def remote(src, dst, ssem, rsem, target):
        return pltpu.make_async_remote_copy(src_ref=src, dst_ref=dst, send_sem=ssem, recv_sem=rsem,
                                            device_id=target, device_id_type=MESH)

    def rows_of(owner, j, size=CHUNK):
        return pl.ds(pl.multiple_of(owner * own_i + j * size, size), size)

    barrier = pltpu.get_barrier_semaphore()
    for target in (to_mate, to_far, to_col):
        pl.semaphore_signal(barrier, inc=1, device_id=target, device_id_type=MESH)
    pl.semaphore_wait(barrier, 3)

    block = pl.ds(pl.multiple_of(row * own_i, own_i), own_i)
    far_block = pl.ds(pl.multiple_of(far * own_i, own_i), own_i)
    ublock = pl.ds(pl.multiple_of(col * own_u, own_u), own_u)
    oblock = pl.ds(pl.multiple_of(other_col * own_u, own_u), own_u)
    ag0_x = remote(ei_ref, panel.at[0, block], ag0_s.at[0], ag0_r.at[0], to_far)
    ag0_d = remote(ei_ref, panel.at[0, block], ag0_s.at[1], ag0_r.at[1], to_mate)
    ag0_f = remote(panel.at[0, far_block], panel.at[0, far_block], ag0_s.at[2], ag0_r.at[2], to_mate)
    ag0_x.start()
    ag0_d.start()
    u0 = remote(eu_ref, upanel.at[0, ublock], u_s.at[0], u_r.at[0], to_col)
    u0.start()

    n_mask = items // MASK_COLS

    def mask_copy(i):
        cols = pl.ds(pl.multiple_of(i * MASK_COLS, MASK_COLS), MASK_COLS)
        slot = i % MASK_SLOTS
        return pltpu.make_async_copy(mask_hbm.at[:, cols], mbuf.at[slot], msem.at[slot])

    for i in range(MASK_SLOTS - 1):
        mask_copy(i).start()
    panel[0, block, :] = ei_ref[...]
    upanel[0, ublock, :] = eu_ref[...]
    rsum[...] = jnp.zeros_like(rsum)

    def mask_step(i, carry):
        mask_copy(i).wait()

        @pl.when(i + MASK_SLOTS - 1 < n_mask)
        def _():
            mask_copy(i + MASK_SLOTS - 1).start()

        cols = pl.ds(pl.multiple_of(i * MASK_COLS, MASK_COLS), MASK_COLS)
        slot = i % MASK_SLOTS

        def tile(t, acc):
            rows = pl.ds(pl.multiple_of(t * 64, 64), 64)
            m = mbuf[slot, rows, :].astype(F32)
            adj[rows, cols] = m.astype(BF16)
            part = m[:, 0:128]
            for g in range(1, MASK_COLS // 128):
                part = part + m[:, g * 128:(g + 1) * 128]
            rsum[rows, :] += part
            return acc + jnp.sum(m.reshape(8, 8, MASK_COLS), axis=0)

        acc = lax.fori_loop(0, users // 64, tile, jnp.zeros((8, MASK_COLS), F32))
        csum[:, cols] = jnp.sum(acc, axis=0, keepdims=True)
        return carry

    lax.fori_loop(0, n_mask, mask_step, 0)

    deg_d = remote(csum, ccore, deg_s.at[0], deg_r.at[0], to_mate)
    deg_d.start()
    ones = jnp.ones((8, 128), BF16)
    rdeg[...] = lax.dot_general(ones, rsum[...].astype(BF16), (((1,), (1,)), ((), ())),
                                preferred_element_type=F32)
    deg_y = remote(rdeg, rdfar, deg_s.at[1], deg_r.at[1], to_col)
    deg_y.start()
    deg_d.wait()
    cchip[...] = csum[...] + ccore[...]
    deg_x = remote(cchip, cfar, deg_s.at[2], deg_r.at[2], to_far)
    deg_x.start()
    ag0_x.wait_recv()
    ag0_f.start()
    u0.wait_recv()
    deg_y.wait()
    deg_u = jnp.maximum(rdeg[0:1, :] + rdfar[0:1, :], 1.0)
    rscale[...] = lax.rsqrt(jnp.broadcast_to(deg_u, (128, users)).T)
    deg_x.wait()
    csum[...] = lax.rsqrt(jnp.maximum(cchip[...] + cfar[...], 1.0))

    def scale_block(owner, j):
        cols = rows_of(owner, j)
        ci = csum[:, cols]

        def tile(t, carry):
            rows = pl.ds(pl.multiple_of(t * SCALE_ROWS, SCALE_ROWS), SCALE_ROWS)
            ru = rscale[rows, :]
            for g in range(CHUNK // 128):
                sub = pl.ds(pl.multiple_of(owner * own_i + j * CHUNK + g * 128, 128), 128)
                m = adj[rows, sub].astype(F32)
                adj[rows, sub] = ((ru * m) * ci[:, g * 128:(g + 1) * 128]).astype(BF16)
            return carry

        lax.fori_loop(0, users // SCALE_ROWS, tile, 0)

    def item_part(owner, j, layer):
        return lax.dot_general(adj[:, rows_of(owner, j)], upanel[layer - 1], (((0,), (0,)), ((), ())),
                               preferred_element_type=F32)

    def core_copy(slot):
        return remote(stage.at[slot], drecv.at[slot], d_s.at[slot], d_r.at[slot], to_mate)

    def chunk_rows(j):
        return pl.ds(pl.multiple_of(j * CHUNK, CHUNK), CHUNK)

    def x_copy(j, layer):
        par = layer % 2
        return remote(xsend.at[chunk_rows(j)], xrecv.at[par, chunk_rows(j)], x_s.at[j], x_r.at[par, j], to_far)

    def item_send_step(j, layer):
        slot = j % 2
        if layer == 1:
            @pl.when(j >= 2)
            def _():
                core_copy(slot).wait_send()
            scale_block(far_mate, j)
            scale_block(mate, j)
        else:
            core_copy(slot).wait_send()
        stage[slot, 0:CHUNK, :] = item_part(far_mate, j, layer)
        stage[slot, CHUNK:2 * CHUNK, :] = item_part(mate, j, layer)
        core_copy(slot).start()
        if layer == 1:
            scale_block(far, j)
            scale_block(row, j)
        else:
            x_copy(j, layer - 1).wait_send()
        xsend[chunk_rows(j), :] = item_part(far, j, layer)
        near[chunk_rows(j), :] = item_part(row, j, layer)
        core_copy(slot).wait_recv()
        xsend[chunk_rows(j), :] += drecv[slot, 0:CHUNK, :]
        near[chunk_rows(j), :] += drecv[slot, CHUNK:2 * CHUNK, :]
        x_copy(j, layer).start()

    def ag_copy(kind, j, layer):
        par = layer % 2
        block = panel.at[par, rows_of(far if kind == "fwd" else row, j)]
        ssem, rsem, target = {"x": (agx_s, agx_r, to_far), "mate": (agd_s, agd_r, to_mate),
                              "fwd": (agf_s, agf_r, to_mate)}[kind]
        return remote(block, block, ssem.at[j], rsem.at[par, j], target)

    def finish_item(j, layer):
        x_copy(j, layer).wait_recv()
        par = layer % 2
        value = (near[chunk_rows(j), :] + xrecv[par, chunk_rows(j), :]).astype(BF16)
        if layer < NUM_LAYERS:
            panel[par, rows_of(row, j), :] = value
            ag_copy("x", j, layer).start()
            ag_copy("mate", j, layer).start()
        else:
            total = ei_ref[chunk_rows(j), :].astype(F32) + panel[1, rows_of(row, j), :].astype(F32)
            total = total + panel[0, rows_of(row, j), :].astype(F32)
            total = total + value.astype(F32)
            outi_ref[chunk_rows(j), :] = (total / (NUM_LAYERS + 1)).astype(BF16)

    def gather_items(layer):
        def forward(j, carry):
            ag_copy("x", j, layer).wait_recv()
            ag_copy("fwd", j, layer).start()
            return carry

        def settle(j, carry):
            ag_copy("mate", j, layer).wait_recv()
            ag_copy("fwd", j, layer).wait_recv()
            for kind in ("x", "mate", "fwd"):
                ag_copy(kind, j, layer).wait_send()
            return carry

        lax.fori_loop(0, n_chunk, forward, 0)
        lax.fori_loop(0, n_chunk, settle, 0)

    def user_part(layer):
        par = (layer - 1) % 2
        upart[...] = jnp.zeros_like(upart)

        def fold(i, carry):
            cols = pl.ds(pl.multiple_of(i * FOLD, FOLD), FOLD)
            upart[...] += jnp.dot(adj[:, cols], panel[par, cols, :], preferred_element_type=F32)
            return carry

        lax.fori_loop(0, items // FOLD, fold, 0)

    def y_copy(layer):
        return remote(upart.at[oblock], yrecv.at[layer - 1], y_s.at[layer - 1], y_r.at[layer - 1], to_col)

    def u_copy(layer):
        return remote(upanel.at[layer, ublock], upanel.at[layer, ublock], u_s.at[layer], u_r.at[layer], to_col)

    def finish_user(layer):
        y_copy(layer).wait()
        value = (upart[ublock, :] + yrecv[layer - 1]).astype(BF16)
        if layer < NUM_LAYERS:
            upanel[layer, ublock, :] = value
            u_copy(layer).start()
        else:
            total = eu_ref[...].astype(F32) + upanel[1, ublock, :].astype(F32)
            total = total + upanel[2, ublock, :].astype(F32)
            total = total + value.astype(F32)
            outu_ref[...] = (total / (NUM_LAYERS + 1)).astype(BF16)

    def loop(lo, hi, body):
        def step(j, carry):
            body(j)
            return carry
        lax.fori_loop(lo, hi, step, 0)

    for layer in range(1, NUM_LAYERS + 1):
        loop(0, n_chunk, functools.partial(item_send_step, layer=layer))
        if layer == 1:
            ag0_d.wait_recv()
            ag0_f.wait_recv()
            ag0_x.wait_send()
            ag0_d.wait_send()
            ag0_f.wait_send()
            u0.wait_send()
        else:
            gather_items(layer - 1)
        user_part(layer)
        y_copy(layer).start()
        loop(0, n_chunk // 2, functools.partial(finish_item, layer=layer))
        finish_user(layer)
        loop(n_chunk // 2, n_chunk, functools.partial(finish_item, layer=layer))
        if layer < NUM_LAYERS:
            u_copy(layer).wait()

    for slot in range(2):
        core_copy(slot).wait_send()
    for j in range(n_chunk):
        x_copy(j, NUM_LAYERS).wait_send()


def propagate(mask_blk, user_sh, item_sh):
    users, items = mask_blk.shape
    own_u, dim = user_sh.shape
    own_i = item_sh.shape[0]
    n_chunk = own_i // CHUNK
    vmem, dma = pltpu.VMEM, pltpu.SemaphoreType.DMA
    return pl.pallas_call(
        prop_kernel,
        name="propagate",
        out_shape=(jax.ShapeDtypeStruct((own_u, dim), BF16), jax.ShapeDtypeStruct((own_i, dim), BF16)),
        in_specs=[pl.BlockSpec(memory_space=pl.ANY), pl.BlockSpec(memory_space=pltpu.VMEM),
                  pl.BlockSpec(memory_space=pltpu.VMEM)],
        out_specs=(pl.BlockSpec(memory_space=pltpu.VMEM), pl.BlockSpec(memory_space=pltpu.VMEM)),
        scratch_shapes=[
            vmem((users, items), BF16),
            vmem((MASK_SLOTS, users, MASK_COLS), jnp.int32),
            vmem((2, items, dim), BF16),
            vmem((own_i, dim), F32),
            vmem((2, own_i, dim), F32),
            vmem((own_i, dim), F32),
            vmem((2, 2 * CHUNK, dim), F32),
            vmem((2, 2 * CHUNK, dim), F32),
            vmem((3, users, dim), BF16),
            vmem((users, dim), F32),
            vmem((3, own_u, dim), F32),
            vmem((users, 128), F32),
            vmem((users, 128), F32),
            vmem((1, items), F32),
            vmem((1, items), F32),
            vmem((1, items), F32),
            vmem((1, items), F32),
            vmem((8, users), F32),
            vmem((8, users), F32),
            dma((MASK_SLOTS,)),
            dma((3,)), dma((3,)),
            dma((3,)), dma((3,)),
            dma((3,)), dma((3,)),
            dma((3,)), dma((3,)),
            dma((2,)), dma((2,)),
            dma((n_chunk,)), dma((2, n_chunk)),
            dma((n_chunk,)), dma((2, n_chunk)),
            dma((n_chunk,)), dma((2, n_chunk)),
            dma((n_chunk,)), dma((2, n_chunk)),
        ],
        compiler_params=pltpu.CompilerParams(collective_id=0, has_side_effects=True,
                                             vmem_limit_bytes=67_043_328),
    )(mask_blk, user_sh, item_sh)


def lookup_rows(table, ids, offset):
    own_rows = table.shape[0]
    local_ids = ids - offset
    owned = (local_ids >= 0) & (local_ids < own_rows)
    picked = jnp.take(table, jnp.clip(local_ids, 0, own_rows - 1), axis=0)
    return jnp.where(owned[:, None], picked, jnp.zeros((), table.dtype))


def bpr_terms(final_user, final_item, triples, user_off, item_off):
    fetched = jnp.stack([
        lookup_rows(final_user, triples[:, 0], user_off),
        lookup_rows(final_item, triples[:, 1], item_off),
        lookup_rows(final_item, triples[:, 2], item_off)], axis=0)
    mine = lax.psum_scatter(fetched, ("row", "col"), scatter_dimension=1, tiled=True).astype(F32)
    score = lax.psum(jnp.sum(mine[0] * (mine[1] - mine[2]), axis=1), "emb")
    return lax.all_gather(jax.nn.softplus(-score), ("row", "col"), axis=0, tiled=True)


def solution(mesh):
    n_col = mesh.shape["col"]
    n_row = mesh.shape["row"]

    def local_fn(mask_blk, user_sh, item_sh, triples):
        final_user, final_item = propagate(mask_blk, user_sh, item_sh)
        user_off = (lax.axis_index("row") * n_col + lax.axis_index("col")) * final_user.shape[0]
        item_off = (lax.axis_index("col") * n_row + lax.axis_index("row")) * final_item.shape[0]
        return final_user, final_item, bpr_terms(final_user, final_item, triples, user_off, item_off)

    return jax.shard_map(
        local_fn, mesh=mesh,
        in_specs=(P("row", "col"), P(("row", "col"), "emb"), P(("col", "row"), "emb"), P()),
        out_specs=(P(("row", "col"), "emb"), P(("col", "row"), "emb"), P()),
        check_vma=False)
```

```python
import functools

import jax
import jax.numpy as jnp
from jax import lax
from jax.experimental import pallas as pl
from jax.experimental.pallas import tpu as pltpu
from jax.sharding import PartitionSpec as P

NUM_LAYERS = 3
F32 = jnp.float32
BF16 = jnp.bfloat16
MESH = pl.DeviceIdType.MESH

CHUNK = 512
MASK_COLS = 256
MASK_SLOTS = 4
SCALE_ROWS = 256
FOLD = 1024


def prop_kernel(mask_hbm, eu_ref, ei_ref, trip_ref, outu_ref, outi_ref, loss_ref,
                adj, mbuf, panel, table, stage, drecv, upanel, upart, yflat,
                rsum, rscale, csum, ccore, cchip, cfar, rdeg, rdfar, pick_idx, pick_out, pick_in, dots,
                msem, ag0_s, ag0_r, deg_s, deg_r, u_s, u_r, y_s, y_r,
                d_s, d_r, x_s, x_r, agx_s, agx_r, agd_s, agd_r, agf_s, agf_r,
                fin_s, fin_r, fu_s, fu_r, pick_s, pick_r, dot_s, dot_r, loss_s, loss_r):
    users, items = adj.shape
    own_u = eu_ref.shape[0]
    own_i = ei_ref.shape[0]
    n_chunk = own_i // CHUNK
    row = lax.axis_index("row")
    col = lax.axis_index("col")
    mate = row + 1 - 2 * (row % 2)
    far = (row + 2) % 4
    far_mate = (mate + 2) % 4
    other_col = 1 - col
    to_mate = {"row": mate}
    to_far = {"row": far}
    to_col = {"col": other_col}
    emb = lax.axis_index("emb")
    to_emb = {"emb": 1 - emb}
    peers = [{"row": (row + dr) % 4, "col": (col + dc) % 2} for dr in range(4) for dc in range(2)][1:]
    share = loss_ref.shape[1] // 8

    def remote(src, dst, ssem, rsem, target):
        return pltpu.make_async_remote_copy(src_ref=src, dst_ref=dst, send_sem=ssem, recv_sem=rsem,
                                            device_id=target, device_id_type=MESH)

    def rows_of(owner, j, size=CHUNK):
        return pl.ds(pl.multiple_of(owner * own_i + j * size, size), size)

    barrier = pltpu.get_barrier_semaphore()
    for target in [*peers, to_emb]:
        pl.semaphore_signal(barrier, inc=1, device_id=target, device_id_type=MESH)
    pl.semaphore_wait(barrier, 8)

    block = pl.ds(pl.multiple_of(row * own_i, own_i), own_i)
    far_block = pl.ds(pl.multiple_of(far * own_i, own_i), own_i)
    ublock = pl.ds(pl.multiple_of(col * own_u, own_u), own_u)
    oblock = pl.ds(pl.multiple_of(other_col * own_u, own_u), own_u)
    ag0_x = remote(ei_ref, panel.at[0, block], ag0_s.at[0], ag0_r.at[0], to_far)
    ag0_d = remote(ei_ref, panel.at[0, block], ag0_s.at[1], ag0_r.at[1], to_mate)
    ag0_f = remote(panel.at[0, far_block], panel.at[0, far_block], ag0_s.at[2], ag0_r.at[2], to_mate)
    ag0_x.start()
    ag0_d.start()
    u0 = remote(eu_ref, upanel.at[0, ublock], u_s.at[0], u_r.at[0], to_col)
    u0.start()

    n_mask = items // MASK_COLS

    def mask_copy(i):
        cols = pl.ds(pl.multiple_of(i * MASK_COLS, MASK_COLS), MASK_COLS)
        slot = i % MASK_SLOTS
        return pltpu.make_async_copy(mask_hbm.at[:, cols], mbuf.at[slot], msem.at[slot])

    for i in range(MASK_SLOTS - 1):
        mask_copy(i).start()
    panel[0, block, :] = ei_ref[...]
    upanel[0, ublock, :] = eu_ref[...]
    rsum[...] = jnp.zeros_like(rsum)

    def mask_step(i, carry):
        mask_copy(i).wait()

        @pl.when(i + MASK_SLOTS - 1 < n_mask)
        def _():
            mask_copy(i + MASK_SLOTS - 1).start()

        cols = pl.ds(pl.multiple_of(i * MASK_COLS, MASK_COLS), MASK_COLS)
        slot = i % MASK_SLOTS

        def tile(t, acc):
            rows = pl.ds(pl.multiple_of(t * 64, 64), 64)
            m = mbuf[slot, rows, :].astype(F32)
            adj[rows, cols] = m.astype(BF16)
            part = m[:, 0:128]
            for g in range(1, MASK_COLS // 128):
                part = part + m[:, g * 128:(g + 1) * 128]
            rsum[rows, :] += part
            return acc + jnp.sum(m.reshape(8, 8, MASK_COLS), axis=0)

        acc = lax.fori_loop(0, users // 64, tile, jnp.zeros((8, MASK_COLS), F32))
        csum[:, cols] = jnp.sum(acc, axis=0, keepdims=True)
        return carry

    lax.fori_loop(0, n_mask, mask_step, 0)

    deg_d = remote(csum, ccore, deg_s.at[0], deg_r.at[0], to_mate)
    deg_d.start()
    ones = jnp.ones((8, 128), BF16)
    rdeg[...] = lax.dot_general(ones, rsum[...].astype(BF16), (((1,), (1,)), ((), ())),
                                preferred_element_type=F32)
    deg_y = remote(rdeg, rdfar, deg_s.at[1], deg_r.at[1], to_col)
    deg_y.start()
    deg_d.wait()
    cchip[...] = csum[...] + ccore[...]
    deg_x = remote(cchip, cfar, deg_s.at[2], deg_r.at[2], to_far)
    deg_x.start()
    ag0_x.wait_recv()
    ag0_f.start()
    u0.wait_recv()
    deg_y.wait()
    deg_u = jnp.maximum(rdeg[0:1, :] + rdfar[0:1, :], 1.0)
    rscale[...] = lax.rsqrt(jnp.broadcast_to(deg_u, (128, users)).T)
    deg_x.wait()
    csum[...] = lax.rsqrt(jnp.maximum(cchip[...] + cfar[...], 1.0))

    def scale_block(owner, j):
        cols = rows_of(owner, j)
        ci = csum[:, cols]

        def tile(t, carry):
            rows = pl.ds(pl.multiple_of(t * SCALE_ROWS, SCALE_ROWS), SCALE_ROWS)
            ru = rscale[rows, :]
            for g in range(CHUNK // 128):
                sub = pl.ds(pl.multiple_of(owner * own_i + j * CHUNK + g * 128, 128), 128)
                m = adj[rows, sub].astype(F32)
                adj[rows, sub] = ((ru * m) * ci[:, g * 128:(g + 1) * 128]).astype(BF16)
            return carry

        lax.fori_loop(0, users // SCALE_ROWS, tile, 0)

    def item_part(owner, j, layer):
        return lax.dot_general(adj[:, rows_of(owner, j)], upanel[layer - 1], (((0,), (0,)), ((), ())),
                               preferred_element_type=F32)

    def core_copy(slot):
        return remote(stage.at[slot_rows(slot)], drecv.at[slot_rows(slot)], d_s.at[slot], d_r.at[slot], to_mate)

    def region(k, j):
        return pl.ds(pl.multiple_of(k * own_i + j * CHUNK, CHUNK), CHUNK)

    def near(j):
        return region(0, j)

    def arrived(j, layer):
        return region(1 + layer % 2, j)

    def xsend(j):
        return region(3, j)

    def chunk_rows(j):
        return pl.ds(pl.multiple_of(j * CHUNK, CHUNK), CHUNK)

    def slot_rows(slot, half=None):
        if half is None:
            return pl.ds(pl.multiple_of(slot * 2 * CHUNK, 2 * CHUNK), 2 * CHUNK)
        return pl.ds(pl.multiple_of(slot * 2 * CHUNK + half * CHUNK, CHUNK), CHUNK)

    def x_copy(j, layer):
        return remote(table.at[xsend(j)], table.at[arrived(j, layer)], x_s.at[j], x_r.at[layer % 2, j], to_far)

    def item_send_step(j, layer):
        slot = j % 2
        if layer == 1:
            @pl.when(j >= 2)
            def _():
                core_copy(slot).wait_send()
            scale_block(far_mate, j)
            scale_block(mate, j)
        else:
            core_copy(slot).wait_send()
        stage[slot_rows(slot, 0), :] = item_part(far_mate, j, layer)
        stage[slot_rows(slot, 1), :] = item_part(mate, j, layer)
        core_copy(slot).start()
        if layer == 1:
            scale_block(far, j)
            scale_block(row, j)
        else:
            x_copy(j, layer - 1).wait_send()
        table[xsend(j), :] = item_part(far, j, layer)
        table[near(j), :] = item_part(row, j, layer)
        core_copy(slot).wait_recv()
        table[xsend(j), :] += drecv[slot_rows(slot, 0), :]
        table[near(j), :] += drecv[slot_rows(slot, 1), :]
        x_copy(j, layer).start()

    def ag_copy(kind, j, layer):
        par = layer % 2
        block = panel.at[par, rows_of(far if kind == "fwd" else row, j)]
        ssem, rsem, target = {"x": (agx_s, agx_r, to_far), "mate": (agd_s, agd_r, to_mate),
                              "fwd": (agf_s, agf_r, to_mate)}[kind]
        return remote(block, block, ssem.at[j], rsem.at[par, j], target)

    def fin_copy(kind, j):
        src, dst, k, target = {
            "col": (outi_ref.at[chunk_rows(j)], panel.at[1, rows_of(far, j)], 0, to_col),
            "mate": (outi_ref.at[chunk_rows(j)], panel.at[1, rows_of(row, j)], 1, to_mate),
            "fwd": (panel.at[1, rows_of(far, j)], panel.at[1, rows_of(far, j)], 2, to_mate)}[kind]
        return remote(src, dst, fin_s.at[k, j], fin_r.at[k, j], target)

    def fin_near(j):
        fin_copy("col", j).wait_recv()
        fin_copy("fwd", j).start()
        table[region(2, j), :] = panel[1, rows_of(far, j), :].astype(F32)
        fin_copy("mate", j).wait_recv()
        table[region(1, j), :] = panel[1, rows_of(mate, j), :].astype(F32)

    def fin_fwd(j):
        x_copy(j, NUM_LAYERS).wait_send()
        fin_copy("fwd", j).wait_recv()
        table[region(3, j), :] = panel[1, rows_of(far_mate, j), :].astype(F32)

    def finish_item(j, layer):
        x_copy(j, layer).wait_recv()
        par = layer % 2
        value = (table[near(j), :] + table[arrived(j, layer), :]).astype(BF16)
        if layer < NUM_LAYERS:
            panel[par, rows_of(row, j), :] = value
            ag_copy("x", j, layer).start()
            ag_copy("mate", j, layer).start()
        else:
            total = ei_ref[chunk_rows(j), :].astype(F32) + panel[1, rows_of(row, j), :].astype(F32)
            total = total + panel[0, rows_of(row, j), :].astype(F32)
            total = total + value.astype(F32)
            final = (total / (NUM_LAYERS + 1)).astype(BF16)
            outi_ref[chunk_rows(j), :] = final
            table[near(j), :] = final.astype(F32)
            fin_copy("col", j).start()
            fin_copy("mate", j).start()

    def gather_items(layer):
        def forward(j, carry):
            ag_copy("x", j, layer).wait_recv()
            ag_copy("fwd", j, layer).start()
            return carry

        def settle(j, carry):
            ag_copy("mate", j, layer).wait_recv()
            ag_copy("fwd", j, layer).wait_recv()
            for kind in ("x", "mate", "fwd"):
                ag_copy(kind, j, layer).wait_send()
            return carry

        lax.fori_loop(0, n_chunk, forward, 0)
        lax.fori_loop(0, n_chunk, settle, 0)

    def user_part(layer):
        par = (layer - 1) % 2
        upart[...] = jnp.zeros_like(upart)

        def fold(i, carry):
            cols = pl.ds(pl.multiple_of(i * FOLD, FOLD), FOLD)
            upart[...] += jnp.dot(adj[:, cols], panel[par, cols, :], preferred_element_type=F32)
            return carry

        lax.fori_loop(0, items // FOLD, fold, 0)

    def yrows(layer):
        return pl.ds((layer - 1) * own_u, own_u)

    def y_copy(layer):
        return remote(upart.at[oblock], yflat.at[yrows(layer)], y_s.at[layer - 1], y_r.at[layer - 1], to_col)

    def u_copy(layer):
        return remote(upanel.at[layer, ublock], upanel.at[layer, ublock], u_s.at[layer], u_r.at[layer], to_col)

    def finish_user(layer):
        y_copy(layer).wait()
        value = (upart[ublock, :] + yflat[yrows(layer), :]).astype(BF16)
        if layer < NUM_LAYERS:
            upanel[layer, ublock, :] = value
            u_copy(layer).start()
        else:
            total = eu_ref[...].astype(F32) + upanel[1, ublock, :].astype(F32)
            total = total + upanel[2, ublock, :].astype(F32)
            total = total + value.astype(F32)
            final = (total / (NUM_LAYERS + 1)).astype(BF16)
            outu_ref[...] = final
            stage[0:own_u, :] = final.astype(F32)
            fu_copy("col").start()
            fu_copy("mate").start()

    def fu_copy(kind):
        src, dst, k, target = {
            "col": (outu_ref, upanel.at[0, pl.ds(0, own_u)], 0, to_col),
            "mate": (outu_ref, upanel.at[0, pl.ds(own_u, own_u)], 1, to_mate),
            "fwd": (upanel.at[0, pl.ds(0, own_u)], upanel.at[1, oblock], 2, to_mate)}[kind]
        return remote(src, dst, fu_s.at[k], fu_r.at[k], target)

    def gather_users():
        fu_copy("col").wait_recv()
        fu_copy("fwd").start()
        stage[2 * own_u:3 * own_u, :] = upanel[0, 0:own_u, :].astype(F32)
        fu_copy("mate").wait_recv()
        stage[own_u:2 * own_u, :] = upanel[0, own_u:2 * own_u, :].astype(F32)
        fu_copy("fwd").wait_recv()
        stage[3 * own_u:4 * own_u, :] = upanel[1, oblock, :].astype(F32)

    def place_rows():
        def side(r):
            return r // 2

        def step(t, carry):
            for k, owner in ((0, far), (1, row)):
                base = (owner * 2 + col) * share + t
                user = trip_ref[0, base]
                ur = lax.shift_right_logical(user, 10)
                uc = lax.bitwise_and(lax.shift_right_logical(user, 9), 1)
                pos = (jnp.where(uc == col, 0, 2) + jnp.where(ur == row, 0, 1)) * own_u + lax.bitwise_and(user, 511)
                pick_idx[k * 3 * share + t] = jnp.where(lax.shift_right_logical(ur, 1) == side(row), pos, 4 * own_u)
                for which in (1, 2):
                    item = trip_ref[which, base]
                    ic = lax.shift_right_logical(item, 14)
                    ir = lax.bitwise_and(lax.shift_right_logical(item, 12), 3)
                    pos = (jnp.where(ic == col, 0, 2) + jnp.where(ir == row, 0, 1)) * own_i + lax.bitwise_and(item, 4095)
                    pick_idx[(k * 3 + which) * share + t] = jnp.where(
                        lax.shift_right_logical(ir, 1) == side(row), pos, 4 * own_i)
            return carry

        lax.fori_loop(0, share, step, 0)

    def pick(src, k, which, dst):
        def step(t, carry):
            for i in range(8):
                at = t * 8 + i
                dst[pl.ds(which * share + at, 1), :] = src[pl.ds(pick_idx[(k * 3 + which) * share + at], 1), :]
            return carry

        lax.fori_loop(0, share // 8, step, 0)

    def pick_copy(which):
        rows = pl.ds(which * share, share)
        return remote(pick_out.at[rows], pick_in.at[rows], pick_s.at[which], pick_r.at[which], to_far)

    def pick_far(src, which):
        pick(src, 0, which, yflat)
        rows = pl.ds(which * share, share)
        pick_out[rows, :] = yflat[rows, :].astype(BF16)
        pick_copy(which).start()

    def loop(lo, hi, body):
        def step(j, carry):
            body(j)
            return carry
        lax.fori_loop(lo, hi, step, 0)

    for layer in range(1, NUM_LAYERS + 1):
        loop(0, n_chunk, functools.partial(item_send_step, layer=layer))
        if layer == 1:
            ag0_d.wait_recv()
            ag0_f.wait_recv()
            ag0_x.wait_send()
            ag0_d.wait_send()
            ag0_f.wait_send()
            u0.wait_send()
        else:
            gather_items(layer - 1)
        user_part(layer)
        y_copy(layer).start()
        if layer < NUM_LAYERS:
            loop(0, n_chunk // 2, functools.partial(finish_item, layer=layer))
            finish_user(layer)
            loop(n_chunk // 2, n_chunk, functools.partial(finish_item, layer=layer))
            u_copy(layer).wait()

    for slot in range(2):
        core_copy(slot).wait_send()
    table[pl.ds(4 * own_i, 8), :] = jnp.zeros((8, 128), F32)
    stage[pl.ds(4 * own_u, 8), :] = jnp.zeros((8, 128), F32)
    place_rows()
    finish_user(NUM_LAYERS)

    def last_step(j):
        finish_item(j, NUM_LAYERS)

        @pl.when(j >= 1)
        def _():
            fin_near(j - 1)

        @pl.when(j >= 2)
        def _():
            fin_fwd(j - 2)

    loop(0, n_chunk // 2, last_step)
    gather_users()
    pick_far(stage, 0)
    pick(stage, 1, 0, drecv)
    loop(n_chunk // 2, n_chunk, last_step)
    fin_near(n_chunk - 1)
    fin_fwd(n_chunk - 2)
    fin_fwd(n_chunk - 1)
    pick_far(table, 1)
    pick_far(table, 2)
    pick(table, 1, 1, drecv)
    pick(table, 1, 2, drecv)

    def both(which):
        rows = pl.ds(which * share, share)
        pick_copy(which).wait_recv()
        return drecv[rows, :] + pick_in[rows, :].astype(F32)

    e_user, e_pos, e_neg = both(0), both(1), both(2)
    prod = e_user * (e_pos - e_neg)
    dots[0] = jnp.sum(prod.T, axis=0, keepdims=True)
    dot_copy = remote(dots.at[0], dots.at[1], dot_s.at[0], dot_r.at[0], to_emb)
    dot_copy.start()
    dot_copy.wait()
    z = -(dots[0] + dots[1])
    mine = pl.ds(pl.multiple_of((row * 2 + col) * share, share), share)
    loss_ref[:, mine] = jnp.maximum(z, 0.0) + jnp.log1p(jnp.exp(-jnp.abs(z)))
    copies = [remote(loss_ref.at[:, mine], loss_ref.at[:, mine], loss_s.at[k], loss_r.at[k], target)
              for k, target in enumerate(peers)]
    for copy in copies:
        copy.start()

    for which in range(3):
        pick_copy(which).wait_send()
    for kind in ("col", "mate", "fwd"):
        fu_copy(kind).wait_send()
        loop(0, n_chunk, lambda j: fin_copy(kind, j).wait_send())
    for copy in copies:
        copy.wait()


def propagate(mask_blk, user_sh, item_sh, triples):
    users, items = mask_blk.shape
    own_u, dim = user_sh.shape
    own_i = item_sh.shape[0]
    n_chunk = own_i // CHUNK
    num_trip = triples.shape[0]
    share = num_trip // 8
    vmem, dma = pltpu.VMEM, pltpu.SemaphoreType.DMA
    return pl.pallas_call(
        prop_kernel,
        name="propagate",
        out_shape=(jax.ShapeDtypeStruct((own_u, dim), BF16), jax.ShapeDtypeStruct((own_i, dim), BF16),
                   jax.ShapeDtypeStruct((1, num_trip), F32)),
        in_specs=[pl.BlockSpec(memory_space=pl.ANY), pl.BlockSpec(memory_space=pltpu.VMEM),
                  pl.BlockSpec(memory_space=pltpu.VMEM), pl.BlockSpec(memory_space=pltpu.SMEM)],
        out_specs=(pl.BlockSpec(memory_space=pltpu.VMEM),) * 3,
        scratch_shapes=[
            vmem((users, items), BF16),
            vmem((MASK_SLOTS, users, MASK_COLS), jnp.int32),
            vmem((2, items, dim), BF16),
            vmem((4 * own_i + 8, dim), F32),
            vmem((4 * CHUNK + 8, dim), F32),
            vmem((4 * CHUNK, dim), F32),
            vmem((3, users, dim), BF16),
            vmem((users, dim), F32),
            vmem((3 * own_u, dim), F32),
            vmem((users, 128), F32),
            vmem((users, 128), F32),
            vmem((1, items), F32),
            vmem((1, items), F32),
            vmem((1, items), F32),
            vmem((1, items), F32),
            vmem((8, users), F32),
            vmem((8, users), F32),
            pltpu.SMEM((6 * share,), jnp.int32),
            vmem((3 * share, dim), BF16),
            vmem((3 * share, dim), BF16),
            vmem((2, 1, share), F32),
            dma((MASK_SLOTS,)),
            dma((3,)), dma((3,)),
            dma((3,)), dma((3,)),
            dma((3,)), dma((3,)),
            dma((3,)), dma((3,)),
            dma((2,)), dma((2,)),
            dma((n_chunk,)), dma((2, n_chunk)),
            dma((n_chunk,)), dma((2, n_chunk)),
            dma((n_chunk,)), dma((2, n_chunk)),
            dma((n_chunk,)), dma((2, n_chunk)),
            dma((3, n_chunk)), dma((3, n_chunk)),
            dma((3,)), dma((3,)),
            dma((3,)), dma((3,)),
            dma((1,)), dma((1,)),
            dma((7,)), dma((7,)),
        ],
        compiler_params=pltpu.CompilerParams(collective_id=0, has_side_effects=True,
                                             vmem_limit_bytes=67_043_328),
    )(mask_blk, user_sh, item_sh, triples.T)


def solution(mesh):
    def local_fn(mask_blk, user_sh, item_sh, triples):
        final_user, final_item, loss = propagate(mask_blk, user_sh, item_sh, triples)
        return final_user, final_item, loss.reshape(-1)

    return jax.shard_map(
        local_fn, mesh=mesh,
        in_specs=(P("row", "col"), P(("row", "col"), "emb"), P(("col", "row"), "emb"), P()),
        out_specs=(P(("row", "col"), "emb"), P(("col", "row"), "emb"), P()),
        check_vma=False)
```

```python
import functools

import jax
import jax.numpy as jnp
from jax import lax
from jax.experimental import pallas as pl
from jax.experimental.pallas import tpu as pltpu
from jax.sharding import PartitionSpec as P

NUM_LAYERS = 3
F32 = jnp.float32
BF16 = jnp.bfloat16
MESH = pl.DeviceIdType.MESH

CHUNK = 256
MASK_COLS = 256
MASK_SLOTS = 7
PIECES = 16
CORE_SLOTS = 4
SCALE_ROWS = 256
LAG = 3
FOLD = 2048


def prop_kernel(mask_hbm, eu_ref, ei_ref, trip_ref, outu_ref, outi_ref, loss_ref,
                adj, mbuf, panel, table, stage, drecv, upanel, upart, yflat,
                csum, ccore, cchip, cfar, rdeg, rdfar, pick_idx, pick_in, dots,
                msem, ag0_s, ag0_r, deg_s, deg_r, u_s, u_r, y_s, y_r,
                d_s, d_r, x_s, x_r, agx_s, agx_r, agd_s, agd_r, agf_s, agf_r,
                fin_s, fin_r, fu_s, fu_r, pick_s, pick_r, dot_s, dot_r, out_s, loss_s, loss_r):
    users, items = adj.shape
    rsum = rscale = upart
    own_u = eu_ref.shape[0]
    own_i = ei_ref.shape[0]
    n_chunk = own_i // CHUNK
    row = lax.axis_index("row")
    col = lax.axis_index("col")
    mate = row + 1 - 2 * (row % 2)
    far = (row + 2) % 4
    far_mate = (mate + 2) % 4
    other_col = 1 - col
    to_mate = {"row": mate}
    to_far = {"row": far}
    to_col = {"col": other_col}
    emb = lax.axis_index("emb")
    to_emb = {"emb": 1 - emb}
    peers = [{"row": (row + dr) % 4, "col": (col + dc) % 2} for dr in range(4) for dc in range(2)][1:]
    share = loss_ref.shape[1] // 8

    def remote(src, dst, ssem, rsem, target):
        return pltpu.make_async_remote_copy(src_ref=src, dst_ref=dst, send_sem=ssem, recv_sem=rsem,
                                            device_id=target, device_id_type=MESH)

    def rows_of(owner, j, size=CHUNK):
        return pl.ds(pl.multiple_of(owner * own_i + j * size, size), size)

    barrier = pltpu.get_barrier_semaphore()
    for target in [*peers, to_emb]:
        pl.semaphore_signal(barrier, inc=1, device_id=target, device_id_type=MESH)
    pl.semaphore_wait(barrier, 8)

    block = pl.ds(pl.multiple_of(row * own_i, own_i), own_i)
    far_block = pl.ds(pl.multiple_of(far * own_i, own_i), own_i)
    ublock = pl.ds(pl.multiple_of(col * own_u, own_u), own_u)
    oblock = pl.ds(pl.multiple_of(other_col * own_u, own_u), own_u)
    ag0_x = remote(ei_ref, panel.at[0, block], ag0_s.at[0], ag0_r.at[0], to_far)
    ag0_d = remote(ei_ref, panel.at[0, block], ag0_s.at[1], ag0_r.at[1], to_mate)
    ag0_f = remote(panel.at[0, far_block], panel.at[0, far_block], ag0_s.at[2], ag0_r.at[2], to_mate)
    ag0_x.start()
    ag0_d.start()
    u0 = remote(eu_ref, upanel.at[0, ublock], u_s.at[0], u_r.at[0], to_col)
    u0.start()

    n_mask = items // MASK_COLS

    def mask_copy(i):
        cols = pl.ds(pl.multiple_of(i * MASK_COLS, MASK_COLS), MASK_COLS)
        slot = i % MASK_SLOTS
        return pltpu.make_async_copy(mask_hbm.at[:, cols], mbuf.at[slot], msem.at[slot])

    for i in range(MASK_SLOTS - 1):
        mask_copy(i).start()
    panel[0, block, :] = ei_ref[...]
    upanel[0, ublock, :] = eu_ref[...]
    rsum[...] = jnp.zeros_like(rsum)

    def mask_step(i, carry):
        mask_copy(i).wait()

        @pl.when(i + MASK_SLOTS - 1 < n_mask)
        def _():
            mask_copy(i + MASK_SLOTS - 1).start()

        cols = pl.ds(pl.multiple_of(i * MASK_COLS, MASK_COLS), MASK_COLS)
        slot = i % MASK_SLOTS

        def tile(t, acc):
            rows = pl.ds(pl.multiple_of(t * 64, 64), 64)
            m = mbuf[slot, rows, :].astype(F32)
            adj[rows, cols] = m.astype(BF16)
            part = m[:, 0:128]
            for g in range(1, MASK_COLS // 128):
                part = part + m[:, g * 128:(g + 1) * 128]
            rsum[rows, :] += part
            return acc + jnp.sum(m.reshape(8, 8, MASK_COLS), axis=0)

        acc = lax.fori_loop(0, users // 64, tile, jnp.zeros((8, MASK_COLS), F32))
        csum[:, cols] = jnp.sum(acc, axis=0, keepdims=True)
        return carry

    lax.fori_loop(0, n_mask, mask_step, 0)

    deg_d = remote(csum, ccore, deg_s.at[0], deg_r.at[0], to_mate)
    deg_d.start()
    ones = jnp.ones((8, 128), BF16)
    rdeg[...] = lax.dot_general(ones, rsum[...].astype(BF16), (((1,), (1,)), ((), ())),
                                preferred_element_type=F32)
    deg_y = remote(rdeg, rdfar, deg_s.at[1], deg_r.at[1], to_col)
    deg_y.start()
    deg_d.wait()
    cchip[...] = csum[...] + ccore[...]
    deg_x = remote(cchip, cfar, deg_s.at[2], deg_r.at[2], to_far)
    deg_x.start()
    ag0_x.wait_recv()
    ag0_f.start()
    u0.wait_recv()
    deg_y.wait()
    deg_u = jnp.maximum(rdeg[0:1, :] + rdfar[0:1, :], 1.0)
    rscale[...] = lax.rsqrt(jnp.broadcast_to(deg_u, (128, users)).T)
    deg_x.wait()
    csum[...] = lax.rsqrt(jnp.maximum(cchip[...] + cfar[...], 1.0))

    def scale_block(owner, j):
        cols = rows_of(owner, j)
        ci = csum[:, cols]

        def tile(t, carry):
            rows = pl.ds(pl.multiple_of(t * SCALE_ROWS, SCALE_ROWS), SCALE_ROWS)
            ru = rscale[rows, :]
            for g in range(CHUNK // 128):
                sub = pl.ds(pl.multiple_of(owner * own_i + j * CHUNK + g * 128, 128), 128)
                m = adj[rows, sub].astype(F32)
                adj[rows, sub] = ((ru * m) * ci[:, g * 128:(g + 1) * 128]).astype(BF16)
            return carry

        lax.fori_loop(0, users // SCALE_ROWS, tile, 0)

    def item_part(owner, j, layer):
        return lax.dot_general(adj[:, rows_of(owner, j)], upanel[layer - 1], (((0,), (0,)), ((), ())),
                               preferred_element_type=F32)

    def core_copy(slot):
        return remote(stage.at[slot_rows(slot)], drecv.at[slot_rows(slot)], d_s.at[slot], d_r.at[slot], to_mate)

    def region(k, j):
        return pl.ds(pl.multiple_of(k * own_i + j * CHUNK, CHUNK), CHUNK)

    def near(j):
        return region(0, j)

    def arrived(j, layer):
        return region(1 + layer % 2, j)

    def xsend(j):
        return region(3, j)

    def chunk_rows(j):
        return pl.ds(pl.multiple_of(j * CHUNK, CHUNK), CHUNK)

    def slot_rows(slot, half=None):
        if half is None:
            return pl.ds(pl.multiple_of(slot * 2 * CHUNK, 2 * CHUNK), 2 * CHUNK)
        return pl.ds(pl.multiple_of(slot * 2 * CHUNK + half * CHUNK, CHUNK), CHUNK)

    def x_copy(j, layer):
        return remote(table.at[xsend(j)], table.at[arrived(j, layer)], x_s.at[j], x_r.at[layer % 2, j], to_far)

    def item_send_step(j, layer):
        slot = j % CORE_SLOTS
        if layer == 1:
            @pl.when(j >= CORE_SLOTS)
            def _():
                core_copy(slot).wait_send()
            scale_block(far_mate, j)
            scale_block(mate, j)
        else:
            core_copy(slot).wait_send()
        stage[slot_rows(slot, 0), :] = item_part(far_mate, j, layer)
        stage[slot_rows(slot, 1), :] = item_part(mate, j, layer)
        core_copy(slot).start()
        if layer == 1:
            scale_block(far, j)
            scale_block(row, j)
        else:
            x_copy(j, layer - 1).wait_send()
        table[xsend(j), :] = item_part(far, j, layer)
        table[near(j), :] = item_part(row, j, layer)

        @pl.when(j == 0)
        def _():
            add_mate(0, layer)

        @pl.when(j >= 2)
        def _():
            add_mate(j - 1, layer)

    def add_mate(j, layer):
        slot = j % CORE_SLOTS
        core_copy(slot).wait_recv()
        table[xsend(j), :] += drecv[slot_rows(slot, 0), :]
        table[near(j), :] += drecv[slot_rows(slot, 1), :]
        x_copy(j, layer).start()

    def ag_copy(kind, j, layer):
        par = layer % 2
        block = panel.at[par, rows_of(far if kind == "fwd" else row, j)]
        ssem, rsem, target = {"x": (agx_s, agx_r, to_far), "mate": (agd_s, agd_r, to_mate),
                              "fwd": (agf_s, agf_r, to_mate)}[kind]
        return remote(block, block, ssem.at[j], rsem.at[par, j], target)

    def fin_copy(kind, j):
        src, dst, k, target = {
            "col": (panel.at[1, rows_of(row, j)], panel.at[1, rows_of(far, j)], 0, to_col),
            "mate": (panel.at[1, rows_of(row, j)], panel.at[1, rows_of(row, j)], 1, to_mate),
            "fwd": (panel.at[1, rows_of(far, j)], panel.at[1, rows_of(far, j)], 2, to_mate)}[kind]
        return remote(src, dst, fin_s.at[k, j], fin_r.at[k, j], target)

    def out_copy(j):
        return pltpu.make_async_copy(panel.at[1, rows_of(row, j)], outi_ref.at[chunk_rows(j)], out_s.at[j])

    def fin_near(j):
        fin_copy("col", j).wait_recv()
        fin_copy("fwd", j).start()
        table[region(2, j), :] = panel[1, rows_of(far, j), :].astype(F32)
        fin_copy("mate", j).wait_recv()
        table[region(1, j), :] = panel[1, rows_of(mate, j), :].astype(F32)

    def fin_fwd(j):
        x_copy(j, NUM_LAYERS).wait_send()
        fin_copy("fwd", j).wait_recv()
        table[region(3, j), :] = panel[1, rows_of(far_mate, j), :].astype(F32)

    def finish_item(j, layer):
        x_copy(j, layer).wait_recv()
        par = layer % 2
        value = (table[near(j), :] + table[arrived(j, layer), :]).astype(BF16)
        if layer < NUM_LAYERS:
            panel[par, rows_of(row, j), :] = value
            ag_copy("x", j, layer).start()
            ag_copy("mate", j, layer).start()
        else:
            total = ei_ref[chunk_rows(j), :].astype(F32) + panel[1, rows_of(row, j), :].astype(F32)
            total = total + panel[0, rows_of(row, j), :].astype(F32)
            total = total + value.astype(F32)
            final = (total / (NUM_LAYERS + 1)).astype(BF16)
            panel[1, rows_of(row, j), :] = final
            table[near(j), :] = final.astype(F32)
            fin_copy("col", j).start()
            fin_copy("mate", j).start()
            out_copy(j).start()

    def gather_items(layer):
        def forward(j, carry):
            ag_copy("x", j, layer).wait_recv()
            ag_copy("fwd", j, layer).start()
            return carry

        def settle(j, carry):
            ag_copy("mate", j, layer).wait_recv()
            ag_copy("fwd", j, layer).wait_recv()
            for kind in ("x", "mate", "fwd"):
                ag_copy(kind, j, layer).wait_send()
            return carry

        lax.fori_loop(0, n_chunk, forward, 0)
        lax.fori_loop(0, n_chunk, settle, 0)

    def user_part(layer):
        par = (layer - 1) % 2
        upart[...] = jnp.zeros_like(upart)

        def fold(i, carry):
            cols = pl.ds(pl.multiple_of(i * FOLD, FOLD), FOLD)
            upart[...] += jnp.dot(adj[:, cols], panel[par, cols, :], preferred_element_type=F32)
            return carry

        lax.fori_loop(0, items // FOLD, fold, 0)

    def yrows(layer):
        return pl.ds((layer - 1) * own_u, own_u)

    def y_copy(layer):
        return remote(upart.at[oblock], yflat.at[yrows(layer)], y_s.at[layer - 1], y_r.at[layer - 1], to_col)

    def u_copy(layer):
        return remote(upanel.at[layer, ublock], upanel.at[layer, ublock], u_s.at[layer], u_r.at[layer], to_col)

    def finish_user(layer):
        y_copy(layer).wait()
        value = (upart[ublock, :] + yflat[yrows(layer), :]).astype(BF16)
        if layer < NUM_LAYERS:
            upanel[layer, ublock, :] = value
            u_copy(layer).start()
        else:
            total = eu_ref[...].astype(F32) + upanel[1, ublock, :].astype(F32)
            total = total + upanel[2, ublock, :].astype(F32)
            total = total + value.astype(F32)
            final = (total / (NUM_LAYERS + 1)).astype(BF16)
            outu_ref[...] = final
            stage[0:own_u, :] = final.astype(F32)
            fu_copy("col").start()
            fu_copy("mate").start()

    def fu_copy(kind):
        src, dst, k, target = {
            "col": (outu_ref, upanel.at[0, pl.ds(0, own_u)], 0, to_col),
            "mate": (outu_ref, upanel.at[0, pl.ds(own_u, own_u)], 1, to_mate),
            "fwd": (upanel.at[0, pl.ds(0, own_u)], upanel.at[1, oblock], 2, to_mate)}[kind]
        return remote(src, dst, fu_s.at[k], fu_r.at[k], target)

    def gather_users():
        fu_copy("col").wait_recv()
        fu_copy("fwd").start()
        stage[2 * own_u:3 * own_u, :] = upanel[0, 0:own_u, :].astype(F32)
        fu_copy("mate").wait_recv()
        stage[own_u:2 * own_u, :] = upanel[0, own_u:2 * own_u, :].astype(F32)
        fu_copy("fwd").wait_recv()
        stage[3 * own_u:4 * own_u, :] = upanel[1, oblock, :].astype(F32)

    def place_rows(piece):
        def side(r):
            return r // 2

        def step(t, carry):
            for k, owner in ((0, far), (1, row)):
                base = (owner * 2 + col) * share + t
                user = trip_ref[0, base]
                ur = lax.shift_right_logical(user, 10)
                uc = lax.bitwise_and(lax.shift_right_logical(user, 9), 1)
                pos = (jnp.where(uc == col, 0, 2) + jnp.where(ur == row, 0, 1)) * own_u + lax.bitwise_and(user, 511)
                pick_idx[k * 3 * share + t] = jnp.where(lax.shift_right_logical(ur, 1) == side(row), pos, 4 * own_u)
                for which in (1, 2):
                    item = trip_ref[which, base]
                    ic = lax.shift_right_logical(item, 14)
                    ir = lax.bitwise_and(lax.shift_right_logical(item, 12), 3)
                    pos = (jnp.where(ic == col, 0, 2) + jnp.where(ir == row, 0, 1)) * own_i + lax.bitwise_and(item, 4095)
                    pick_idx[(k * 3 + which) * share + t] = jnp.where(
                        lax.shift_right_logical(ir, 1) == side(row), pos, 4 * own_i)
            return carry

        lax.fori_loop(piece * (share // PIECES), (piece + 1) * (share // PIECES), step, 0)

    def pick(src, k, which, dst):
        def step(t, carry):
            for i in range(8):
                at = t * 8 + i
                dst[pl.ds(which * share + at, 1), :] = src[pl.ds(pick_idx[(k * 3 + which) * share + at], 1), :]
            return carry

        lax.fori_loop(0, share // 8, step, 0)

    def out_rows(which):
        return pl.ds(pl.multiple_of(far * own_i + which * share, share), share)

    def pick_copy(which):
        rows = pl.ds(which * share, share)
        return remote(panel.at[0, out_rows(which)], pick_in.at[rows], pick_s.at[which], pick_r.at[which], to_far)

    def pick_far(src, which):
        pick(src, 0, which, yflat)
        rows = pl.ds(which * share, share)
        panel[0, out_rows(which), :] = yflat[rows, :].astype(BF16)
        pick_copy(which).start()

    def loop(lo, hi, body):
        def step(j, carry):
            body(j)
            return carry
        lax.fori_loop(lo, hi, step, 0)

    for layer in range(1, NUM_LAYERS + 1):
        loop(0, n_chunk, functools.partial(item_send_step, layer=layer))
        add_mate(n_chunk - 1, layer)
        if layer == 1:
            ag0_d.wait_recv()
            ag0_f.wait_recv()
            ag0_x.wait_send()
            ag0_d.wait_send()
            ag0_f.wait_send()
            u0.wait_send()
        else:
            gather_items(layer - 1)
        user_part(layer)
        y_copy(layer).start()
        if layer < NUM_LAYERS:
            loop(0, n_chunk // 2, functools.partial(finish_item, layer=layer))
            if layer == 1:
                loop(0, 4, place_rows)
            finish_user(layer)
            if layer > 1:
                loop(4, PIECES, place_rows)
            loop(n_chunk // 2, n_chunk, functools.partial(finish_item, layer=layer))
            u_copy(layer).wait()

    for slot in range(CORE_SLOTS):
        core_copy(slot).wait_send()
    table[pl.ds(4 * own_i, 8), :] = jnp.zeros((8, 128), F32)
    stage[pl.ds(4 * own_u, 8), :] = jnp.zeros((8, 128), F32)

    def last_step(j):
        finish_item(j, NUM_LAYERS)

        @pl.when(j >= LAG)
        def _():
            fin_near(j - LAG)

        @pl.when(j >= LAG + 2)
        def _():
            fin_fwd(j - LAG - 2)

    loop(0, n_chunk // 2, last_step)
    finish_user(NUM_LAYERS)
    loop(n_chunk // 2, 3 * n_chunk // 4, last_step)
    gather_users()
    pick_far(stage, 0)
    pick(stage, 1, 0, drecv)
    loop(3 * n_chunk // 4, n_chunk, last_step)
    loop(n_chunk - LAG, n_chunk, fin_near)
    loop(n_chunk - LAG - 2, n_chunk, fin_fwd)
    pick_far(table, 1)
    pick_far(table, 2)
    pick(table, 1, 1, drecv)
    pick(table, 1, 2, drecv)

    def both(which):
        rows = pl.ds(which * share, share)
        pick_copy(which).wait_recv()
        return drecv[rows, :] + pick_in[rows, :].astype(F32)

    e_user, e_pos, e_neg = both(0), both(1), both(2)
    prod = e_user * (e_pos - e_neg)
    dots[0] = jnp.sum(prod.T, axis=0, keepdims=True)
    dot_copy = remote(dots.at[0], dots.at[1], dot_s.at[0], dot_r.at[0], to_emb)
    dot_copy.start()
    dot_copy.wait()
    z = -(dots[0] + dots[1])
    mine = pl.ds(pl.multiple_of((row * 2 + col) * share, share), share)
    loss_ref[:, mine] = jnp.maximum(z, 0.0) + jnp.log1p(jnp.exp(-jnp.abs(z)))
    copies = [remote(loss_ref.at[:, mine], loss_ref.at[:, mine], loss_s.at[k], loss_r.at[k], target)
              for k, target in enumerate(peers)]
    for copy in copies:
        copy.start()

    for which in range(3):
        pick_copy(which).wait_send()
    for kind in ("col", "mate", "fwd"):
        fu_copy(kind).wait_send()
        loop(0, n_chunk, lambda j: fin_copy(kind, j).wait_send())
    loop(0, n_chunk, lambda j: out_copy(j).wait())
    for copy in copies:
        copy.wait()


def propagate(mask_blk, user_sh, item_sh, triples):
    users, items = mask_blk.shape
    own_u, dim = user_sh.shape
    own_i = item_sh.shape[0]
    n_chunk = own_i // CHUNK
    num_trip = triples.shape[0]
    share = num_trip // 8
    vmem, dma = pltpu.VMEM, pltpu.SemaphoreType.DMA
    return pl.pallas_call(
        prop_kernel,
        name="propagate",
        out_shape=(jax.ShapeDtypeStruct((own_u, dim), BF16), jax.ShapeDtypeStruct((own_i, dim), BF16),
                   jax.ShapeDtypeStruct((1, num_trip), F32)),
        in_specs=[pl.BlockSpec(memory_space=pl.ANY), pl.BlockSpec(memory_space=pltpu.VMEM),
                  pl.BlockSpec(memory_space=pltpu.VMEM), pl.BlockSpec(memory_space=pltpu.SMEM)],
        out_specs=(pl.BlockSpec(memory_space=pltpu.VMEM), pl.BlockSpec(memory_space=pl.ANY),
                   pl.BlockSpec(memory_space=pltpu.VMEM)),
        scratch_shapes=[
            vmem((users, items), BF16),
            vmem((MASK_SLOTS, users, MASK_COLS), jnp.int32),
            vmem((2, items, dim), BF16),
            vmem((4 * own_i + 8, dim), F32),
            vmem((CORE_SLOTS * 2 * CHUNK + 8, dim), F32),
            vmem((CORE_SLOTS * 2 * CHUNK, dim), F32),
            vmem((3, users, dim), BF16),
            vmem((users, dim), F32),
            vmem((3 * own_u, dim), F32),
            vmem((1, items), F32),
            vmem((1, items), F32),
            vmem((1, items), F32),
            vmem((1, items), F32),
            vmem((8, users), F32),
            vmem((8, users), F32),
            pltpu.SMEM((6 * share,), jnp.int32),
            vmem((3 * share, dim), BF16),
            vmem((2, 1, share), F32),
            dma((MASK_SLOTS,)),
            dma((3,)), dma((3,)),
            dma((3,)), dma((3,)),
            dma((3,)), dma((3,)),
            dma((3,)), dma((3,)),
            dma((CORE_SLOTS,)), dma((CORE_SLOTS,)),
            dma((n_chunk,)), dma((2, n_chunk)),
            dma((n_chunk,)), dma((2, n_chunk)),
            dma((n_chunk,)), dma((2, n_chunk)),
            dma((n_chunk,)), dma((2, n_chunk)),
            dma((3, n_chunk)), dma((3, n_chunk)),
            dma((3,)), dma((3,)),
            dma((3,)), dma((3,)),
            dma((1,)), dma((1,)),
            dma((n_chunk,)),
            dma((7,)), dma((7,)),
        ],
        compiler_params=pltpu.CompilerParams(collective_id=0, has_side_effects=True,
                                             vmem_limit_bytes=67_043_328),
    )(mask_blk, user_sh, item_sh, triples.T)


def solution(mesh):
    def local_fn(mask_blk, user_sh, item_sh, triples):
        final_user, final_item, loss = propagate(mask_blk, user_sh, item_sh, triples)
        return final_user, final_item, loss.reshape(-1)

    return jax.shard_map(
        local_fn, mesh=mesh,
        in_specs=(P("row", "col"), P(("row", "col"), "emb"), P(("col", "row"), "emb"), P()),
        out_specs=(P(("row", "col"), "emb"), P(("col", "row"), "emb"), P()),
        check_vma=False)
```

```python
import functools

import jax
import jax.numpy as jnp
from jax import lax
from jax.experimental import pallas as pl
from jax.experimental.pallas import tpu as pltpu
from jax.sharding import PartitionSpec as P

NUM_LAYERS = 3
F32 = jnp.float32
BF16 = jnp.bfloat16
MESH = pl.DeviceIdType.MESH

CHUNK = 256
MASK_SLOTS = 7
EARLY = 12
PIECES = 16
CORE_SLOTS = 4
SCALE_ROWS = 256
LAG = 3
FOLD = 2048


def prop_kernel(mask_hbm, eu_hbm, ei_hbm, trip_hbm, outu_ref, outi_ref, loss_ref,
                adj, mbuf, panel, table, stage, drecv, upanel, upart, yflat, eu_ref, ei_ref, trip_ref,
                csum, ccore, cchip, cfar, rdeg, rdfar, pick_idx, pick_in, dots,
                in_s, msem, ag0_s, ag0_r, deg_s, deg_r, u_s, u_r, y_s, y_r,
                d_s, d_r, x_s, x_r, agx_s, agx_r, agd_s, agd_r, agf_s, agf_r,
                fin_s, fin_r, fu_s, fu_r, pick_s, pick_r, out_s, loss_s, loss_r):
    users, items = adj.shape
    rsum = rscale = upart
    own_u = eu_ref.shape[0]
    own_i = ei_ref.shape[0]
    n_chunk = own_i // CHUNK
    row = lax.axis_index("row")
    col = lax.axis_index("col")
    mate = row + 1 - 2 * (row % 2)
    far = (row + 2) % 4
    far_mate = (mate + 2) % 4
    other_col = 1 - col
    to_mate = {"row": mate}
    to_far = {"row": far}
    to_col = {"col": other_col}
    emb = lax.axis_index("emb")
    peers = [{"emb": (emb + de) % 2, "row": (row + dr) % 4, "col": (col + dc) % 2}
             for de in range(2) for dr in range(4) for dc in range(2)][1:]
    share = loss_ref.shape[1] // 8

    def remote(src, dst, ssem, rsem, target):
        return pltpu.make_async_remote_copy(src_ref=src, dst_ref=dst, send_sem=ssem, recv_sem=rsem,
                                            device_id=target, device_id_type=MESH)

    def rows_of(owner, j, size=CHUNK):
        return pl.ds(pl.multiple_of(owner * own_i + j * size, size), size)

    block = pl.ds(pl.multiple_of(row * own_i, own_i), own_i)
    far_block = pl.ds(pl.multiple_of(far * own_i, own_i), own_i)
    ublock = pl.ds(pl.multiple_of(col * own_u, own_u), own_u)
    oblock = pl.ds(pl.multiple_of(other_col * own_u, own_u), own_u)
    n_mask = items // CHUNK

    def mask_copy(i):
        slot = i % MASK_SLOTS
        return pltpu.make_async_copy(mask_hbm.at[:, rows_of(i % 4, i // 4)], mbuf.at[slot], msem.at[slot])

    for i in range(MASK_SLOTS - 1):
        mask_copy(i).start()
    inputs = [pltpu.make_async_copy(src, dst, in_s.at[k]) for k, (src, dst) in enumerate((
        (eu_hbm, upanel.at[0, ublock]), (ei_hbm, panel.at[0, block]), (eu_hbm, eu_ref), (ei_hbm, ei_ref),
        (trip_hbm, trip_ref)))]
    for copy in inputs:
        copy.start()

    barrier = pltpu.get_barrier_semaphore()
    for target in peers:
        pl.semaphore_signal(barrier, inc=1, device_id=target, device_id_type=MESH)
    pl.semaphore_wait(barrier, len(peers))

    quarter = own_i // 4

    def ag0_x(k):
        return remote(ei_hbm.at[pl.ds(k * quarter, quarter)],
                      panel.at[0, pl.ds(pl.multiple_of(row * own_i + k * quarter, quarter), quarter)],
                      ag0_s.at[k], ag0_r.at[k], to_far)

    ag0_d = remote(ei_hbm, panel.at[0, block], ag0_s.at[4], ag0_r.at[4], to_mate)
    ag0_f = remote(panel.at[0, far_block], panel.at[0, far_block], ag0_s.at[5], ag0_r.at[5], to_mate)
    for k in range(3):
        ag0_x(k).start()
    ag0_d.start()
    u0 = remote(eu_hbm, upanel.at[0, ublock], u_s.at[0], u_r.at[0], to_col)
    u0.start()

    rsum[...] = jnp.zeros_like(rsum)

    def mask_step(i, carry):
        mask_copy(i).wait()

        @pl.when(i + MASK_SLOTS - 1 < n_mask)
        def _():
            mask_copy(i + MASK_SLOTS - 1).start()

        cols = rows_of(i % 4, i // 4)
        slot = i % MASK_SLOTS

        def tile(t, acc):
            rows = pl.ds(pl.multiple_of(t * 64, 64), 64)
            m = mbuf[slot, rows, :].astype(F32)
            adj[rows, cols] = m.astype(BF16)
            part = m[:, 0:128]
            for g in range(1, CHUNK // 128):
                part = part + m[:, g * 128:(g + 1) * 128]
            rsum[rows, :] += part
            return acc + jnp.sum(m.reshape(8, 8, CHUNK), axis=0)

        acc = lax.fori_loop(0, users // 64, tile, jnp.zeros((8, CHUNK), F32))
        csum[:, pl.ds(pl.multiple_of(i * CHUNK, CHUNK), CHUNK)] = jnp.sum(acc, axis=0, keepdims=True)
        return carry

    early = EARLY * 4 * CHUNK
    parts = (pl.ds(0, early), pl.ds(early, items - early))

    def deg_d(k):
        return remote(csum.at[:, parts[k]], ccore.at[:, parts[k]], deg_s.at[k], deg_r.at[k], to_mate)

    def deg_x(k):
        return remote(cchip.at[:, parts[k]], cfar.at[:, parts[k]], deg_s.at[2 + k], deg_r.at[2 + k], to_far)

    def add_core(k):
        deg_d(k).wait()
        cchip[:, parts[k]] = csum[:, parts[k]] + ccore[:, parts[k]]
        deg_x(k).start()

    def col_factors(k):
        deg_x(k).wait()
        csum[:, parts[k]] = lax.rsqrt(jnp.maximum(cchip[:, parts[k]] + cfar[:, parts[k]], 1.0))

    lax.fori_loop(0, 4 * EARLY, mask_step, 0)
    deg_d(0).start()
    lax.fori_loop(4 * EARLY, 4 * EARLY + 4, mask_step, 0)
    add_core(0)
    ag0_x(3).start()
    lax.fori_loop(4 * EARLY + 4, n_mask, mask_step, 0)

    ones = jnp.ones((8, 128), BF16)
    rdeg[...] = lax.dot_general(ones, rsum[...].astype(BF16), (((1,), (1,)), ((), ())),
                                preferred_element_type=F32)
    deg_y = remote(rdeg, rdfar, deg_s.at[4], deg_r.at[4], to_col)
    deg_y.start()
    deg_d(1).start()
    for copy in inputs:
        copy.wait()
    u0.wait_recv()
    col_factors(0)
    add_core(1)
    deg_y.wait()
    deg_u = jnp.maximum(rdeg[0:1, :] + rdfar[0:1, :], 1.0)
    rscale[...] = lax.rsqrt(jnp.broadcast_to(deg_u, (128, users)).T)

    def scale_block(owner, j):
        ci = csum[:, pl.ds(pl.multiple_of((j * 4 + owner) * CHUNK, CHUNK), CHUNK)]

        def tile(t, carry):
            rows = pl.ds(pl.multiple_of(t * SCALE_ROWS, SCALE_ROWS), SCALE_ROWS)
            ru = rscale[rows, :]
            for g in range(CHUNK // 128):
                sub = pl.ds(pl.multiple_of(owner * own_i + j * CHUNK + g * 128, 128), 128)
                m = adj[rows, sub].astype(F32)
                adj[rows, sub] = ((ru * m) * ci[:, g * 128:(g + 1) * 128]).astype(BF16)
            return carry

        lax.fori_loop(0, users // SCALE_ROWS, tile, 0)

    def item_part(owner, j, layer):
        return lax.dot_general(adj[:, rows_of(owner, j)], upanel[layer - 1], (((0,), (0,)), ((), ())),
                               preferred_element_type=F32)

    def core_copy(slot):
        return remote(stage.at[slot_rows(slot)], drecv.at[slot_rows(slot)], d_s.at[slot], d_r.at[slot], to_mate)

    def region(k, j):
        return pl.ds(pl.multiple_of(k * own_i + j * CHUNK, CHUNK), CHUNK)

    def near(j):
        return region(0, j)

    def arrived(j, layer):
        return region(1 + layer % 2, j)

    def xsend(j):
        return region(3, j)

    def chunk_rows(j):
        return pl.ds(pl.multiple_of(j * CHUNK, CHUNK), CHUNK)

    def slot_rows(slot, half=None):
        if half is None:
            return pl.ds(pl.multiple_of(slot * 2 * CHUNK, 2 * CHUNK), 2 * CHUNK)
        return pl.ds(pl.multiple_of(slot * 2 * CHUNK + half * CHUNK, CHUNK), CHUNK)

    def x_copy(j, layer):
        return remote(table.at[xsend(j)], table.at[arrived(j, layer)], x_s.at[j], x_r.at[layer % 2, j], to_far)

    def item_send_step(j, layer):
        slot = j % CORE_SLOTS
        if layer == 1:
            @pl.when(j >= CORE_SLOTS)
            def _():
                core_copy(slot).wait_send()
            scale_block(far_mate, j)
            scale_block(mate, j)
        else:
            core_copy(slot).wait_send()
        stage[slot_rows(slot, 0), :] = item_part(far_mate, j, layer)
        stage[slot_rows(slot, 1), :] = item_part(mate, j, layer)
        core_copy(slot).start()
        if layer == 1:
            scale_block(far, j)
            scale_block(row, j)
        else:
            x_copy(j, layer - 1).wait_send()
        table[xsend(j), :] = item_part(far, j, layer)
        table[near(j), :] = item_part(row, j, layer)

        @pl.when(j == 0)
        def _():
            add_mate(0, layer)

        @pl.when(j >= 2)
        def _():
            add_mate(j - 1, layer)

    def add_mate(j, layer):
        slot = j % CORE_SLOTS
        core_copy(slot).wait_recv()
        table[xsend(j), :] += drecv[slot_rows(slot, 0), :]
        table[near(j), :] += drecv[slot_rows(slot, 1), :]
        x_copy(j, layer).start()

    def ag_copy(kind, j, layer):
        par = layer % 2
        block = panel.at[par, rows_of(far if kind == "fwd" else row, j)]
        ssem, rsem, target = {"x": (agx_s, agx_r, to_far), "mate": (agd_s, agd_r, to_mate),
                              "fwd": (agf_s, agf_r, to_mate)}[kind]
        return remote(block, block, ssem.at[j], rsem.at[par, j], target)

    def fin_copy(kind, j):
        src, dst, k, target = {
            "col": (panel.at[1, rows_of(row, j)], panel.at[1, rows_of(far, j)], 0, to_col),
            "mate": (panel.at[1, rows_of(row, j)], panel.at[1, rows_of(row, j)], 1, to_mate),
            "fwd": (panel.at[1, rows_of(far, j)], panel.at[1, rows_of(far, j)], 2, to_mate)}[kind]
        return remote(src, dst, fin_s.at[k, j], fin_r.at[k, j], target)

    def out_copy(j):
        return pltpu.make_async_copy(panel.at[1, rows_of(row, j)], outi_ref.at[chunk_rows(j)], out_s.at[j])

    def fin_near(j):
        fin_copy("col", j).wait_recv()
        fin_copy("fwd", j).start()
        table[region(2, j), :] = panel[1, rows_of(far, j), :].astype(F32)
        fin_copy("mate", j).wait_recv()
        table[region(1, j), :] = panel[1, rows_of(mate, j), :].astype(F32)

    def fin_fwd(j):
        x_copy(j, NUM_LAYERS).wait_send()
        fin_copy("fwd", j).wait_recv()
        table[region(3, j), :] = panel[1, rows_of(far_mate, j), :].astype(F32)

    def finish_item(j, layer):
        x_copy(j, layer).wait_recv()
        par = layer % 2
        value = (table[near(j), :] + table[arrived(j, layer), :]).astype(BF16)
        if layer < NUM_LAYERS:
            panel[par, rows_of(row, j), :] = value
            ag_copy("x", j, layer).start()
            ag_copy("mate", j, layer).start()
        else:
            total = ei_ref[chunk_rows(j), :].astype(F32) + panel[1, rows_of(row, j), :].astype(F32)
            total = total + panel[0, rows_of(row, j), :].astype(F32)
            total = total + value.astype(F32)
            final = (total / (NUM_LAYERS + 1)).astype(BF16)
            panel[1, rows_of(row, j), :] = final
            table[near(j), :] = final.astype(F32)
            fin_copy("col", j).start()
            fin_copy("mate", j).start()
            out_copy(j).start()

    def gather_items(layer):
        def forward(j, carry):
            ag_copy("x", j, layer).wait_recv()
            ag_copy("fwd", j, layer).start()
            return carry

        def settle(j, carry):
            ag_copy("mate", j, layer).wait_recv()
            ag_copy("fwd", j, layer).wait_recv()
            for kind in ("x", "mate", "fwd"):
                ag_copy(kind, j, layer).wait_send()
            return carry

        lax.fori_loop(0, n_chunk, forward, 0)
        lax.fori_loop(0, n_chunk, settle, 0)

    def user_part(layer):
        par = (layer - 1) % 2
        upart[...] = jnp.zeros_like(upart)

        def fold(i, carry):
            cols = pl.ds(pl.multiple_of(i * FOLD, FOLD), FOLD)
            upart[...] += jnp.dot(adj[:, cols], panel[par, cols, :], preferred_element_type=F32)
            return carry

        lax.fori_loop(0, items // FOLD, fold, 0)

    def yrows(layer):
        return pl.ds((layer - 1) * own_u, own_u)

    def y_copy(layer):
        return remote(upart.at[oblock], yflat.at[yrows(layer)], y_s.at[layer - 1], y_r.at[layer - 1], to_col)

    def u_copy(layer):
        return remote(upanel.at[layer, ublock], upanel.at[layer, ublock], u_s.at[layer], u_r.at[layer], to_col)

    def finish_user(layer):
        y_copy(layer).wait()
        value = (upart[ublock, :] + yflat[yrows(layer), :]).astype(BF16)
        if layer < NUM_LAYERS:
            upanel[layer, ublock, :] = value
            u_copy(layer).start()
        else:
            total = eu_ref[...].astype(F32) + upanel[1, ublock, :].astype(F32)
            total = total + upanel[2, ublock, :].astype(F32)
            total = total + value.astype(F32)
            final = (total / (NUM_LAYERS + 1)).astype(BF16)
            outu_ref[...] = final
            stage[0:own_u, :] = final.astype(F32)
            fu_copy("col").start()
            fu_copy("mate").start()

    def fu_copy(kind):
        src, dst, k, target = {
            "col": (outu_ref, upanel.at[0, pl.ds(0, own_u)], 0, to_col),
            "mate": (outu_ref, upanel.at[0, pl.ds(own_u, own_u)], 1, to_mate),
            "fwd": (upanel.at[0, pl.ds(0, own_u)], upanel.at[1, oblock], 2, to_mate)}[kind]
        return remote(src, dst, fu_s.at[k], fu_r.at[k], target)

    def gather_users():
        fu_copy("col").wait_recv()
        fu_copy("fwd").start()
        stage[2 * own_u:3 * own_u, :] = upanel[0, 0:own_u, :].astype(F32)
        fu_copy("mate").wait_recv()
        stage[own_u:2 * own_u, :] = upanel[0, own_u:2 * own_u, :].astype(F32)
        fu_copy("fwd").wait_recv()
        stage[3 * own_u:4 * own_u, :] = upanel[1, oblock, :].astype(F32)

    def place_rows(piece):
        def side(r):
            return r // 2

        def step(t, carry):
            for k, owner in ((0, far), (1, row)):
                base = (owner * 2 + col) * share + t
                user = trip_ref[0, base]
                ur = lax.shift_right_logical(user, 10)
                uc = lax.bitwise_and(lax.shift_right_logical(user, 9), 1)
                pos = (jnp.where(uc == col, 0, 2) + jnp.where(ur == row, 0, 1)) * own_u + lax.bitwise_and(user, 511)
                pick_idx[k * 3 * share + t] = jnp.where(lax.shift_right_logical(ur, 1) == side(row), pos, 4 * own_u)
                for which in (1, 2):
                    item = trip_ref[which, base]
                    ic = lax.shift_right_logical(item, 14)
                    ir = lax.bitwise_and(lax.shift_right_logical(item, 12), 3)
                    pos = (jnp.where(ic == col, 0, 2) + jnp.where(ir == row, 0, 1)) * own_i + lax.bitwise_and(item, 4095)
                    pick_idx[(k * 3 + which) * share + t] = jnp.where(
                        lax.shift_right_logical(ir, 1) == side(row), pos, 4 * own_i)
            return carry

        lax.fori_loop(piece * (share // PIECES), (piece + 1) * (share // PIECES), step, 0)

    def pick(src, k, which, dst):
        def step(t, carry):
            for i in range(8):
                at = t * 8 + i
                dst[pl.ds(which * share + at, 1), :] = src[pl.ds(pick_idx[(k * 3 + which) * share + at], 1), :]
            return carry

        lax.fori_loop(0, share // 8, step, 0)

    def out_rows(which):
        return pl.ds(pl.multiple_of(far * own_i + which * share, share), share)

    def pick_copy(which):
        rows = pl.ds(which * share, share)
        return remote(panel.at[0, out_rows(which)], pick_in.at[rows], pick_s.at[which], pick_r.at[which], to_far)

    def pick_far(src, which):
        pick(src, 0, which, yflat)
        rows = pl.ds(which * share, share)
        panel[0, out_rows(which), :] = yflat[rows, :].astype(BF16)
        pick_copy(which).start()

    def loop(lo, hi, body):
        def step(j, carry):
            body(j)
            return carry
        lax.fori_loop(lo, hi, step, 0)

    for layer in range(1, NUM_LAYERS + 1):
        if layer == 1:
            loop(0, EARLY, functools.partial(item_send_step, layer=layer))
            col_factors(1)
            for k in range(4):
                ag0_x(k).wait()
            ag0_f.start()
            loop(EARLY, n_chunk, functools.partial(item_send_step, layer=layer))
        else:
            loop(0, n_chunk, functools.partial(item_send_step, layer=layer))
        add_mate(n_chunk - 1, layer)
        if layer == 1:
            ag0_d.wait()
            ag0_f.wait()
            u0.wait_send()
        else:
            gather_items(layer - 1)
        user_part(layer)
        y_copy(layer).start()
        if layer < NUM_LAYERS:
            loop(0, n_chunk // 2, functools.partial(finish_item, layer=layer))
            if layer == 1:
                loop(0, 4, place_rows)
            finish_user(layer)
            if layer > 1:
                loop(4, PIECES, place_rows)
            loop(n_chunk // 2, n_chunk, functools.partial(finish_item, layer=layer))
            u_copy(layer).wait()

    for slot in range(CORE_SLOTS):
        core_copy(slot).wait_send()
    table[pl.ds(4 * own_i, 8), :] = jnp.zeros((8, 128), F32)
    stage[pl.ds(4 * own_u, 8), :] = jnp.zeros((8, 128), F32)

    def last_step(j):
        finish_item(j, NUM_LAYERS)

        @pl.when(j >= LAG)
        def _():
            fin_near(j - LAG)

        @pl.when(j >= LAG + 2)
        def _():
            fin_fwd(j - LAG - 2)

    loop(0, n_chunk // 2, last_step)
    finish_user(NUM_LAYERS)
    loop(n_chunk // 2, 3 * n_chunk // 4, last_step)
    gather_users()
    pick_far(stage, 0)
    pick(stage, 1, 0, drecv)
    loop(3 * n_chunk // 4, n_chunk, last_step)
    loop(n_chunk - LAG, n_chunk, fin_near)
    loop(n_chunk - LAG - 2, n_chunk, fin_fwd)
    pick_far(table, 1)
    pick_far(table, 2)
    pick(table, 1, 1, drecv)
    pick(table, 1, 2, drecv)

    def both(which):
        rows = pl.ds(which * share, share)
        pick_copy(which).wait_recv()
        return drecv[rows, :] + pick_in[rows, :].astype(F32)

    e_user, e_pos, e_neg = both(0), both(1), both(2)
    prod = e_user * (e_pos - e_neg)
    mine = pl.ds(pl.multiple_of((row * 2 + col) * share, share), share)
    dots[emb, :, mine] = jnp.sum(prod.T, axis=0, keepdims=True)
    copies = [remote(dots.at[emb, :, mine], dots.at[emb, :, mine], loss_s.at[k], loss_r.at[k], target)
              for k, target in enumerate(peers)]
    for copy in copies:
        copy.start()

    for which in range(3):
        pick_copy(which).wait_send()
    for kind in ("col", "mate", "fwd"):
        fu_copy(kind).wait_send()
        loop(0, n_chunk, lambda j: fin_copy(kind, j).wait_send())
    loop(0, n_chunk, lambda j: out_copy(j).wait())
    for copy in copies:
        copy.wait()
    z = -(dots[0] + dots[1])
    loss_ref[...] = jnp.maximum(z, 0.0) + jnp.log1p(jnp.exp(-jnp.abs(z)))


def hand_out_kernel(u_in, i_in, l_in, u_out, i_out, l_out, u_buf, i_buf, l_buf, in_s, out_s):
    pieces = [(u_in, u_buf, u_out), (l_in, l_buf, l_out)]
    rows = i_in.shape[0] // 4
    pieces += [tuple(ref.at[pl.ds(k * rows, rows)] for ref in (i_in, i_buf, i_out)) for k in range(4)]
    for k, (src, buf, dst) in enumerate(pieces):
        pltpu.make_async_copy(src, buf, in_s.at[k]).start()
    for k, (src, buf, dst) in enumerate(pieces):
        pltpu.make_async_copy(src, buf, in_s.at[k]).wait()
        pltpu.make_async_copy(buf, dst, out_s.at[k]).start()
    for k, (src, buf, dst) in enumerate(pieces):
        pltpu.make_async_copy(buf, dst, out_s.at[k]).wait()


def hand_out(*arrays):
    return pl.pallas_call(
        hand_out_kernel,
        name="hand_out",
        out_shape=tuple(jax.ShapeDtypeStruct(a.shape, a.dtype) for a in arrays),
        in_specs=[pl.BlockSpec(memory_space=pl.ANY)] * 3,
        out_specs=(pl.BlockSpec(memory_space=pl.ANY),) * 3,
        scratch_shapes=[*(pltpu.VMEM(a.shape, a.dtype) for a in arrays),
                        pltpu.SemaphoreType.DMA((6,)), pltpu.SemaphoreType.DMA((6,))],
    )(*arrays)


def propagate(mask_blk, user_sh, item_sh, triples):
    users, items = mask_blk.shape
    own_u, dim = user_sh.shape
    own_i = item_sh.shape[0]
    n_chunk = own_i // CHUNK
    num_trip = triples.shape[0]
    share = num_trip // 8
    vmem, dma = pltpu.VMEM, pltpu.SemaphoreType.DMA
    return pl.pallas_call(
        prop_kernel,
        name="propagate",
        out_shape=(jax.ShapeDtypeStruct((own_u, dim), BF16), jax.ShapeDtypeStruct((own_i, dim), BF16),
                   jax.ShapeDtypeStruct((1, num_trip), F32)),
        in_specs=[pl.BlockSpec(memory_space=pl.ANY)] * 4,
        out_specs=(pl.BlockSpec(memory_space=pltpu.VMEM), pl.BlockSpec(memory_space=pl.ANY),
                   pl.BlockSpec(memory_space=pltpu.VMEM)),
        scratch_shapes=[
            vmem((users, items), BF16),
            vmem((MASK_SLOTS, users, CHUNK), jnp.int32),
            vmem((2, items, dim), BF16),
            vmem((4 * own_i + 8, dim), F32),
            vmem((CORE_SLOTS * 2 * CHUNK + 8, dim), F32),
            vmem((CORE_SLOTS * 2 * CHUNK, dim), F32),
            vmem((3, users, dim), BF16),
            vmem((users, dim), F32),
            vmem((3 * own_u, dim), F32),
            vmem((own_u, dim), BF16),
            vmem((own_i, dim), BF16),
            pltpu.SMEM((3, num_trip), jnp.int32),
            vmem((1, items), F32),
            vmem((1, items), F32),
            vmem((1, items), F32),
            vmem((1, items), F32),
            vmem((8, users), F32),
            vmem((8, users), F32),
            pltpu.SMEM((6 * share,), jnp.int32),
            vmem((3 * share, dim), BF16),
            vmem((2, 1, num_trip), F32),
            dma((5,)),
            dma((MASK_SLOTS,)),
            dma((6,)), dma((6,)),
            dma((5,)), dma((5,)),
            dma((3,)), dma((3,)),
            dma((3,)), dma((3,)),
            dma((CORE_SLOTS,)), dma((CORE_SLOTS,)),
            dma((n_chunk,)), dma((2, n_chunk)),
            dma((n_chunk,)), dma((2, n_chunk)),
            dma((n_chunk,)), dma((2, n_chunk)),
            dma((n_chunk,)), dma((2, n_chunk)),
            dma((3, n_chunk)), dma((3, n_chunk)),
            dma((3,)), dma((3,)),
            dma((3,)), dma((3,)),
            dma((n_chunk,)),
            dma((15,)), dma((15,)),
        ],
        compiler_params=pltpu.CompilerParams(collective_id=0, has_side_effects=True,
                                             vmem_limit_bytes=67_043_328),
    )(mask_blk, user_sh, item_sh, triples.T)


def solution(mesh):
    def local_fn(mask_blk, user_sh, item_sh, triples):
        final_user, final_item, loss = hand_out(*propagate(mask_blk, user_sh, item_sh, triples))
        return final_user, final_item, loss.reshape(-1)

    return jax.shard_map(
        local_fn, mesh=mesh,
        in_specs=(P("row", "col"), P(("row", "col"), "emb"), P(("col", "row"), "emb"), P()),
        out_specs=(P(("row", "col"), "emb"), P(("col", "row"), "emb"), P()),
        check_vma=False)
```

```python
import functools

import jax
import jax.numpy as jnp
from jax import lax
from jax.experimental import pallas as pl
from jax.experimental.pallas import tpu as pltpu
from jax.sharding import PartitionSpec as P

NUM_LAYERS = 3
F32 = jnp.float32
BF16 = jnp.bfloat16
MESH = pl.DeviceIdType.MESH

CHUNK = 256
MASK_SLOTS = 7
GROUP = 4
EARLY = 8
PIECES = 16
CORE_SLOTS = 4
SCALE_ROWS = 256
LAG = 3
FOLD = 2048


def prop_kernel(mask_hbm, eu_hbm, ei_hbm, trip_hbm, outu_ref, outi_ref, loss_ref,
                adj, mbuf, panel, table, stage, drecv, upanel, upart, yflat, eu_ref, ei_ref, trip_ref, trip_vec,
                csum, ccore, cchip, cfar, rdeg, rdfar, pick_idx, pick_in, mixed, dots,
                in_s, msem, ag0_s, ag0_r, deg_s, deg_r, u_s, u_r, y_s, y_r,
                d_s, d_r, x_s, x_r, agx_s, agx_r, agd_s, agd_r, agf_s, agf_r,
                fin_s, fin_r, fu_s, fu_r, pick_s, pick_r, out_s, loss_s, loss_r):
    users, items = adj.shape
    rsum = rscale = upart
    own_u = eu_ref.shape[0]
    own_i = ei_ref.shape[0]
    n_chunk = own_i // CHUNK
    row = lax.axis_index("row")
    col = lax.axis_index("col")
    mate = row + 1 - 2 * (row % 2)
    far = (row + 2) % 4
    far_mate = (mate + 2) % 4
    other_col = 1 - col
    to_mate = {"row": mate}
    to_far = {"row": far}
    to_col = {"col": other_col}
    emb = lax.axis_index("emb")
    peers = [{"emb": (emb + de) % 2, "row": (row + dr) % 4, "col": (col + dc) % 2}
             for de in range(2) for dr in range(4) for dc in range(2)][1:]
    share = loss_ref.shape[1] // 8

    def remote(src, dst, ssem, rsem, target):
        return pltpu.make_async_remote_copy(src_ref=src, dst_ref=dst, send_sem=ssem, recv_sem=rsem,
                                            device_id=target, device_id_type=MESH)

    def rows_of(owner, j, size=CHUNK):
        return pl.ds(pl.multiple_of(owner * own_i + j * size, size), size)

    block = pl.ds(pl.multiple_of(row * own_i, own_i), own_i)
    far_block = pl.ds(pl.multiple_of(far * own_i, own_i), own_i)
    ublock = pl.ds(pl.multiple_of(col * own_u, own_u), own_u)
    oblock = pl.ds(pl.multiple_of(other_col * own_u, own_u), own_u)
    n_mask = items // CHUNK

    def mask_copy(i):
        slot = i % MASK_SLOTS
        return pltpu.make_async_copy(mask_hbm.at[:, rows_of(i % 4, i // 4)], mbuf.at[slot], msem.at[slot])

    for i in range(MASK_SLOTS - 1):
        mask_copy(i).start()
    inputs = [pltpu.make_async_copy(src, dst, in_s.at[k]) for k, (src, dst) in enumerate((
        (eu_hbm, upanel.at[0, ublock]), (ei_hbm, panel.at[0, block]), (eu_hbm, eu_ref), (ei_hbm, ei_ref),
        (trip_hbm, trip_ref), (trip_hbm, trip_vec)))]
    for copy in inputs:
        copy.start()

    barrier = pltpu.get_barrier_semaphore()
    for target in peers:
        pl.semaphore_signal(barrier, inc=1, device_id=target, device_id_type=MESH)

    rsum[...] = jnp.zeros_like(rsum)

    def mask_step(i, carry):
        mask_copy(i).wait()

        @pl.when(i + MASK_SLOTS - 1 < n_mask)
        def _():
            mask_copy(i + MASK_SLOTS - 1).start()

        cols = rows_of(i % 4, i // 4)
        slot = i % MASK_SLOTS

        def tile(t, acc):
            rows = pl.ds(pl.multiple_of(t * 64, 64), 64)
            m = mbuf[slot, rows, :].astype(F32)
            adj[rows, cols] = m.astype(BF16)
            part = m[:, 0:128]
            for g in range(1, CHUNK // 128):
                part = part + m[:, g * 128:(g + 1) * 128]
            rsum[rows, :] += part
            return acc + jnp.sum(m.reshape(8, 8, CHUNK), axis=0)

        acc = lax.fori_loop(0, users // 64, tile, jnp.zeros((8, CHUNK), F32))
        csum[:, pl.ds(pl.multiple_of(i * CHUNK, CHUNK), CHUNK)] = jnp.sum(acc, axis=0, keepdims=True)
        return carry

    pl.semaphore_wait(barrier, len(peers))

    quarter = own_i // 4

    def ag0_x(k):
        return remote(ei_hbm.at[pl.ds(k * quarter, quarter)],
                      panel.at[0, pl.ds(pl.multiple_of(row * own_i + k * quarter, quarter), quarter)],
                      ag0_s.at[0], ag0_r.at[0], to_far)

    ag0_d = remote(ei_hbm, panel.at[0, block], ag0_s.at[1], ag0_r.at[1], to_mate)
    ag0_f = remote(panel.at[0, far_block], panel.at[0, far_block], ag0_s.at[2], ag0_r.at[2], to_mate)
    for k in range(2):
        ag0_x(k).start()
    ag0_d.start()
    u0 = remote(eu_hbm, upanel.at[0, ublock], u_s.at[0], u_r.at[0], to_col)
    u0.start()

    early = EARLY * 4 * CHUNK
    parts = (pl.ds(0, early), pl.ds(early, items - early))

    def deg_d(k):
        return remote(csum.at[:, parts[k]], ccore.at[:, parts[k]], deg_s.at[k], deg_r.at[k], to_mate)

    def deg_x(k):
        return remote(cchip.at[:, parts[k]], cfar.at[:, parts[k]], deg_s.at[2 + k], deg_r.at[2 + k], to_far)

    def add_core(k):
        deg_d(k).wait()
        cchip[:, parts[k]] = csum[:, parts[k]] + ccore[:, parts[k]]
        deg_x(k).start()

    def col_factors(k):
        deg_x(k).wait()
        csum[:, parts[k]] = lax.rsqrt(jnp.maximum(cchip[:, parts[k]] + cfar[:, parts[k]], 1.0))

    lax.fori_loop(0, 4 * EARLY, mask_step, 0)
    deg_d(0).start()
    lax.fori_loop(4 * EARLY, 4 * EARLY + 4, mask_step, 0)
    add_core(0)
    ag0_x(2).start()
    ag0_x(3).start()
    lax.fori_loop(4 * EARLY + 4, n_mask, mask_step, 0)

    ones = jnp.ones((8, 128), BF16)
    rdeg[...] = lax.dot_general(ones, rsum[...].astype(BF16), (((1,), (1,)), ((), ())),
                                preferred_element_type=F32)[0:1, :]
    deg_y = remote(rdeg, rdfar, deg_s.at[4], deg_r.at[4], to_col)
    deg_y.start()
    deg_d(1).start()
    for copy in inputs:
        copy.wait()
    u0.wait_recv()
    col_factors(0)
    add_core(1)
    deg_y.wait()
    deg_u = jnp.maximum(rdeg[...] + rdfar[...], 1.0)
    rscale[...] = lax.rsqrt(jnp.broadcast_to(deg_u, (128, users)).T)

    def scale_block(owner, j):
        ci = csum[:, pl.ds(pl.multiple_of((j * 4 + owner) * CHUNK, CHUNK), CHUNK)]

        def tile(t, carry):
            rows = pl.ds(pl.multiple_of(t * SCALE_ROWS, SCALE_ROWS), SCALE_ROWS)
            ru = rscale[rows, :]
            for g in range(CHUNK // 128):
                sub = pl.ds(pl.multiple_of(owner * own_i + j * CHUNK + g * 128, 128), 128)
                m = adj[rows, sub].astype(F32)
                adj[rows, sub] = ((ru * m) * ci[:, g * 128:(g + 1) * 128]).astype(BF16)
            return carry

        lax.fori_loop(0, users // SCALE_ROWS, tile, 0)

    def item_part(owner, j, layer):
        return lax.dot_general(adj[:, rows_of(owner, j)], upanel[layer - 1], (((0,), (0,)), ((), ())),
                               preferred_element_type=F32)

    def core_copy(slot):
        rows = slot_rows(slot)
        return remote(stage.at[rows], drecv.at[rows], d_s.at[slot], d_r.at[slot], to_mate)

    def region(k, j):
        return pl.ds(pl.multiple_of(k * own_i + j * CHUNK, CHUNK), CHUNK)

    def near(j):
        return region(0, j)

    def arrived(j, layer):
        return region(1 + layer % 2, j)

    def xsend(j):
        return region(3, j)

    def chunk_rows(j):
        return pl.ds(pl.multiple_of(j * CHUNK, CHUNK), CHUNK)

    def slot_rows(slot, half=None):
        if half is None:
            return pl.ds(pl.multiple_of(slot * 2 * CHUNK, 2 * CHUNK), 2 * CHUNK)
        return pl.ds(pl.multiple_of(slot * 2 * CHUNK + half * CHUNK, CHUNK), CHUNK)

    def x_copy(j, layer):
        return remote(table.at[xsend(j)], table.at[arrived(j, layer)], x_s.at[j // GROUP], x_r.at[layer % 2, j], to_far)

    def x_sent(g):
        rows = pl.ds(pl.multiple_of(3 * own_i + g * GROUP * CHUNK, GROUP * CHUNK), GROUP * CHUNK)
        remote(table.at[rows], table.at[rows], x_s.at[g], x_r.at[0, 0], to_far).wait_send()

    def item_send_step(j, layer):
        slot = j % CORE_SLOTS
        if layer == 1:
            @pl.when(j >= CORE_SLOTS)
            def _():
                core_copy(slot).wait_send()
            scale_block(far_mate, j)
            scale_block(mate, j)
        else:
            core_copy(slot).wait_send()

            @pl.when(j % GROUP == 0)
            def _():
                x_sent(j // GROUP)
        stage[slot_rows(slot, 0), :] = item_part(far_mate, j, layer)
        stage[slot_rows(slot, 1), :] = item_part(mate, j, layer)
        core_copy(slot).start()
        if layer == 1:
            scale_block(far, j)
            scale_block(row, j)
        table[xsend(j), :] = item_part(far, j, layer)
        table[near(j), :] = item_part(row, j, layer)
        if layer > 1:
            @pl.when(j == 0)
            def _():
                add_mate(0, layer)

        @pl.when(j >= 2)
        def _():
            add_mate(j - 1, layer)

    def first_send_step():
        scale_block(far_mate, 0)
        scale_block(mate, 0)
        stage[slot_rows(0, 0), :] = item_part(far_mate, 0, 1)
        stage[slot_rows(0, 1), :] = item_part(mate, 0, 1)
        core_copy(0).start()
        scale_block(far, 0)
        table[xsend(0), :] = item_part(far, 0, 1)
        add_far(0, 1)
        scale_block(row, 0)
        table[near(0), :] = item_part(row, 0, 1)
        add_near(0)

    def add_mate(j, layer):
        add_far(j, layer)
        add_near(j)

    def add_far(j, layer):
        slot = j % CORE_SLOTS
        core_copy(slot).wait_recv()
        table[xsend(j), :] += drecv[slot_rows(slot, 0), :]
        x_copy(j, layer).start()

    def add_near(j):
        table[near(j), :] += drecv[slot_rows(j % CORE_SLOTS, 1), :]

    def ag_copy(kind, g, layer, whole=False):
        par = layer % 2
        rows = rows_of(far if kind == "fwd" else row, 0 if whole else g, own_i if whole else GROUP * CHUNK)
        piece = panel.at[par, rows]
        ssem, rsem, target = {"x": (agx_s, agx_r, to_far), "mate": (agd_s, agd_r, to_mate),
                              "fwd": (agf_s, agf_r, to_mate)}[kind]
        return remote(piece, piece, ssem.at[0], rsem.at[par, g], target)

    def fin_copy(kind, j):
        src, dst, k, target = {
            "col": (panel.at[1, rows_of(row, j)], panel.at[1, rows_of(far, j)], 0, to_col),
            "mate": (panel.at[1, rows_of(row, j)], panel.at[1, rows_of(row, j)], 1, to_mate),
            "fwd": (panel.at[1, rows_of(far, j)], panel.at[1, rows_of(far, j)], 2, to_mate)}[kind]
        return remote(src, dst, fin_s.at[k], fin_r.at[k, j], target)

    def out_copy(j):
        return pltpu.make_async_copy(panel.at[1, rows_of(row, j)], outi_ref.at[chunk_rows(j)], out_s.at[0])

    def fin_near(j):
        fin_copy("col", j).wait_recv()
        fin_copy("fwd", j).start()
        table[region(2, j), :] = panel[1, rows_of(far, j), :].astype(F32)
        fin_copy("mate", j).wait_recv()
        table[region(1, j), :] = panel[1, rows_of(mate, j), :].astype(F32)

    def fin_fwd(j):
        @pl.when(j % GROUP == 0)
        def _():
            x_sent(j // GROUP)

        fin_copy("fwd", j).wait_recv()
        table[region(3, j), :] = panel[1, rows_of(far_mate, j), :].astype(F32)

    def finish_item(j, layer):
        x_copy(j, layer).wait_recv()
        par = layer % 2
        value = (table[near(j), :] + table[arrived(j, layer), :]).astype(BF16)
        if layer < NUM_LAYERS:
            panel[par, rows_of(row, j), :] = value

            @pl.when(j % GROUP == GROUP - 1)
            def _():
                ag_copy("x", j // GROUP, layer).start()
                ag_copy("mate", j // GROUP, layer).start()
        else:
            total = ei_ref[chunk_rows(j), :].astype(F32) + panel[1, rows_of(row, j), :].astype(F32)
            total = total + panel[0, rows_of(row, j), :].astype(F32)
            total = total + value.astype(F32)
            final = (total / (NUM_LAYERS + 1)).astype(BF16)
            panel[1, rows_of(row, j), :] = final
            table[near(j), :] = final.astype(F32)
            fin_copy("col", j).start()
            fin_copy("mate", j).start()
            out_copy(j).start()

    def gather_items(layer):
        for g in range(n_chunk // GROUP):
            ag_copy("x", g, layer).wait_recv()
            ag_copy("fwd", g, layer).start()
        for g in range(n_chunk // GROUP):
            ag_copy("mate", g, layer).wait_recv()
            ag_copy("fwd", g, layer).wait_recv()
        for kind in ("x", "mate", "fwd"):
            ag_copy(kind, 0, layer, whole=True).wait_send()

    def user_part(layer):
        par = (layer - 1) % 2
        upart[...] = jnp.zeros_like(upart)

        def fold(i, carry):
            cols = pl.ds(pl.multiple_of(i * FOLD, FOLD), FOLD)
            upart[...] += jnp.dot(adj[:, cols], panel[par, cols, :], preferred_element_type=F32)
            return carry

        lax.fori_loop(0, items // FOLD, fold, 0)

    def yrows(layer):
        return pl.ds((layer - 1) * own_u, own_u)

    def y_copy(layer):
        return remote(upart.at[oblock], yflat.at[yrows(layer)], y_s.at[0], y_r.at[0], to_col)

    def u_copy(layer):
        return remote(upanel.at[layer, ublock], upanel.at[layer, ublock], u_s.at[0], u_r.at[0], to_col)

    def finish_user(layer):
        y_copy(layer).wait()
        value = (upart[ublock, :] + yflat[yrows(layer), :]).astype(BF16)
        if layer < NUM_LAYERS:
            upanel[layer, ublock, :] = value
            u_copy(layer).start()
        else:
            total = eu_ref[...].astype(F32) + upanel[1, ublock, :].astype(F32)
            total = total + upanel[2, ublock, :].astype(F32)
            total = total + value.astype(F32)
            final = (total / (NUM_LAYERS + 1)).astype(BF16)
            eu_ref[...] = final
            pltpu.make_async_copy(eu_ref, outu_ref, out_s.at[1]).start()
            stage[0:own_u, :] = final.astype(F32)
            fu_copy("col").start()
            fu_copy("mate").start()

    def fu_copy(kind):
        src, dst, k, target = {
            "col": (eu_ref, upanel.at[0, pl.ds(0, own_u)], 0, to_col),
            "mate": (eu_ref, upanel.at[0, pl.ds(own_u, own_u)], 1, to_mate),
            "fwd": (upanel.at[0, pl.ds(0, own_u)], upanel.at[1, oblock], 2, to_mate)}[kind]
        return remote(src, dst, fu_s.at[k], fu_r.at[k], target)

    def gather_users():
        fu_copy("col").wait_recv()
        fu_copy("fwd").start()
        stage[2 * own_u:3 * own_u, :] = upanel[0, 0:own_u, :].astype(F32)
        fu_copy("mate").wait_recv()
        stage[own_u:2 * own_u, :] = upanel[0, own_u:2 * own_u, :].astype(F32)
        fu_copy("fwd").wait_recv()
        stage[3 * own_u:4 * own_u, :] = upanel[1, oblock, :].astype(F32)

    def place_rows(piece):
        def side(r):
            return r // 2

        def step(t, carry):
            for k, owner in ((0, far), (1, row)):
                base = (owner * 2 + col) * share + t
                user = trip_ref[0, base]
                ur = lax.shift_right_logical(user, 10)
                uc = lax.bitwise_and(lax.shift_right_logical(user, 9), 1)
                pos = (jnp.where(uc == col, 0, 2) + jnp.where(ur == row, 0, 1)) * own_u + lax.bitwise_and(user, 511)
                pick_idx[k * 3 * share + t] = jnp.where(lax.shift_right_logical(ur, 1) == side(row), pos, 4 * own_u)
                for which in (1, 2):
                    item = trip_ref[which, base]
                    ic = lax.shift_right_logical(item, 14)
                    ir = lax.bitwise_and(lax.shift_right_logical(item, 12), 3)
                    pos = (jnp.where(ic == col, 0, 2) + jnp.where(ir == row, 0, 1)) * own_i + lax.bitwise_and(item, 4095)
                    pick_idx[(k * 3 + which) * share + t] = jnp.where(
                        lax.shift_right_logical(ir, 1) == side(row), pos, 4 * own_i)
            return carry

        lax.fori_loop(piece * (share // PIECES), (piece + 1) * (share // PIECES), step, 0)

    def pick(src, k, which, dst):
        def step(t, carry):
            for i in range(8):
                at = t * 8 + i
                dst[pl.ds(which * share + at, 1), :] = src[pl.ds(pick_idx[(k * 3 + which) * share + at], 1), :]
            return carry

        lax.fori_loop(0, share // 8, step, 0)

    def out_rows(at, size):
        return pl.ds(pl.multiple_of(far * own_i + at * share, share), size * share)

    def pick_copy(k):
        at, size = ((0, 2), (2, 1))[k]
        return remote(panel.at[0, out_rows(at, size)], pick_in.at[pl.ds(at * share, size * share)],
                      pick_s.at[k], pick_r.at[k], to_far)

    def thirds(k):
        return pl.ds(k * share, share)

    def swap_users():
        pick(stage, 0, 0, yflat)
        pick(stage, 1, 0, drecv)
        panel[0, out_rows(0, 1), :] = yflat[thirds(0), :].astype(BF16)
        panel[0, out_rows(1, 1), :] = drecv[thirds(0), :].astype(BF16)
        pick_copy(0).start()

    def mark_mixed():
        ids = trip_vec[1:3, pl.ds(pl.multiple_of((far * 2 + col) * share, share), share)]
        sides = lax.bitwise_and(lax.shift_right_logical(ids, 13), 1)
        flag = jnp.where(sides[0:1] == sides[1:2], 0.0, 1.0)
        mixed[...] = jnp.broadcast_to(flag, (128, share)).T

    def loop(lo, hi, body):
        def step(j, carry):
            body(j)
            return carry
        lax.fori_loop(lo, hi, step, 0)

    for layer in range(1, NUM_LAYERS + 1):
        if layer == 1:
            first_send_step()
            loop(1, EARLY, functools.partial(item_send_step, layer=layer))
            col_factors(1)
            remote(panel.at[0, far_block], panel.at[0, far_block], ag0_s.at[0], ag0_r.at[0], to_far).wait()
            ag0_f.start()
            loop(EARLY, n_chunk, functools.partial(item_send_step, layer=layer))
        else:
            loop(0, n_chunk, functools.partial(item_send_step, layer=layer))
        add_mate(n_chunk - 1, layer)
        if layer == 1:
            ag0_d.wait()
            ag0_f.wait()
            u0.wait_send()
        else:
            gather_items(layer - 1)
        finish = functools.partial(finish_item, layer=layer)
        if layer == 1:
            loop(0, n_chunk // 2, finish)
            user_part(layer)
            y_copy(layer).start()
            loop(n_chunk // 2, n_chunk, finish)
            loop(0, 4, place_rows)
            mark_mixed()
            finish_user(layer)
            u_copy(layer).wait()
        elif layer < NUM_LAYERS:
            user_part(layer)
            y_copy(layer).start()
            loop(0, n_chunk // 2, finish)
            finish_user(layer)
            loop(4, PIECES, place_rows)
            loop(n_chunk // 2, n_chunk, finish)
            u_copy(layer).wait()
        else:
            user_part(layer)
            y_copy(layer).start()

    for slot in range(CORE_SLOTS):
        core_copy(slot).wait_send()
    table[pl.ds(4 * own_i, 8), :] = jnp.zeros((8, 128), F32)
    stage[pl.ds(4 * own_u, 8), :] = jnp.zeros((8, 128), F32)

    def last_step(j):
        finish_item(j, NUM_LAYERS)

        @pl.when(j >= LAG)
        def _():
            fin_near(j - LAG)

        @pl.when(j >= LAG + 2)
        def _():
            fin_fwd(j - LAG - 2)

    loop(0, n_chunk // 2, last_step)
    finish_user(NUM_LAYERS)
    loop(n_chunk // 2, 3 * n_chunk // 4, last_step)
    gather_users()
    swap_users()
    loop(3 * n_chunk // 4, n_chunk, last_step)
    loop(n_chunk - LAG, n_chunk, fin_near)
    loop(n_chunk - LAG - 2, n_chunk, fin_fwd)
    pick(table, 0, 1, yflat)
    pick(table, 0, 2, yflat)
    diff = yflat[thirds(1), :] - yflat[thirds(2), :]
    panel[0, out_rows(2, 1), :] = jnp.where(mixed[...] > 0.5, diff, 0.0).astype(BF16)
    pick_copy(1).start()
    pick(table, 1, 1, drecv)
    pick(table, 1, 2, drecv)

    def score(user, items_diff):
        return jnp.sum((user * items_diff).T, axis=0, keepdims=True)

    n_dev = len(peers) + 1
    base = (emb * (n_dev // 2) + row * 2 + col) * 2 * share
    pick_copy(0).wait_recv()
    e_far = yflat[thirds(0), :] + pick_in[thirds(1), :].astype(F32)
    diff = jnp.where(mixed[...] > 0.5, 0.0, yflat[thirds(1), :] - yflat[thirds(2), :])
    dots[:, pl.ds(pl.multiple_of(base + share, share), share)] = score(e_far, diff)
    e_own = drecv[thirds(0), :] + pick_in[thirds(0), :].astype(F32)
    diff = drecv[thirds(1), :] - drecv[thirds(2), :]
    pick_copy(1).wait_recv()
    diff = diff + pick_in[thirds(2), :].astype(F32)
    dots[:, pl.ds(pl.multiple_of(base, share), share)] = score(e_own, diff)
    mine = pl.ds(pl.multiple_of(base, 2 * share), 2 * share)
    for target in peers:
        remote(dots.at[:, mine], dots.at[:, mine], loss_s.at[0], loss_r.at[0], target).start()

    for k in range(2):
        pick_copy(k).wait_send()
    for k, kind in enumerate(("col", "mate", "fwd")):
        fu_copy(kind).wait_send()
        remote(panel.at[1, block], panel.at[1, block], fin_s.at[k], fin_r.at[0, 0], to_mate).wait_send()
    pltpu.make_async_copy(panel.at[1, block], outi_ref, out_s.at[0]).wait()
    pltpu.make_async_copy(eu_ref, outu_ref, out_s.at[1]).wait()
    others = dots.at[:, pl.ds(0, len(peers) * 2 * share)]
    remote(others, others, loss_s.at[0], loss_r.at[0], to_far).wait()
    half = n_dev // 2
    for g in range(half):
        near_far = [[dots[:, ((e * half + owner) * 2 + k) * share:((e * half + owner) * 2 + k + 1) * share]
                     for k, owner in ((0, g), (1, (g + half // 2) % half))] for e in range(2)]
        z = -((near_far[0][0] + near_far[0][1]) + (near_far[1][0] + near_far[1][1]))
        loss_ref[:, g * share:(g + 1) * share] = jnp.maximum(z, 0.0) + jnp.log1p(jnp.exp(-jnp.abs(z)))


def hand_out_kernel(u_in, i_in, l_in, u_out, i_out, l_out, u_buf, i_buf, l_buf, in_s, out_s):
    pieces = [(u_in, u_buf, u_out), (l_in, l_buf, l_out)]
    rows = i_in.shape[0] // 4
    pieces += [tuple(ref.at[pl.ds(k * rows, rows)] for ref in (i_in, i_buf, i_out)) for k in range(4)]
    for k, (src, buf, dst) in enumerate(pieces):
        pltpu.make_async_copy(src, buf, in_s.at[k]).start()
    for k, (src, buf, dst) in enumerate(pieces):
        pltpu.make_async_copy(src, buf, in_s.at[k]).wait()
        pltpu.make_async_copy(buf, dst, out_s.at[k]).start()
    for k, (src, buf, dst) in enumerate(pieces):
        pltpu.make_async_copy(buf, dst, out_s.at[k]).wait()


def hand_out(*arrays):
    return pl.pallas_call(
        hand_out_kernel,
        name="hand_out",
        out_shape=tuple(jax.ShapeDtypeStruct(a.shape, a.dtype) for a in arrays),
        in_specs=[pl.BlockSpec(memory_space=pl.ANY)] * 3,
        out_specs=(pl.BlockSpec(memory_space=pl.ANY),) * 3,
        scratch_shapes=[*(pltpu.VMEM(a.shape, a.dtype) for a in arrays),
                        pltpu.SemaphoreType.DMA((6,)), pltpu.SemaphoreType.DMA((6,))],
    )(*arrays)


def propagate(mask_blk, user_sh, item_sh, triples):
    users, items = mask_blk.shape
    own_u, dim = user_sh.shape
    own_i = item_sh.shape[0]
    n_chunk = own_i // CHUNK
    num_trip = triples.shape[0]
    share = num_trip // 8
    n_group = n_chunk // GROUP
    vmem, dma = pltpu.VMEM, pltpu.SemaphoreType.DMA
    return pl.pallas_call(
        prop_kernel,
        name="propagate",
        out_shape=(jax.ShapeDtypeStruct((own_u, dim), BF16), jax.ShapeDtypeStruct((own_i, dim), BF16),
                   jax.ShapeDtypeStruct((1, num_trip), F32)),
        in_specs=[pl.BlockSpec(memory_space=pl.ANY)] * 4,
        out_specs=(pl.BlockSpec(memory_space=pl.ANY), pl.BlockSpec(memory_space=pl.ANY),
                   pl.BlockSpec(memory_space=pltpu.VMEM)),
        scratch_shapes=[
            vmem((users, items), BF16),
            vmem((MASK_SLOTS, users, CHUNK), jnp.int32),
            vmem((2, items, dim), BF16),
            vmem((4 * own_i + 8, dim), F32),
            vmem((CORE_SLOTS * 2 * CHUNK + 8, dim), F32),
            vmem((CORE_SLOTS * 2 * CHUNK, dim), F32),
            vmem((3, users, dim), BF16),
            vmem((users, dim), F32),
            vmem((3 * own_u, dim), F32),
            vmem((own_u, dim), BF16),
            vmem((own_i, dim), BF16),
            pltpu.SMEM((3, num_trip), jnp.int32),
            vmem((3, num_trip), jnp.int32),
            vmem((1, items), F32),
            vmem((1, items), F32),
            vmem((1, items), F32),
            vmem((1, items), F32),
            vmem((1, users), F32),
            vmem((1, users), F32),
            pltpu.SMEM((6 * share,), jnp.int32),
            vmem((3 * share, dim), BF16),
            vmem((share, 128), F32),
            vmem((1, 4 * num_trip), F32),
            dma((6,)), dma((MASK_SLOTS,)),
            dma((3,)), dma((3,)),
            dma((5,)), dma((5,)),
            dma((1,)), dma((1,)),
            dma((1,)), dma((1,)),
            dma((CORE_SLOTS,)), dma((CORE_SLOTS,)),
            dma((n_group,)), dma((2, n_chunk)),
            dma((1,)), dma((2, n_group)),
            dma((1,)), dma((2, n_group)),
            dma((1,)), dma((2, n_group)),
            dma((3,)), dma((3, n_chunk)),
            dma((3,)), dma((3,)),
            dma((2,)), dma((2,)),
            dma((2,)),
            dma((1,)), dma((1,)),
        ],
        compiler_params=pltpu.CompilerParams(collective_id=0, has_side_effects=True,
                                             vmem_limit_bytes=67_043_328),
    )(mask_blk, user_sh, item_sh, triples.T)


def solution(mesh):
    def local_fn(mask_blk, user_sh, item_sh, triples):
        final_user, final_item, loss = hand_out(*propagate(mask_blk, user_sh, item_sh, triples))
        return final_user, final_item, loss.reshape(-1)

    return jax.shard_map(
        local_fn, mesh=mesh,
        in_specs=(P("row", "col"), P(("row", "col"), "emb"), P(("col", "row"), "emb"), P()),
        out_specs=(P(("row", "col"), "emb"), P(("col", "row"), "emb"), P()),
        check_vma=False)
```

```python
import functools

import jax
import jax.numpy as jnp
from jax import lax
from jax.experimental import pallas as pl
from jax.experimental.pallas import tpu as pltpu
from jax.sharding import PartitionSpec as P

NUM_LAYERS = 3
F32 = jnp.float32
BF16 = jnp.bfloat16
MESH = pl.DeviceIdType.MESH

CHUNK = 256
MASK_SLOTS = 7
GROUP = 4
EARLY = 8
PIECES = 16
CORE_SLOTS = 4
SCALE_ROWS = 256
LAG = 3
FOLD = 2048


def prop_kernel(mask_hbm, eu_hbm, ei_hbm, trip_hbm, outu_ref, outi_ref, loss_ref,
                adj, mbuf, panel, table, stage, drecv, upanel, upart, yflat, eu_ref, ei_ref, trip_ref, trip_vec,
                csum, ccore, cchip, cfar, rdeg, rdfar, pick_idx, pick_in, mixed, dots,
                in_s, msem, ag0_s, ag0_r, deg_s, deg_r, u_s, u_r, y_s, y_r,
                d_s, d_r, x_s, x_r, agx_s, agx_r, agd_s, agd_r, agf_s, agf_r,
                fin_s, fin_r, fu_s, fu_r, pick_s, pick_r, out_s, loss_s, loss_r):
    users, items = adj.shape
    rsum = rscale = upart
    own_u = eu_ref.shape[0]
    own_i = ei_ref.shape[0]
    n_chunk = own_i // CHUNK
    row = lax.axis_index("row")
    col = lax.axis_index("col")
    mate = row + 1 - 2 * (row % 2)
    far = (row + 2) % 4
    far_mate = (mate + 2) % 4
    other_col = 1 - col
    to_mate = {"row": mate}
    to_far = {"row": far}
    to_col = {"col": other_col}
    emb = lax.axis_index("emb")
    peers = [{"emb": (emb + de) % 2, "row": (row + dr) % 4, "col": (col + dc) % 2}
             for de in range(2) for dr in range(4) for dc in range(2)][1:]
    share = loss_ref.shape[1] // 8

    def remote(src, dst, ssem, rsem, target):
        return pltpu.make_async_remote_copy(src_ref=src, dst_ref=dst, send_sem=ssem, recv_sem=rsem,
                                            device_id=target, device_id_type=MESH)

    def rows_of(owner, j, size=CHUNK):
        return pl.ds(pl.multiple_of(owner * own_i + j * size, size), size)

    block = pl.ds(pl.multiple_of(row * own_i, own_i), own_i)
    far_block = pl.ds(pl.multiple_of(far * own_i, own_i), own_i)
    ublock = pl.ds(pl.multiple_of(col * own_u, own_u), own_u)
    oblock = pl.ds(pl.multiple_of(other_col * own_u, own_u), own_u)
    n_mask = items // CHUNK

    def mask_copy(i):
        slot = i % MASK_SLOTS
        return pltpu.make_async_copy(mask_hbm.at[:, rows_of(i % 4, i // 4)], mbuf.at[slot], msem.at[slot])

    for i in range(MASK_SLOTS - 1):
        mask_copy(i).start()
    inputs = [pltpu.make_async_copy(src, dst, in_s.at[k]) for k, (src, dst) in enumerate((
        (eu_hbm, upanel.at[0, ublock]), (ei_hbm, panel.at[0, block]), (eu_hbm, eu_ref), (ei_hbm, ei_ref),
        (trip_hbm, trip_ref), (trip_hbm, trip_vec)))]
    for copy in inputs:
        copy.start()

    barrier = pltpu.get_barrier_semaphore()
    for target in peers:
        pl.semaphore_signal(barrier, inc=1, device_id=target, device_id_type=MESH)

    rsum[...] = jnp.zeros_like(rsum)

    def mask_step(i, carry):
        mask_copy(i).wait()

        @pl.when(i + MASK_SLOTS - 1 < n_mask)
        def _():
            mask_copy(i + MASK_SLOTS - 1).start()

        cols = rows_of(i % 4, i // 4)
        slot = i % MASK_SLOTS

        def tile(t, acc):
            rows = pl.ds(pl.multiple_of(t * 64, 64), 64)
            m = mbuf[slot, rows, :].astype(F32)
            adj[rows, cols] = m.astype(BF16)
            part = m[:, 0:128]
            for g in range(1, CHUNK // 128):
                part = part + m[:, g * 128:(g + 1) * 128]
            rsum[rows, :] += part
            return acc + jnp.sum(m.reshape(8, 8, CHUNK), axis=0)

        acc = lax.fori_loop(0, users // 64, tile, jnp.zeros((8, CHUNK), F32))
        csum[:, pl.ds(pl.multiple_of(i * CHUNK, CHUNK), CHUNK)] = jnp.sum(acc, axis=0, keepdims=True)
        return carry

    pl.semaphore_wait(barrier, len(peers))

    quarter = own_i // 4

    def ag0_x(k):
        return remote(ei_hbm.at[pl.ds(k * quarter, quarter)],
                      panel.at[0, pl.ds(pl.multiple_of(row * own_i + k * quarter, quarter), quarter)],
                      ag0_s.at[0], ag0_r.at[0], to_far)

    ag0_d = remote(ei_hbm, panel.at[0, block], ag0_s.at[1], ag0_r.at[1], to_mate)
    ag0_f = remote(panel.at[0, far_block], panel.at[0, far_block], ag0_s.at[2], ag0_r.at[2], to_mate)
    for k in range(2):
        ag0_x(k).start()
    ag0_d.start()
    u0 = remote(eu_hbm, upanel.at[0, ublock], u_s.at[0], u_r.at[0], to_col)
    u0.start()

    early = EARLY * 4 * CHUNK
    parts = (pl.ds(0, early), pl.ds(early, items - early))

    def deg_d(k):
        return remote(csum.at[:, parts[k]], ccore.at[:, parts[k]], deg_s.at[k], deg_r.at[k], to_mate)

    def deg_x(k):
        return remote(cchip.at[:, parts[k]], cfar.at[:, parts[k]], deg_s.at[2 + k], deg_r.at[2 + k], to_far)

    def add_core(k):
        deg_d(k).wait()
        cchip[:, parts[k]] = csum[:, parts[k]] + ccore[:, parts[k]]
        deg_x(k).start()

    def col_factors(k):
        deg_x(k).wait()
        csum[:, parts[k]] = lax.rsqrt(jnp.maximum(cchip[:, parts[k]] + cfar[:, parts[k]], 1.0))

    lax.fori_loop(0, 4 * EARLY, mask_step, 0)
    deg_d(0).start()
    lax.fori_loop(4 * EARLY, 4 * EARLY + 4, mask_step, 0)
    add_core(0)
    ag0_x(2).start()
    ag0_x(3).start()
    lax.fori_loop(4 * EARLY + 4, n_mask, mask_step, 0)

    ones = jnp.ones((8, 128), BF16)
    rdeg[...] = lax.dot_general(ones, rsum[...].astype(BF16), (((1,), (1,)), ((), ())),
                                preferred_element_type=F32)[0:1, :]
    deg_y = remote(rdeg, rdfar, deg_s.at[4], deg_r.at[4], to_col)
    deg_y.start()
    deg_d(1).start()
    for copy in inputs:
        copy.wait()
    u0.wait_recv()
    col_factors(0)
    add_core(1)
    deg_y.wait()
    deg_u = jnp.maximum(rdeg[...] + rdfar[...], 1.0)
    rscale[...] = lax.rsqrt(jnp.broadcast_to(deg_u, (128, users)).T)

    def scale_block(owner, j):
        ci = csum[:, pl.ds(pl.multiple_of((j * 4 + owner) * CHUNK, CHUNK), CHUNK)]

        def tile(t, carry):
            rows = pl.ds(pl.multiple_of(t * SCALE_ROWS, SCALE_ROWS), SCALE_ROWS)
            ru = rscale[rows, :]
            for g in range(CHUNK // 128):
                sub = pl.ds(pl.multiple_of(owner * own_i + j * CHUNK + g * 128, 128), 128)
                m = adj[rows, sub].astype(F32)
                adj[rows, sub] = ((ru * m) * ci[:, g * 128:(g + 1) * 128]).astype(BF16)
            return carry

        lax.fori_loop(0, users // SCALE_ROWS, tile, 0)

    def item_part(owner, j, layer):
        return lax.dot_general(adj[:, rows_of(owner, j)], upanel[layer - 1], (((0,), (0,)), ((), ())),
                               preferred_element_type=F32)

    def core_copy(slot, half=None):
        rows = slot_rows(slot, half)
        return remote(stage.at[rows], drecv.at[rows], d_s.at[slot], d_r.at[slot], to_mate)

    def region(k, j):
        return pl.ds(pl.multiple_of(k * own_i + j * CHUNK, CHUNK), CHUNK)

    def near(j):
        return region(0, j)

    def arrived(j, layer):
        return region(1 + layer % 2, j)

    def xsend(j):
        return region(3, j)

    def chunk_rows(j):
        return pl.ds(pl.multiple_of(j * CHUNK, CHUNK), CHUNK)

    def slot_rows(slot, half=None):
        if half is None:
            return pl.ds(pl.multiple_of(slot * 2 * CHUNK, 2 * CHUNK), 2 * CHUNK)
        return pl.ds(pl.multiple_of(slot * 2 * CHUNK + half * CHUNK, CHUNK), CHUNK)

    def x_copy(j, layer):
        return remote(table.at[xsend(j)], table.at[arrived(j, layer)], x_s.at[j // GROUP], x_r.at[layer % 2, j], to_far)

    def x_sent(g):
        rows = pl.ds(pl.multiple_of(3 * own_i + g * GROUP * CHUNK, GROUP * CHUNK), GROUP * CHUNK)
        remote(table.at[rows], table.at[rows], x_s.at[g], x_r.at[0, 0], to_far).wait_send()

    def item_send_step(j, layer):
        slot = j % CORE_SLOTS
        if layer == 2:
            pl.when(j >= CORE_SLOTS)(core_copy(slot).wait_send)
        else:
            core_copy(slot).wait_send()

        @pl.when(j % GROUP == 0)
        def _():
            x_sent(j // GROUP)

        stage[slot_rows(slot, 0), :] = item_part(far_mate, j, layer)
        stage[slot_rows(slot, 1), :] = item_part(mate, j, layer)
        core_copy(slot).start()
        table[xsend(j), :] = item_part(far, j, layer)
        table[near(j), :] = item_part(row, j, layer)

        @pl.when(j == 0)
        def _():
            add_mate(0, layer)

        @pl.when(j >= 2)
        def _():
            add_mate(j - 1, layer)

    def add_mate(j, layer):
        slot = j % CORE_SLOTS
        core_copy(slot).wait_recv()
        table[xsend(j), :] += drecv[slot_rows(slot, 0), :]
        table[near(j), :] += drecv[slot_rows(slot, 1), :]
        x_copy(j, layer).start()

    def layer1_step(j, to_far_chip):
        slot = j % CORE_SLOTS
        theirs, ours, here = (far_mate, far, xsend) if to_far_chip else (mate, row, near)
        if to_far_chip:
            pl.when(j >= CORE_SLOTS)(core_copy(slot, 0).wait_send)
        else:
            core_copy(slot, 0).wait_send()
        scale_block(theirs, j)
        scale_block(ours, j)
        stage[slot_rows(slot, 0), :] = item_part(theirs, j, 1)
        table[here(j), :] = item_part(ours, j, 1)
        core_copy(slot, 0).start()
        if not to_far_chip:
            @pl.when(j == 0)
            def _():
                layer1_add(0, to_far_chip)

        @pl.when(j >= 2)
        def _():
            layer1_add(j - 1, to_far_chip)

    def layer1_first():
        scale_block(far_mate, 0)
        stage[slot_rows(0, 0), :] = item_part(far_mate, 0, 1)
        core_copy(0, 0).start()
        scale_block(far, 0)
        table[xsend(0), :] = item_part(far, 0, 1)
        layer1_add(0, True)

    def layer1_add(j, to_far_chip):
        slot = j % CORE_SLOTS
        here = xsend if to_far_chip else near
        core_copy(slot, 0).wait_recv()
        table[here(j), :] += drecv[slot_rows(slot, 0), :]
        if to_far_chip:
            x_copy(j, 1).start()

    def ag_copy(kind, g, layer, whole=False):
        par = layer % 2
        rows = rows_of(far if kind == "fwd" else row, 0 if whole else g, own_i if whole else GROUP * CHUNK)
        piece = panel.at[par, rows]
        ssem, rsem, target = {"x": (agx_s, agx_r, to_far), "mate": (agd_s, agd_r, to_mate),
                              "fwd": (agf_s, agf_r, to_mate)}[kind]
        return remote(piece, piece, ssem.at[0], rsem.at[par, g], target)

    def fin_copy(kind, j):
        src, dst, k, target = {
            "col": (panel.at[1, rows_of(row, j)], panel.at[1, rows_of(far, j)], 0, to_col),
            "mate": (panel.at[1, rows_of(row, j)], panel.at[1, rows_of(row, j)], 1, to_mate),
            "fwd": (panel.at[1, rows_of(far, j)], panel.at[1, rows_of(far, j)], 2, to_mate)}[kind]
        return remote(src, dst, fin_s.at[k], fin_r.at[k, j], target)

    def out_copy(j):
        return pltpu.make_async_copy(panel.at[1, rows_of(row, j)], outi_ref.at[chunk_rows(j)], out_s.at[0])

    def fin_near(j):
        fin_copy("col", j).wait_recv()
        fin_copy("fwd", j).start()
        table[region(2, j), :] = panel[1, rows_of(far, j), :].astype(F32)
        fin_copy("mate", j).wait_recv()
        table[region(1, j), :] = panel[1, rows_of(mate, j), :].astype(F32)

    def fin_fwd(j):
        @pl.when(j % GROUP == 0)
        def _():
            x_sent(j // GROUP)

        fin_copy("fwd", j).wait_recv()
        table[region(3, j), :] = panel[1, rows_of(far_mate, j), :].astype(F32)

    def finish_item(j, layer):
        x_copy(j, layer).wait_recv()
        par = layer % 2
        value = (table[near(j), :] + table[arrived(j, layer), :]).astype(BF16)
        if layer < NUM_LAYERS:
            panel[par, rows_of(row, j), :] = value

            @pl.when(j % GROUP == GROUP - 1)
            def _():
                ag_copy("x", j // GROUP, layer).start()
                ag_copy("mate", j // GROUP, layer).start()
        else:
            total = ei_ref[chunk_rows(j), :].astype(F32) + panel[1, rows_of(row, j), :].astype(F32)
            total = total + panel[0, rows_of(row, j), :].astype(F32)
            total = total + value.astype(F32)
            final = (total / (NUM_LAYERS + 1)).astype(BF16)
            panel[1, rows_of(row, j), :] = final
            table[near(j), :] = final.astype(F32)
            fin_copy("col", j).start()
            fin_copy("mate", j).start()
            out_copy(j).start()

    def gather_items(layer):
        for g in range(n_chunk // GROUP):
            ag_copy("x", g, layer).wait_recv()
            ag_copy("fwd", g, layer).start()
        for g in range(n_chunk // GROUP):
            ag_copy("mate", g, layer).wait_recv()
            ag_copy("fwd", g, layer).wait_recv()
        for kind in ("x", "mate", "fwd"):
            ag_copy(kind, 0, layer, whole=True).wait_send()

    def user_part(layer):
        par = (layer - 1) % 2
        upart[...] = jnp.zeros_like(upart)

        def fold(i, carry):
            cols = pl.ds(pl.multiple_of(i * FOLD, FOLD), FOLD)
            upart[...] += jnp.dot(adj[:, cols], panel[par, cols, :], preferred_element_type=F32)
            return carry

        lax.fori_loop(0, items // FOLD, fold, 0)

    def yrows(layer):
        return pl.ds((layer - 1) * own_u, own_u)

    def y_copy(layer):
        return remote(upart.at[oblock], yflat.at[yrows(layer)], y_s.at[0], y_r.at[0], to_col)

    def u_copy(layer):
        return remote(upanel.at[layer, ublock], upanel.at[layer, ublock], u_s.at[0], u_r.at[0], to_col)

    def finish_user(layer):
        y_copy(layer).wait()
        value = (upart[ublock, :] + yflat[yrows(layer), :]).astype(BF16)
        if layer < NUM_LAYERS:
            upanel[layer, ublock, :] = value
            u_copy(layer).start()
        else:
            total = eu_ref[...].astype(F32) + upanel[1, ublock, :].astype(F32)
            total = total + upanel[2, ublock, :].astype(F32)
            total = total + value.astype(F32)
            final = (total / (NUM_LAYERS + 1)).astype(BF16)
            eu_ref[...] = final
            pltpu.make_async_copy(eu_ref, outu_ref, out_s.at[1]).start()
            stage[0:own_u, :] = final.astype(F32)
            fu_copy("col").start()
            fu_copy("mate").start()

    def fu_copy(kind):
        src, dst, k, target = {
            "col": (eu_ref, upanel.at[0, pl.ds(0, own_u)], 0, to_col),
            "mate": (eu_ref, upanel.at[0, pl.ds(own_u, own_u)], 1, to_mate),
            "fwd": (upanel.at[0, pl.ds(0, own_u)], upanel.at[1, oblock], 2, to_mate)}[kind]
        return remote(src, dst, fu_s.at[k], fu_r.at[k], target)

    def gather_users():
        fu_copy("col").wait_recv()
        fu_copy("fwd").start()
        stage[2 * own_u:3 * own_u, :] = upanel[0, 0:own_u, :].astype(F32)
        fu_copy("mate").wait_recv()
        stage[own_u:2 * own_u, :] = upanel[0, own_u:2 * own_u, :].astype(F32)
        fu_copy("fwd").wait_recv()
        stage[3 * own_u:4 * own_u, :] = upanel[1, oblock, :].astype(F32)

    def place_rows(piece):
        def side(r):
            return r // 2

        def step(t, carry):
            for k, owner in ((0, far), (1, row)):
                base = (owner * 2 + col) * share + t
                user = trip_ref[0, base]
                ur = lax.shift_right_logical(user, 10)
                uc = lax.bitwise_and(lax.shift_right_logical(user, 9), 1)
                pos = (jnp.where(uc == col, 0, 2) + jnp.where(ur == row, 0, 1)) * own_u + lax.bitwise_and(user, 511)
                pick_idx[k * 3 * share + t] = jnp.where(lax.shift_right_logical(ur, 1) == side(row), pos, 4 * own_u)
                for which in (1, 2):
                    item = trip_ref[which, base]
                    ic = lax.shift_right_logical(item, 14)
                    ir = lax.bitwise_and(lax.shift_right_logical(item, 12), 3)
                    pos = (jnp.where(ic == col, 0, 2) + jnp.where(ir == row, 0, 1)) * own_i + lax.bitwise_and(item, 4095)
                    pick_idx[(k * 3 + which) * share + t] = jnp.where(
                        lax.shift_right_logical(ir, 1) == side(row), pos, 4 * own_i)
            return carry

        lax.fori_loop(piece * (share // PIECES), (piece + 1) * (share // PIECES), step, 0)

    def pick(src, k, which, dst, lo=0, hi=None):
        def step(t, carry):
            for i in range(8):
                at = t * 8 + i
                dst[pl.ds(which * share + at, 1), :] = src[pl.ds(pick_idx[(k * 3 + which) * share + at], 1), :]
            return carry

        lax.fori_loop(lo // 8, (hi or share) // 8, step, 0)

    def out_rows(lo, size):
        return pl.ds(pl.multiple_of(far * own_i + lo, size), size)

    def pick_copy(k):
        lo, size = ((0, 2 * share), (2 * share, share // 2), (5 * share // 2, share // 2))[k]
        return remote(panel.at[0, out_rows(lo, size)], pick_in.at[pl.ds(lo, size)],
                      pick_s.at[k], pick_r.at[k], to_far)

    def thirds(k):
        return pl.ds(k * share, share)

    def swap_users():
        pick(stage, 0, 0, yflat)
        pick(stage, 1, 0, drecv)
        panel[0, out_rows(0, share), :] = yflat[thirds(0), :].astype(BF16)
        panel[0, out_rows(share, share), :] = drecv[thirds(0), :].astype(BF16)
        pick_copy(0).start()

    def mark_mixed():
        ids = trip_vec[1:3, pl.ds(pl.multiple_of((far * 2 + col) * share, share), share)]
        sides = lax.bitwise_and(lax.shift_right_logical(ids, 13), 1)
        flag = jnp.where(sides[0:1] == sides[1:2], 0.0, 1.0)
        mixed[...] = jnp.broadcast_to(flag, (128, share)).T

    def loop(lo, hi, body):
        def step(j, carry):
            body(j)
            return carry
        lax.fori_loop(lo, hi, step, 0)

    for layer in range(1, NUM_LAYERS + 1):
        if layer == 1:
            send_far = functools.partial(layer1_step, to_far_chip=True)
            send_near = functools.partial(layer1_step, to_far_chip=False)
            layer1_first()
            loop(1, EARLY, send_far)
            col_factors(1)
            remote(panel.at[0, far_block], panel.at[0, far_block], ag0_s.at[0], ag0_r.at[0], to_far).wait()
            ag0_f.start()
            loop(EARLY, n_chunk, send_far)
            layer1_add(n_chunk - 1, True)
            loop(0, n_chunk, send_near)
            layer1_add(n_chunk - 1, False)
            for slot in range(CORE_SLOTS):
                core_copy(slot, 0).wait_send()
        else:
            loop(0, n_chunk, functools.partial(item_send_step, layer=layer))
            add_mate(n_chunk - 1, layer)
        if layer == 1:
            ag0_d.wait()
            ag0_f.wait()
            u0.wait_send()
        else:
            gather_items(layer - 1)
        finish = functools.partial(finish_item, layer=layer)
        if layer == 1:
            loop(0, n_chunk // 2, finish)
            user_part(layer)
            y_copy(layer).start()
            loop(n_chunk // 2, n_chunk, finish)
            loop(0, 4, place_rows)
            mark_mixed()
            finish_user(layer)
            u_copy(layer).wait()
        elif layer < NUM_LAYERS:
            user_part(layer)
            y_copy(layer).start()
            loop(0, n_chunk // 2, finish)
            finish_user(layer)
            loop(4, PIECES, place_rows)
            loop(n_chunk // 2, n_chunk, finish)
            u_copy(layer).wait()
        else:
            user_part(layer)
            y_copy(layer).start()

    for slot in range(CORE_SLOTS):
        core_copy(slot).wait_send()
    table[pl.ds(4 * own_i, 8), :] = jnp.zeros((8, 128), F32)
    stage[pl.ds(4 * own_u, 8), :] = jnp.zeros((8, 128), F32)

    def last_step(j):
        finish_item(j, NUM_LAYERS)

        @pl.when(j >= LAG)
        def _():
            fin_near(j - LAG)

        @pl.when(j >= LAG + 2)
        def _():
            fin_fwd(j - LAG - 2)

    loop(0, n_chunk // 2, last_step)
    finish_user(NUM_LAYERS)
    loop(n_chunk // 2, 3 * n_chunk // 4, last_step)
    gather_users()
    swap_users()
    loop(3 * n_chunk // 4, n_chunk, last_step)
    loop(n_chunk - LAG, n_chunk, fin_near)
    loop(n_chunk - LAG - 2, n_chunk, fin_fwd)
    for k in (1, 2):
        lo, hi = (k - 1) * share // 2, k * share // 2
        pick(table, 0, 1, yflat, lo, hi)
        pick(table, 0, 2, yflat, lo, hi)
        diff = yflat[share + lo:share + hi, :] - yflat[2 * share + lo:2 * share + hi, :]
        panel[0, out_rows(2 * share + lo, share // 2), :] = jnp.where(mixed[lo:hi, :] > 0.5, diff, 0.0).astype(BF16)
        pick_copy(k).start()
    pick(table, 1, 1, drecv)
    pick(table, 1, 2, drecv)

    def score(user, items_diff):
        return jnp.sum((user * items_diff).T, axis=0, keepdims=True)

    n_dev = len(peers) + 1
    base = (emb * (n_dev // 2) + row * 2 + col) * 2 * share
    pick_copy(0).wait_recv()
    e_far = yflat[thirds(0), :] + pick_in[thirds(1), :].astype(F32)
    diff = jnp.where(mixed[...] > 0.5, 0.0, yflat[thirds(1), :] - yflat[thirds(2), :])
    dots[:, pl.ds(pl.multiple_of(base + share, share), share)] = score(e_far, diff)
    e_own = drecv[thirds(0), :] + pick_in[thirds(0), :].astype(F32)
    diff = drecv[thirds(1), :] - drecv[thirds(2), :]
    pick_copy(1).wait_recv()
    pick_copy(2).wait_recv()
    diff = diff + pick_in[thirds(2), :].astype(F32)
    dots[:, pl.ds(pl.multiple_of(base, share), share)] = score(e_own, diff)
    mine = pl.ds(pl.multiple_of(base, 2 * share), 2 * share)
    for target in peers:
        remote(dots.at[:, mine], dots.at[:, mine], loss_s.at[0], loss_r.at[0], target).start()

    for k in range(3):
        pick_copy(k).wait_send()
    for k, kind in enumerate(("col", "mate", "fwd")):
        fu_copy(kind).wait_send()
        remote(panel.at[1, block], panel.at[1, block], fin_s.at[k], fin_r.at[0, 0], to_mate).wait_send()
    pltpu.make_async_copy(panel.at[1, block], outi_ref, out_s.at[0]).wait()
    pltpu.make_async_copy(eu_ref, outu_ref, out_s.at[1]).wait()
    others = dots.at[:, pl.ds(0, len(peers) * 2 * share)]
    remote(others, others, loss_s.at[0], loss_r.at[0], to_far).wait()
    half = n_dev // 2
    for g in range(half):
        near_far = [[dots[:, ((e * half + owner) * 2 + k) * share:((e * half + owner) * 2 + k + 1) * share]
                     for k, owner in ((0, g), (1, (g + half // 2) % half))] for e in range(2)]
        z = -((near_far[0][0] + near_far[0][1]) + (near_far[1][0] + near_far[1][1]))
        loss_ref[:, g * share:(g + 1) * share] = jnp.maximum(z, 0.0) + jnp.log1p(jnp.exp(-jnp.abs(z)))


def hand_out_kernel(u_in, i_in, l_in, u_out, i_out, l_out, u_buf, i_buf, l_buf, in_s, out_s):
    pieces = [(u_in, u_buf, u_out), (l_in, l_buf, l_out)]
    rows = i_in.shape[0] // 4
    pieces += [tuple(ref.at[pl.ds(k * rows, rows)] for ref in (i_in, i_buf, i_out)) for k in range(4)]
    for k, (src, buf, dst) in enumerate(pieces):
        pltpu.make_async_copy(src, buf, in_s.at[k]).start()
    for k, (src, buf, dst) in enumerate(pieces):
        pltpu.make_async_copy(src, buf, in_s.at[k]).wait()
        pltpu.make_async_copy(buf, dst, out_s.at[k]).start()
    for k, (src, buf, dst) in enumerate(pieces):
        pltpu.make_async_copy(buf, dst, out_s.at[k]).wait()


def hand_out(*arrays):
    return pl.pallas_call(
        hand_out_kernel,
        name="hand_out",
        out_shape=tuple(jax.ShapeDtypeStruct(a.shape, a.dtype) for a in arrays),
        in_specs=[pl.BlockSpec(memory_space=pl.ANY)] * 3,
        out_specs=(pl.BlockSpec(memory_space=pl.ANY),) * 3,
        scratch_shapes=[*(pltpu.VMEM(a.shape, a.dtype) for a in arrays),
                        pltpu.SemaphoreType.DMA((6,)), pltpu.SemaphoreType.DMA((6,))],
    )(*arrays)


def propagate(mask_blk, user_sh, item_sh, triples):
    users, items = mask_blk.shape
    own_u, dim = user_sh.shape
    own_i = item_sh.shape[0]
    n_chunk = own_i // CHUNK
    num_trip = triples.shape[0]
    share = num_trip // 8
    n_group = n_chunk // GROUP
    vmem, dma = pltpu.VMEM, pltpu.SemaphoreType.DMA
    return pl.pallas_call(
        prop_kernel,
        name="propagate",
        out_shape=(jax.ShapeDtypeStruct((own_u, dim), BF16), jax.ShapeDtypeStruct((own_i, dim), BF16),
                   jax.ShapeDtypeStruct((1, num_trip), F32)),
        in_specs=[pl.BlockSpec(memory_space=pl.ANY)] * 4,
        out_specs=(pl.BlockSpec(memory_space=pl.ANY), pl.BlockSpec(memory_space=pl.ANY),
                   pl.BlockSpec(memory_space=pltpu.VMEM)),
        scratch_shapes=[
            vmem((users, items), BF16),
            vmem((MASK_SLOTS, users, CHUNK), jnp.int32),
            vmem((2, items, dim), BF16),
            vmem((4 * own_i + 8, dim), F32),
            vmem((CORE_SLOTS * 2 * CHUNK + 8, dim), F32),
            vmem((CORE_SLOTS * 2 * CHUNK, dim), F32),
            vmem((3, users, dim), BF16),
            vmem((users, dim), F32),
            vmem((3 * own_u, dim), F32),
            vmem((own_u, dim), BF16),
            vmem((own_i, dim), BF16),
            pltpu.SMEM((3, num_trip), jnp.int32),
            vmem((3, num_trip), jnp.int32),
            vmem((1, items), F32),
            vmem((1, items), F32),
            vmem((1, items), F32),
            vmem((1, items), F32),
            vmem((1, users), F32),
            vmem((1, users), F32),
            pltpu.SMEM((6 * share,), jnp.int32),
            vmem((3 * share, dim), BF16),
            vmem((share, 128), F32),
            vmem((1, 4 * num_trip), F32),
            dma((6,)), dma((MASK_SLOTS,)),
            dma((3,)), dma((3,)),
            dma((5,)), dma((5,)),
            dma((1,)), dma((1,)),
            dma((1,)), dma((1,)),
            dma((CORE_SLOTS,)), dma((CORE_SLOTS,)),
            dma((n_group,)), dma((2, n_chunk)),
            dma((1,)), dma((2, n_group)),
            dma((1,)), dma((2, n_group)),
            dma((1,)), dma((2, n_group)),
            dma((3,)), dma((3, n_chunk)),
            dma((3,)), dma((3,)),
            dma((3,)), dma((3,)),
            dma((2,)),
            dma((1,)), dma((1,)),
        ],
        compiler_params=pltpu.CompilerParams(collective_id=0, has_side_effects=True,
                                             vmem_limit_bytes=67_043_328),
    )(mask_blk, user_sh, item_sh, triples.T)


def solution(mesh):
    def local_fn(mask_blk, user_sh, item_sh, triples):
        final_user, final_item, loss = hand_out(*propagate(mask_blk, user_sh, item_sh, triples))
        return final_user, final_item, loss.reshape(-1)

    return jax.shard_map(
        local_fn, mesh=mesh,
        in_specs=(P("row", "col"), P(("row", "col"), "emb"), P(("col", "row"), "emb"), P()),
        out_specs=(P(("row", "col"), "emb"), P(("col", "row"), "emb"), P()),
        check_vma=False)
```

```python
import functools

import jax
import jax.numpy as jnp
from jax import lax
from jax.experimental import pallas as pl
from jax.experimental.pallas import tpu as pltpu
from jax.sharding import PartitionSpec as P

NUM_LAYERS = 3
F32 = jnp.float32
BF16 = jnp.bfloat16
MESH = pl.DeviceIdType.MESH

CHUNK = 256
MASK_SLOTS = 7
GROUP = 4
EARLY = 8
PIECES = 16
CORE_SLOTS = 4
SCALE_ROWS = 256
LAG = 3
FOLD = 2048


def prop_kernel(mask_hbm, eu_hbm, ei_hbm, trip_hbm, outu_ref, outi_ref, loss_ref,
                adj, mbuf, panel, table, stage, drecv, upanel, upart, yflat, eu_ref, ei_ref, trip_ref, trip_vec,
                csum, ccore, cchip, cfar, rdeg, rdfar, pick_idx, pick_in, mixed, dots,
                u_s, u_r, y_s, y_r,
                d_s, d_r, x_s, x_r, agx_s, agx_r, agd_s, agd_r, agf_s, agf_r,
                fin_s, fin_r, loss_s, loss_r):
    users, items = adj.shape
    rsum = rscale = upart
    own_u = eu_ref.shape[0]
    own_i = ei_ref.shape[0]
    n_chunk = own_i // CHUNK
    row = lax.axis_index("row")
    col = lax.axis_index("col")
    mate = row + 1 - 2 * (row % 2)
    far = (row + 2) % 4
    far_mate = (mate + 2) % 4
    other_col = 1 - col
    to_mate = {"row": mate}
    to_far = {"row": far}
    to_col = {"col": other_col}
    emb = lax.axis_index("emb")
    peers = [{"emb": (emb + de) % 2, "row": (row + dr) % 4, "col": (col + dc) % 2}
             for de in range(2) for dr in range(4) for dc in range(2)][1:]
    share = loss_ref.shape[1] // 8

    def remote(src, dst, ssem, rsem, target):
        return pltpu.make_async_remote_copy(src_ref=src, dst_ref=dst, send_sem=ssem, recv_sem=rsem,
                                            device_id=target, device_id_type=MESH)

    def rows_of(owner, j, size=CHUNK):
        return pl.ds(pl.multiple_of(owner * own_i + j * size, size), size)

    block = pl.ds(pl.multiple_of(row * own_i, own_i), own_i)
    far_block = pl.ds(pl.multiple_of(far * own_i, own_i), own_i)
    ublock = pl.ds(pl.multiple_of(col * own_u, own_u), own_u)
    oblock = pl.ds(pl.multiple_of(other_col * own_u, own_u), own_u)
    n_mask = items // CHUNK

    def mask_copy(i):
        slot = i % MASK_SLOTS
        return pltpu.make_async_copy(mask_hbm.at[:, rows_of(i % 4, i // 4)], mbuf.at[slot], fin_r.at[0, slot])

    for i in range(MASK_SLOTS - 1):
        mask_copy(i).start()
    inputs = [pltpu.make_async_copy(src, dst, fin_r.at[0, 8 + k]) for k, (src, dst) in enumerate((
        (eu_hbm, upanel.at[0, ublock]), (ei_hbm, panel.at[0, block]), (eu_hbm, eu_ref), (ei_hbm, ei_ref),
        (trip_hbm, trip_ref), (trip_hbm, trip_vec)))]
    for copy in inputs:
        copy.start()

    barrier = pltpu.get_barrier_semaphore()
    neighbours = (to_mate, to_far, to_col, {"emb": 1 - emb})
    for target in neighbours:
        pl.semaphore_signal(barrier, inc=1, device_id=target, device_id_type=MESH)

    rsum[...] = jnp.zeros_like(rsum)

    def mask_step(i, carry):
        mask_copy(i).wait()

        @pl.when(i + MASK_SLOTS - 1 < n_mask)
        def _():
            mask_copy(i + MASK_SLOTS - 1).start()

        cols = rows_of(i % 4, i // 4)
        slot = i % MASK_SLOTS

        def tile(t, acc):
            rows = pl.ds(pl.multiple_of(t * 64, 64), 64)
            m = mbuf[slot, rows, :].astype(F32)
            adj[rows, cols] = m.astype(BF16)
            part = m[:, 0:128]
            for g in range(1, CHUNK // 128):
                part = part + m[:, g * 128:(g + 1) * 128]
            rsum[rows, :] += part
            return acc + jnp.sum(m.reshape(8, 8, CHUNK), axis=0)

        acc = lax.fori_loop(0, users // 64, tile, jnp.zeros((8, CHUNK), F32))
        csum[:, pl.ds(pl.multiple_of(i * CHUNK, CHUNK), CHUNK)] = jnp.sum(acc, axis=0, keepdims=True)
        return carry

    pl.semaphore_wait(barrier, len(neighbours))

    quarter = own_i // 4

    def ag0_x(k):
        return remote(ei_hbm.at[pl.ds(k * quarter, quarter)],
                      panel.at[0, pl.ds(pl.multiple_of(row * own_i + k * quarter, quarter), quarter)],
                      fin_r.at[1, 0], fin_r.at[1, 3], to_far)

    ag0_d = remote(ei_hbm, panel.at[0, block], fin_r.at[1, 1], fin_r.at[1, 4], to_mate)
    ag0_f = remote(panel.at[0, far_block], panel.at[0, far_block], fin_r.at[1, 2], fin_r.at[1, 5], to_mate)
    for k in range(2):
        ag0_x(k).start()
    ag0_d.start()
    u0 = remote(eu_hbm, upanel.at[0, ublock], u_s.at[0], u_r.at[0], to_col)
    u0.start()

    early = EARLY * 4 * CHUNK
    parts = (pl.ds(0, early), pl.ds(early, items - early))

    def deg_d(k):
        return remote(csum.at[:, parts[k]], ccore.at[:, parts[k]], fin_r.at[1, 6 + k], fin_r.at[2, k], to_mate)

    def deg_x(k):
        return remote(cchip.at[:, parts[k]], cfar.at[:, parts[k]], fin_r.at[1, 8 + k], fin_r.at[2, 2 + k], to_far)

    def add_core(k):
        deg_d(k).wait()
        cchip[:, parts[k]] = csum[:, parts[k]] + ccore[:, parts[k]]
        deg_x(k).start()

    def col_factors(k):
        deg_x(k).wait()
        csum[:, parts[k]] = lax.rsqrt(jnp.maximum(cchip[:, parts[k]] + cfar[:, parts[k]], 1.0))

    lax.fori_loop(0, 4 * EARLY, mask_step, 0)
    deg_d(0).start()
    lax.fori_loop(4 * EARLY, 4 * EARLY + 4, mask_step, 0)
    add_core(0)
    ag0_x(2).start()
    ag0_x(3).start()
    lax.fori_loop(4 * EARLY + 4, n_mask, mask_step, 0)

    ones = jnp.ones((8, 128), BF16)
    rdeg[...] = lax.dot_general(ones, rsum[...].astype(BF16), (((1,), (1,)), ((), ())),
                                preferred_element_type=F32)[0:1, :]
    deg_y = remote(rdeg, rdfar, fin_r.at[1, 10], fin_r.at[2, 4], to_col)
    deg_y.start()
    deg_d(1).start()
    for copy in inputs:
        copy.wait()
    u0.wait_recv()
    col_factors(0)
    add_core(1)
    deg_y.wait()
    deg_u = jnp.maximum(rdeg[...] + rdfar[...], 1.0)
    rscale[...] = lax.rsqrt(jnp.broadcast_to(deg_u, (128, users)).T)

    def scale_block(owner, j):
        ci = csum[:, pl.ds(pl.multiple_of((j * 4 + owner) * CHUNK, CHUNK), CHUNK)]

        def tile(t, carry):
            rows = pl.ds(pl.multiple_of(t * SCALE_ROWS, SCALE_ROWS), SCALE_ROWS)
            ru = rscale[rows, :]
            for g in range(CHUNK // 128):
                sub = pl.ds(pl.multiple_of(owner * own_i + j * CHUNK + g * 128, 128), 128)
                m = adj[rows, sub].astype(F32)
                adj[rows, sub] = ((ru * m) * ci[:, g * 128:(g + 1) * 128]).astype(BF16)
            return carry

        lax.fori_loop(0, users // SCALE_ROWS, tile, 0)

    def item_part(owner, j, layer):
        return lax.dot_general(adj[:, rows_of(owner, j)], upanel[layer - 1], (((0,), (0,)), ((), ())),
                               preferred_element_type=F32)

    def core_copy(slot, half=None):
        rows = slot_rows(slot, half)
        return remote(stage.at[rows], drecv.at[rows], d_s.at[slot], d_r.at[slot], to_mate)

    def region(k, j):
        return pl.ds(pl.multiple_of(k * own_i + j * CHUNK, CHUNK), CHUNK)

    def near(j):
        return region(0, j)

    def arrived(j, layer):
        return region(1 + layer % 2, j)

    def xsend(j):
        return region(3, j)

    def chunk_rows(j):
        return pl.ds(pl.multiple_of(j * CHUNK, CHUNK), CHUNK)

    def slot_rows(slot, half=None):
        if half is None:
            return pl.ds(pl.multiple_of(slot * 2 * CHUNK, 2 * CHUNK), 2 * CHUNK)
        return pl.ds(pl.multiple_of(slot * 2 * CHUNK + half * CHUNK, CHUNK), CHUNK)

    def x_copy(j, layer):
        return remote(table.at[xsend(j)], table.at[arrived(j, layer)], x_s.at[j // GROUP], x_r.at[layer % 2, j], to_far)

    def x_sent(g):
        rows = pl.ds(pl.multiple_of(3 * own_i + g * GROUP * CHUNK, GROUP * CHUNK), GROUP * CHUNK)
        remote(table.at[rows], table.at[rows], x_s.at[g], x_r.at[0, 0], to_far).wait_send()

    def item_send_step(j, layer):
        slot = j % CORE_SLOTS
        if layer == 2:
            pl.when(j >= CORE_SLOTS)(core_copy(slot).wait_send)
        else:
            core_copy(slot).wait_send()

        @pl.when(j % GROUP == 0)
        def _():
            x_sent(j // GROUP)

        stage[slot_rows(slot, 0), :] = item_part(far_mate, j, layer)
        stage[slot_rows(slot, 1), :] = item_part(mate, j, layer)
        core_copy(slot).start()
        table[xsend(j), :] = item_part(far, j, layer)
        table[near(j), :] = item_part(row, j, layer)

        @pl.when(j == 0)
        def _():
            add_mate(0, layer)

        @pl.when(j >= 2)
        def _():
            add_mate(j - 1, layer)

    def add_mate(j, layer):
        slot = j % CORE_SLOTS
        core_copy(slot).wait_recv()
        table[xsend(j), :] += drecv[slot_rows(slot, 0), :]
        table[near(j), :] += drecv[slot_rows(slot, 1), :]
        x_copy(j, layer).start()

    def layer1_step(j, to_far_chip):
        slot = j % CORE_SLOTS
        theirs, ours, here = (far_mate, far, xsend) if to_far_chip else (mate, row, near)
        if to_far_chip:
            pl.when(j >= CORE_SLOTS)(core_copy(slot, 0).wait_send)
        else:
            core_copy(slot, 0).wait_send()
        scale_block(theirs, j)
        scale_block(ours, j)
        stage[slot_rows(slot, 0), :] = item_part(theirs, j, 1)
        table[here(j), :] = item_part(ours, j, 1)
        core_copy(slot, 0).start()
        if not to_far_chip:
            @pl.when(j == 0)
            def _():
                layer1_add(0, to_far_chip)

        @pl.when(j >= 2)
        def _():
            layer1_add(j - 1, to_far_chip)

    def layer1_first():
        scale_block(far_mate, 0)
        stage[slot_rows(0, 0), :] = item_part(far_mate, 0, 1)
        core_copy(0, 0).start()
        scale_block(far, 0)
        table[xsend(0), :] = item_part(far, 0, 1)
        layer1_add(0, True)

    def layer1_add(j, to_far_chip):
        slot = j % CORE_SLOTS
        here = xsend if to_far_chip else near
        core_copy(slot, 0).wait_recv()
        table[here(j), :] += drecv[slot_rows(slot, 0), :]
        if to_far_chip:
            x_copy(j, 1).start()

    def ag_copy(kind, g, layer, whole=False):
        par = layer % 2
        rows = rows_of(far if kind == "fwd" else row, 0 if whole else g, own_i if whole else GROUP * CHUNK)
        piece = panel.at[par, rows]
        ssem, rsem, target = {"x": (agx_s, agx_r, to_far), "mate": (agd_s, agd_r, to_mate),
                              "fwd": (agf_s, agf_r, to_mate)}[kind]
        return remote(piece, piece, ssem.at[0], rsem.at[par, g], target)

    def fin_copy(kind, j):
        src, dst, k, target = {
            "col": (panel.at[1, rows_of(row, j)], panel.at[1, rows_of(far, j)], 0, to_col),
            "mate": (panel.at[1, rows_of(row, j)], panel.at[1, rows_of(row, j)], 1, to_mate),
            "fwd": (panel.at[1, rows_of(far, j)], panel.at[1, rows_of(far, j)], 2, to_mate)}[kind]
        return remote(src, dst, fin_s.at[k], fin_r.at[k, j], target)

    def fin_near(j):
        fin_copy("col", j).wait_recv()
        fin_copy("fwd", j).start()
        table[region(2, j), :] = panel[1, rows_of(far, j), :].astype(F32)
        fin_copy("mate", j).wait_recv()
        table[region(1, j), :] = panel[1, rows_of(mate, j), :].astype(F32)

    def fin_fwd(j):
        @pl.when(j % GROUP == 0)
        def _():
            x_sent(j // GROUP)

        fin_copy("fwd", j).wait_recv()
        table[region(3, j), :] = panel[1, rows_of(far_mate, j), :].astype(F32)

    def finish_item(j, layer):
        x_copy(j, layer).wait_recv()
        par = layer % 2
        value = (table[near(j), :] + table[arrived(j, layer), :]).astype(BF16)
        if layer < NUM_LAYERS:
            panel[par, rows_of(row, j), :] = value

            @pl.when(j % GROUP == GROUP - 1)
            def _():
                ag_copy("x", j // GROUP, layer).start()
                ag_copy("mate", j // GROUP, layer).start()
        else:
            total = ei_ref[chunk_rows(j), :].astype(F32) + panel[1, rows_of(row, j), :].astype(F32)
            total = total + panel[0, rows_of(row, j), :].astype(F32)
            total = total + value.astype(F32)
            final = (total / (NUM_LAYERS + 1)).astype(BF16)
            panel[1, rows_of(row, j), :] = final
            outi_ref[chunk_rows(j), :] = final
            table[near(j), :] = final.astype(F32)
            fin_copy("col", j).start()
            fin_copy("mate", j).start()

    def gather_items(layer):
        for g in range(n_chunk // GROUP):
            ag_copy("x", g, layer).wait_recv()
            ag_copy("fwd", g, layer).start()
        for g in range(n_chunk // GROUP):
            ag_copy("mate", g, layer).wait_recv()
            ag_copy("fwd", g, layer).wait_recv()
        for kind in ("x", "mate", "fwd"):
            ag_copy(kind, 0, layer, whole=True).wait_send()

    def user_part(layer):
        par = (layer - 1) % 2
        upart[...] = jnp.zeros_like(upart)

        def fold(i, carry):
            cols = pl.ds(pl.multiple_of(i * FOLD, FOLD), FOLD)
            upart[...] += jnp.dot(adj[:, cols], panel[par, cols, :], preferred_element_type=F32)
            return carry

        lax.fori_loop(0, items // FOLD, fold, 0)

    def yrows(layer):
        return pl.ds((layer - 1) * own_u, own_u)

    def y_copy(layer):
        return remote(upart.at[oblock], yflat.at[yrows(layer)], y_s.at[0], y_r.at[0], to_col)

    def u_copy(layer):
        return remote(upanel.at[layer, ublock], upanel.at[layer, ublock], u_s.at[0], u_r.at[0], to_col)

    def finish_user(layer):
        y_copy(layer).wait()
        value = (upart[ublock, :] + yflat[yrows(layer), :]).astype(BF16)
        if layer < NUM_LAYERS:
            upanel[layer, ublock, :] = value
            u_copy(layer).start()
        else:
            total = eu_ref[...].astype(F32) + upanel[1, ublock, :].astype(F32)
            total = total + upanel[2, ublock, :].astype(F32)
            total = total + value.astype(F32)
            final = (total / (NUM_LAYERS + 1)).astype(BF16)
            eu_ref[...] = final
            outu_ref[...] = final
            stage[0:own_u, :] = final.astype(F32)
            fu_copy("col").start()
            fu_copy("mate").start()

    def fu_copy(kind):
        src, dst, k, target = {
            "col": (eu_ref, upanel.at[0, pl.ds(0, own_u)], 0, to_col),
            "mate": (eu_ref, upanel.at[0, pl.ds(own_u, own_u)], 1, to_mate),
            "fwd": (upanel.at[0, pl.ds(0, own_u)], upanel.at[1, oblock], 2, to_mate)}[kind]
        return remote(src, dst, agd_r.at[0, k], agd_r.at[1, k], target)

    def gather_users():
        fu_copy("col").wait_recv()
        fu_copy("fwd").start()
        stage[2 * own_u:3 * own_u, :] = upanel[0, 0:own_u, :].astype(F32)
        fu_copy("mate").wait_recv()
        stage[own_u:2 * own_u, :] = upanel[0, own_u:2 * own_u, :].astype(F32)
        fu_copy("fwd").wait_recv()
        stage[3 * own_u:4 * own_u, :] = upanel[1, oblock, :].astype(F32)

    def place_rows(piece):
        def side(r):
            return r // 2

        def step(t, carry):
            for k, owner in ((0, far), (1, row)):
                base = (owner * 2 + col) * share + t
                user = trip_ref[0, base]
                ur = lax.shift_right_logical(user, 10)
                uc = lax.bitwise_and(lax.shift_right_logical(user, 9), 1)
                pos = (jnp.where(uc == col, 0, 2) + jnp.where(ur == row, 0, 1)) * own_u + lax.bitwise_and(user, 511)
                pick_idx[k * 3 * share + t] = jnp.where(lax.shift_right_logical(ur, 1) == side(row), pos, 4 * own_u)
                for which in (1, 2):
                    item = trip_ref[which, base]
                    ic = lax.shift_right_logical(item, 14)
                    ir = lax.bitwise_and(lax.shift_right_logical(item, 12), 3)
                    pos = (jnp.where(ic == col, 0, 2) + jnp.where(ir == row, 0, 1)) * own_i + lax.bitwise_and(item, 4095)
                    pick_idx[(k * 3 + which) * share + t] = jnp.where(
                        lax.shift_right_logical(ir, 1) == side(row), pos, 4 * own_i)
            return carry

        lax.fori_loop(piece * (share // PIECES), (piece + 1) * (share // PIECES), step, 0)

    def pick(src, k, which, dst, lo=0, hi=None):
        def step(t, carry):
            for i in range(8):
                at = t * 8 + i
                dst[pl.ds(which * share + at, 1), :] = src[pl.ds(pick_idx[(k * 3 + which) * share + at], 1), :]
            return carry

        lax.fori_loop(lo // 8, (hi or share) // 8, step, 0)

    def out_rows(lo, size):
        return pl.ds(pl.multiple_of(far * own_i + lo, size), size)

    def pick_copy(k):
        lo, size = ((0, 2 * share), (2 * share, share // 2), (5 * share // 2, share // 2))[k]
        return remote(panel.at[0, out_rows(lo, size)], pick_in.at[pl.ds(lo, size)],
                      agx_r.at[0, k], agx_r.at[1, k], to_far)

    def thirds(k):
        return pl.ds(k * share, share)

    def swap_users():
        pick(stage, 0, 0, yflat)
        pick(stage, 1, 0, drecv)
        panel[0, out_rows(0, share), :] = yflat[thirds(0), :].astype(BF16)
        panel[0, out_rows(share, share), :] = drecv[thirds(0), :].astype(BF16)
        pick_copy(0).start()

    def mark_mixed():
        ids = trip_vec[1:3, pl.ds(pl.multiple_of((far * 2 + col) * share, share), share)]
        sides = lax.bitwise_and(lax.shift_right_logical(ids, 13), 1)
        flag = jnp.where(sides[0:1] == sides[1:2], 0.0, 1.0)
        mixed[...] = jnp.broadcast_to(flag, (128, share)).T

    def loop(lo, hi, body):
        def step(j, carry):
            body(j)
            return carry
        lax.fori_loop(lo, hi, step, 0)

    for layer in range(1, NUM_LAYERS + 1):
        if layer == 1:
            send_far = functools.partial(layer1_step, to_far_chip=True)
            send_near = functools.partial(layer1_step, to_far_chip=False)
            layer1_first()
            loop(1, EARLY, send_far)
            col_factors(1)
            remote(panel.at[0, far_block], panel.at[0, far_block], fin_r.at[1, 0], fin_r.at[1, 3], to_far).wait()
            ag0_f.start()
            loop(EARLY, n_chunk, send_far)
            layer1_add(n_chunk - 1, True)
            loop(0, n_chunk, send_near)
            layer1_add(n_chunk - 1, False)
            for slot in range(CORE_SLOTS):
                core_copy(slot, 0).wait_send()
        else:
            loop(0, n_chunk, functools.partial(item_send_step, layer=layer))
            add_mate(n_chunk - 1, layer)
        if layer == 1:
            ag0_d.wait()
            ag0_f.wait()
            u0.wait_send()
        else:
            gather_items(layer - 1)
        finish = functools.partial(finish_item, layer=layer)
        if layer == 1:
            loop(0, n_chunk // 2, finish)
            user_part(layer)
            y_copy(layer).start()
            loop(n_chunk // 2, n_chunk, finish)
            loop(0, 4, place_rows)
            mark_mixed()
            finish_user(layer)
            u_copy(layer).wait()
        elif layer < NUM_LAYERS:
            user_part(layer)
            y_copy(layer).start()
            loop(0, n_chunk // 2, finish)
            finish_user(layer)
            loop(4, PIECES, place_rows)
            loop(n_chunk // 2, n_chunk, finish)
            u_copy(layer).wait()
        else:
            user_part(layer)
            y_copy(layer).start()

    for slot in range(CORE_SLOTS):
        core_copy(slot).wait_send()
    table[pl.ds(4 * own_i, 8), :] = jnp.zeros((8, 128), F32)
    stage[pl.ds(4 * own_u, 8), :] = jnp.zeros((8, 128), F32)

    def last_step(j):
        finish_item(j, NUM_LAYERS)

        @pl.when(j >= LAG)
        def _():
            fin_near(j - LAG)

        @pl.when(j >= LAG + 2)
        def _():
            fin_fwd(j - LAG - 2)

    loop(0, n_chunk // 2, last_step)
    finish_user(NUM_LAYERS)
    loop(n_chunk // 2, 3 * n_chunk // 4, last_step)
    gather_users()
    swap_users()
    loop(3 * n_chunk // 4, n_chunk, last_step)
    loop(n_chunk - LAG, n_chunk, fin_near)
    loop(n_chunk - LAG - 2, n_chunk, fin_fwd)
    for k in (1, 2):
        lo, hi = (k - 1) * share // 2, k * share // 2
        pick(table, 0, 1, yflat, lo, hi)
        pick(table, 0, 2, yflat, lo, hi)
        diff = yflat[share + lo:share + hi, :] - yflat[2 * share + lo:2 * share + hi, :]
        panel[0, out_rows(2 * share + lo, share // 2), :] = jnp.where(mixed[lo:hi, :] > 0.5, diff, 0.0).astype(BF16)
        pick_copy(k).start()
    pick(table, 1, 1, drecv)
    pick(table, 1, 2, drecv)

    def score(user, items_diff):
        return jnp.sum((user * items_diff).T, axis=0, keepdims=True)

    n_dev = len(peers) + 1
    base = (emb * (n_dev // 2) + row * 2 + col) * 2 * share
    pick_copy(0).wait_recv()
    e_far = yflat[thirds(0), :] + pick_in[thirds(1), :].astype(F32)
    diff = jnp.where(mixed[...] > 0.5, 0.0, yflat[thirds(1), :] - yflat[thirds(2), :])
    dots[:, pl.ds(pl.multiple_of(base + share, share), share)] = score(e_far, diff)
    e_own = drecv[thirds(0), :] + pick_in[thirds(0), :].astype(F32)
    diff = drecv[thirds(1), :] - drecv[thirds(2), :]
    pick_copy(1).wait_recv()
    pick_copy(2).wait_recv()
    diff = diff + pick_in[thirds(2), :].astype(F32)
    dots[:, pl.ds(pl.multiple_of(base, share), share)] = score(e_own, diff)
    mine = pl.ds(pl.multiple_of(base, 2 * share), 2 * share)
    for target in peers:
        remote(dots.at[:, mine], dots.at[:, mine], loss_s.at[0], loss_r.at[0], target).start()

    for k in range(3):
        pick_copy(k).wait_send()
    for k, kind in enumerate(("col", "mate", "fwd")):
        fu_copy(kind).wait_send()
        remote(panel.at[1, block], panel.at[1, block], fin_s.at[k], fin_r.at[0, 0], to_mate).wait_send()
    others = dots.at[:, pl.ds(0, len(peers) * 2 * share)]
    remote(others, others, loss_s.at[0], loss_r.at[0], to_far).wait()
    half = n_dev // 2
    for g in range(half):
        near_far = [[dots[:, ((e * half + owner) * 2 + k) * share:((e * half + owner) * 2 + k + 1) * share]
                     for k, owner in ((0, g), (1, (g + half // 2) % half))] for e in range(2)]
        z = -((near_far[0][0] + near_far[0][1]) + (near_far[1][0] + near_far[1][1]))
        loss_ref[:, g * share:(g + 1) * share] = jnp.maximum(z, 0.0) + jnp.log1p(jnp.exp(-jnp.abs(z)))


def hand_out_kernel(u_in, i_in, l_in, u_out, i_out, l_out, out_s):
    pieces = [pltpu.make_async_copy(src, dst, out_s.at[k])
              for k, (src, dst) in enumerate(((i_in, i_out), (u_in, u_out), (l_in, l_out)))]
    for piece in pieces:
        piece.start()
    for piece in pieces:
        piece.wait()


def hand_out(*arrays):
    return pl.pallas_call(
        hand_out_kernel,
        name="hand_out",
        out_shape=tuple(jax.ShapeDtypeStruct(a.shape, a.dtype) for a in arrays),
        in_specs=[pl.BlockSpec(memory_space=pltpu.VMEM)] * 3,
        out_specs=(pl.BlockSpec(memory_space=pl.ANY),) * 3,
        scratch_shapes=[pltpu.SemaphoreType.DMA((6,))],
        compiler_params=pltpu.CompilerParams(vmem_limit_bytes=2 * 2 ** 20),
    )(*arrays)


def propagate(mask_blk, user_sh, item_sh, triples):
    users, items = mask_blk.shape
    own_u, dim = user_sh.shape
    own_i = item_sh.shape[0]
    n_chunk = own_i // CHUNK
    num_trip = triples.shape[0]
    share = num_trip // 8
    n_group = n_chunk // GROUP
    vmem, dma = pltpu.VMEM, pltpu.SemaphoreType.DMA
    return pl.pallas_call(
        prop_kernel,
        name="propagate",
        out_shape=(vmem((own_u, dim), BF16), vmem((own_i, dim), BF16), vmem((1, num_trip), F32)),
        in_specs=[pl.BlockSpec(memory_space=pl.ANY)] * 4,
        out_specs=(pl.BlockSpec(memory_space=pltpu.VMEM),) * 3,
        scratch_shapes=[
            vmem((users, items), BF16),
            vmem((MASK_SLOTS, users, CHUNK), jnp.int32),
            vmem((2, items, dim), BF16),
            vmem((4 * own_i + 8, dim), F32),
            vmem((CORE_SLOTS * 2 * CHUNK + 8, dim), F32),
            vmem((CORE_SLOTS * 2 * CHUNK, dim), F32),
            vmem((3, users, dim), BF16),
            vmem((users, dim), F32),
            vmem((3 * own_u, dim), F32),
            vmem((own_u, dim), BF16),
            vmem((own_i, dim), BF16),
            pltpu.SMEM((3, num_trip), jnp.int32),
            vmem((3, num_trip), jnp.int32),
            vmem((1, items), F32),
            vmem((1, items), F32),
            vmem((1, items), F32),
            vmem((1, items), F32),
            vmem((1, users), F32),
            vmem((1, users), F32),
            pltpu.SMEM((6 * share,), jnp.int32),
            vmem((3 * share, dim), BF16),
            vmem((share, 128), F32),
            vmem((1, 4 * num_trip), F32),
            dma((1,)), dma((1,)),
            dma((1,)), dma((1,)),
            dma((CORE_SLOTS,)), dma((CORE_SLOTS,)),
            dma((n_group,)), dma((2, n_chunk)),
            dma((1,)), dma((2, n_group)),
            dma((1,)), dma((2, n_group)),
            dma((1,)), dma((2, n_group)),
            dma((3,)), dma((3, n_chunk)),
            dma((1,)), dma((1,)),
        ],
        compiler_params=pltpu.CompilerParams(collective_id=0, has_side_effects=True,
                                             vmem_limit_bytes=65_700_000),
    )(mask_blk, user_sh, item_sh, triples.T)


def solution(mesh):
    def local_fn(mask_blk, user_sh, item_sh, triples):
        final_user, final_item, loss = hand_out(*propagate(mask_blk, user_sh, item_sh, triples))
        return final_user, final_item, loss.reshape(-1)

    return jax.shard_map(
        local_fn, mesh=mesh,
        in_specs=(P("row", "col"), P(("row", "col"), "emb"), P(("col", "row"), "emb"), P()),
        out_specs=(P(("row", "col"), "emb"), P(("col", "row"), "emb"), P()),
        check_vma=False)
```

```python
import functools

import jax
import jax.numpy as jnp
from jax import lax
from jax.experimental import pallas as pl
from jax.experimental.pallas import tpu as pltpu
from jax.sharding import PartitionSpec as P

NUM_LAYERS = 3
F32 = jnp.float32
BF16 = jnp.bfloat16
MESH = pl.DeviceIdType.MESH

CHUNK = 256
MASK_SLOTS = 7
GROUP = 4
EARLY = 8
PIECES = 16
CORE_SLOTS = 4
SCALE_ROWS = 256
LAG = 3
FOLD = 2048


def prop_kernel(mask_hbm, eu_hbm, ei_hbm, trip_hbm, outu_ref, outi_ref, loss_ref,
                adj, mbuf, panel, table, stage, drecv, upanel, upart, yflat, eu_ref, ei_ref, trip_ref, trip_vec,
                csum, ccore, cchip, cfar, rdeg, rdfar, rdemb, pick_idx, pick_in, mixed, dots,
                u_s, u_r, y_s, y_r,
                d_s, d_r, x_s, x_r, agx_s, agx_r, agd_s, agd_r, agf_s, agf_r,
                fin_s, fin_r, loss_s, loss_r):
    users, items = adj.shape
    rsum = rscale = upart
    own_u = eu_ref.shape[0]
    own_i = ei_ref.shape[0]
    n_chunk = own_i // CHUNK
    row = lax.axis_index("row")
    col = lax.axis_index("col")
    mate = row + 1 - 2 * (row % 2)
    far = (row + 2) % 4
    far_mate = (mate + 2) % 4
    other_col = 1 - col
    to_mate = {"row": mate}
    to_far = {"row": far}
    to_col = {"col": other_col}
    emb = lax.axis_index("emb")
    peers = [{"emb": (emb + de) % 2, "row": (row + dr) % 4, "col": (col + dc) % 2}
             for de in range(2) for dr in range(4) for dc in range(2)][1:]
    share = loss_ref.shape[1] // 8

    def remote(src, dst, ssem, rsem, target):
        return pltpu.make_async_remote_copy(src_ref=src, dst_ref=dst, send_sem=ssem, recv_sem=rsem,
                                            device_id=target, device_id_type=MESH)

    def rows_of(owner, j, size=CHUNK):
        return pl.ds(pl.multiple_of(owner * own_i + j * size, size), size)

    block = pl.ds(pl.multiple_of(row * own_i, own_i), own_i)
    far_block = pl.ds(pl.multiple_of(far * own_i, own_i), own_i)
    ublock = pl.ds(pl.multiple_of(col * own_u, own_u), own_u)
    oblock = pl.ds(pl.multiple_of(other_col * own_u, own_u), own_u)
    n_mask = items // CHUNK

    def mask_block(i):
        return (i + emb * (n_mask // 2)) % n_mask

    def mask_copy(i):
        slot = i % MASK_SLOTS
        b = mask_block(i)
        return pltpu.make_async_copy(mask_hbm.at[:, rows_of(b % 4, b // 4)], mbuf.at[slot], fin_r.at[0, slot])

    for i in range(MASK_SLOTS - 1):
        mask_copy(i).start()
    inputs = [pltpu.make_async_copy(src, dst, fin_r.at[0, 8 + k]) for k, (src, dst) in enumerate((
        (eu_hbm, upanel.at[0, ublock]), (ei_hbm, panel.at[0, block]), (eu_hbm, eu_ref), (ei_hbm, ei_ref),
        (trip_hbm, trip_ref), (trip_hbm, trip_vec)))]
    for copy in inputs:
        copy.start()

    barrier = pltpu.get_barrier_semaphore()
    neighbours = (to_mate, to_far, to_col, {"emb": 1 - emb})
    for target in neighbours:
        pl.semaphore_signal(barrier, inc=1, device_id=target, device_id_type=MESH)

    rsum[...] = jnp.zeros_like(rsum)

    def mask_step(i, carry, count):
        mask_copy(i).wait()

        @pl.when(i + MASK_SLOTS - 1 < n_mask)
        def _():
            mask_copy(i + MASK_SLOTS - 1).start()

        b = mask_block(i)
        cols = rows_of(b % 4, b // 4)
        slot = i % MASK_SLOTS

        def tile(t, acc):
            rows = pl.ds(pl.multiple_of(t * 64, 64), 64)
            m = mbuf[slot, rows, :].astype(F32)
            adj[rows, cols] = m.astype(BF16)
            if not count:
                return acc
            part = m[:, 0:128]
            for g in range(1, CHUNK // 128):
                part = part + m[:, g * 128:(g + 1) * 128]
            rsum[rows, :] += part
            return acc + jnp.sum(m.reshape(8, 8, CHUNK), axis=0)

        if count:
            acc = lax.fori_loop(0, users // 64, tile, jnp.zeros((8, CHUNK), F32))
            csum[:, pl.ds(pl.multiple_of(b * CHUNK, CHUNK), CHUNK)] = jnp.sum(acc, axis=0, keepdims=True)
        else:
            lax.fori_loop(0, users // 64, tile, 0)
        return carry

    def stream(lo, hi, count=False):
        lax.fori_loop(lo, hi, functools.partial(mask_step, count=count), 0)

    pl.semaphore_wait(barrier, len(neighbours))

    def head(k):
        return fin_r.at[1, k], fin_r.at[2, k]

    quarter = own_i // 4

    def ag0_x(k):
        return remote(ei_hbm.at[pl.ds(k * quarter, quarter)],
                      panel.at[0, pl.ds(pl.multiple_of(row * own_i + k * quarter, quarter), quarter)],
                      *head(0), to_far)

    ag0_d = remote(ei_hbm, panel.at[0, block], *head(1), to_mate)
    ag0_f = remote(panel.at[0, far_block], panel.at[0, far_block], *head(2), to_mate)
    for k in range(2):
        ag0_x(k).start()
    ag0_d.start()
    u0 = remote(eu_hbm, upanel.at[0, ublock], u_s.at[0], u_r.at[0], to_col)
    u0.start()

    half_cols = pl.ds(pl.multiple_of(emb * (items // 2), items // 2), items // 2)
    to_emb = {"emb": 1 - emb}
    ones = jnp.ones((8, 128), BF16)
    deg_z = remote(rdeg, rdemb, *head(3), to_emb)
    deg_y = remote(rdeg, rdfar, *head(4), to_col)
    deg_d = remote(csum.at[:, half_cols], ccore.at[:, half_cols], *head(5), to_mate)
    deg_x = remote(cchip.at[:, half_cols], cfar.at[:, half_cols], *head(6), to_far)
    deg_e = remote(csum.at[:, half_cols], csum.at[:, half_cols], *head(7), to_emb)
    mid = n_mask // 2

    stream(0, mid, count=True)
    rdeg[...] = lax.dot_general(ones, rsum[...].astype(BF16), (((1,), (1,)), ((), ())),
                                preferred_element_type=F32)[0:1, :]
    deg_z.start()
    deg_d.start()
    stream(mid, mid + 5)
    deg_z.wait()
    rdeg[...] += rdemb[...]
    deg_y.start()
    deg_d.wait()
    cchip[:, half_cols] = csum[:, half_cols] + ccore[:, half_cols]
    deg_x.start()
    ag0_x(2).start()
    ag0_x(3).start()
    stream(mid + 5, mid + 12)
    deg_y.wait()
    deg_u = jnp.maximum(rdeg[...] + rdfar[...], 1.0)
    rscale[...] = lax.rsqrt(jnp.broadcast_to(deg_u, (128, users)).T)
    stream(mid + 12, mid + 18)
    deg_x.wait()
    csum[:, half_cols] = cchip[:, half_cols] + cfar[:, half_cols]
    deg_e.start()
    stream(mid + 18, mid + 26)
    deg_e.wait()
    csum[...] = lax.rsqrt(jnp.maximum(csum[...], 1.0))
    stream(mid + 26, n_mask)
    for copy in inputs:
        copy.wait()
    u0.wait_recv()

    def scale_block(owner, j):
        ci = csum[:, pl.ds(pl.multiple_of((j * 4 + owner) * CHUNK, CHUNK), CHUNK)]

        def tile(t, carry):
            rows = pl.ds(pl.multiple_of(t * SCALE_ROWS, SCALE_ROWS), SCALE_ROWS)
            ru = rscale[rows, :]
            for g in range(CHUNK // 128):
                sub = pl.ds(pl.multiple_of(owner * own_i + j * CHUNK + g * 128, 128), 128)
                m = adj[rows, sub].astype(F32)
                adj[rows, sub] = ((ru * m) * ci[:, g * 128:(g + 1) * 128]).astype(BF16)
            return carry

        lax.fori_loop(0, users // SCALE_ROWS, tile, 0)

    def item_part(owner, j, layer):
        return lax.dot_general(adj[:, rows_of(owner, j)], upanel[layer - 1], (((0,), (0,)), ((), ())),
                               preferred_element_type=F32)

    def core_copy(slot, half=None):
        rows = slot_rows(slot, half)
        return remote(stage.at[rows], drecv.at[rows], d_s.at[slot], d_r.at[slot], to_mate)

    def region(k, j):
        return pl.ds(pl.multiple_of(k * own_i + j * CHUNK, CHUNK), CHUNK)

    def near(j):
        return region(0, j)

    def arrived(j, layer):
        return region(1 + layer % 2, j)

    def xsend(j):
        return region(3, j)

    def chunk_rows(j):
        return pl.ds(pl.multiple_of(j * CHUNK, CHUNK), CHUNK)

    def slot_rows(slot, half=None):
        if half is None:
            return pl.ds(pl.multiple_of(slot * 2 * CHUNK, 2 * CHUNK), 2 * CHUNK)
        return pl.ds(pl.multiple_of(slot * 2 * CHUNK + half * CHUNK, CHUNK), CHUNK)

    def x_copy(j, layer):
        return remote(table.at[xsend(j)], table.at[arrived(j, layer)], x_s.at[j // GROUP], x_r.at[layer % 2, j], to_far)

    def x_sent(g):
        rows = pl.ds(pl.multiple_of(3 * own_i + g * GROUP * CHUNK, GROUP * CHUNK), GROUP * CHUNK)
        remote(table.at[rows], table.at[rows], x_s.at[g], x_r.at[0, 0], to_far).wait_send()

    def item_send_step(j, layer):
        slot = j % CORE_SLOTS
        if layer == 2:
            pl.when(j >= CORE_SLOTS)(core_copy(slot).wait_send)
        else:
            core_copy(slot).wait_send()

        @pl.when(j % GROUP == 0)
        def _():
            x_sent(j // GROUP)

        stage[slot_rows(slot, 0), :] = item_part(far_mate, j, layer)
        stage[slot_rows(slot, 1), :] = item_part(mate, j, layer)
        core_copy(slot).start()
        table[xsend(j), :] = item_part(far, j, layer)
        table[near(j), :] = item_part(row, j, layer)

        @pl.when(j == 0)
        def _():
            add_mate(0, layer)

        @pl.when(j >= 2)
        def _():
            add_mate(j - 1, layer)

    def add_mate(j, layer):
        slot = j % CORE_SLOTS
        core_copy(slot).wait_recv()
        table[xsend(j), :] += drecv[slot_rows(slot, 0), :]
        table[near(j), :] += drecv[slot_rows(slot, 1), :]
        x_copy(j, layer).start()

    def layer1_step(j, to_far_chip):
        slot = j % CORE_SLOTS
        theirs, ours, here = (far_mate, far, xsend) if to_far_chip else (mate, row, near)
        if to_far_chip:
            pl.when(j >= CORE_SLOTS)(core_copy(slot, 0).wait_send)
        else:
            core_copy(slot, 0).wait_send()
        scale_block(theirs, j)
        scale_block(ours, j)
        stage[slot_rows(slot, 0), :] = item_part(theirs, j, 1)
        table[here(j), :] = item_part(ours, j, 1)
        core_copy(slot, 0).start()
        if not to_far_chip:
            @pl.when(j == 0)
            def _():
                layer1_add(0, to_far_chip)

        @pl.when(j >= 2)
        def _():
            layer1_add(j - 1, to_far_chip)

    def layer1_first():
        scale_block(far_mate, 0)
        stage[slot_rows(0, 0), :] = item_part(far_mate, 0, 1)
        core_copy(0, 0).start()
        scale_block(far, 0)
        table[xsend(0), :] = item_part(far, 0, 1)
        layer1_add(0, True)

    def layer1_add(j, to_far_chip):
        slot = j % CORE_SLOTS
        here = xsend if to_far_chip else near
        core_copy(slot, 0).wait_recv()
        table[here(j), :] += drecv[slot_rows(slot, 0), :]
        if to_far_chip:
            x_copy(j, 1).start()

    def ag_copy(kind, g, layer, whole=False):
        par = layer % 2
        rows = rows_of(far if kind == "fwd" else row, 0 if whole else g, own_i if whole else GROUP * CHUNK)
        piece = panel.at[par, rows]
        ssem, rsem, target = {"x": (agx_s, agx_r, to_far), "mate": (agd_s, agd_r, to_mate),
                              "fwd": (agf_s, agf_r, to_mate)}[kind]
        return remote(piece, piece, ssem.at[0], rsem.at[par, g], target)

    def fin_copy(kind, j):
        src, dst, k, target = {
            "col": (panel.at[1, rows_of(row, j)], panel.at[1, rows_of(far, j)], 0, to_col),
            "mate": (panel.at[1, rows_of(row, j)], panel.at[1, rows_of(row, j)], 1, to_mate),
            "fwd": (panel.at[1, rows_of(far, j)], panel.at[1, rows_of(far, j)], 2, to_mate)}[kind]
        return remote(src, dst, fin_s.at[k], fin_r.at[k, j], target)

    def fin_near(j):
        fin_copy("col", j).wait_recv()
        fin_copy("fwd", j).start()
        table[region(2, j), :] = panel[1, rows_of(far, j), :].astype(F32)
        fin_copy("mate", j).wait_recv()
        table[region(1, j), :] = panel[1, rows_of(mate, j), :].astype(F32)

    def fin_fwd(j):
        @pl.when(j % GROUP == 0)
        def _():
            x_sent(j // GROUP)

        fin_copy("fwd", j).wait_recv()
        table[region(3, j), :] = panel[1, rows_of(far_mate, j), :].astype(F32)

    def finish_item(j, layer):
        x_copy(j, layer).wait_recv()
        par = layer % 2
        value = (table[near(j), :] + table[arrived(j, layer), :]).astype(BF16)
        if layer < NUM_LAYERS:
            panel[par, rows_of(row, j), :] = value

            @pl.when(j % GROUP == GROUP - 1)
            def _():
                ag_copy("x", j // GROUP, layer).start()
                ag_copy("mate", j // GROUP, layer).start()
        else:
            total = ei_ref[chunk_rows(j), :].astype(F32) + panel[1, rows_of(row, j), :].astype(F32)
            total = total + panel[0, rows_of(row, j), :].astype(F32)
            total = total + value.astype(F32)
            final = (total / (NUM_LAYERS + 1)).astype(BF16)
            panel[1, rows_of(row, j), :] = final
            outi_ref[chunk_rows(j), :] = final
            table[near(j), :] = final.astype(F32)
            fin_copy("col", j).start()
            fin_copy("mate", j).start()

    def gather_items(layer):
        for g in range(n_chunk // GROUP):
            ag_copy("x", g, layer).wait_recv()
            ag_copy("fwd", g, layer).start()
        for g in range(n_chunk // GROUP):
            ag_copy("mate", g, layer).wait_recv()
            ag_copy("fwd", g, layer).wait_recv()
        for kind in ("x", "mate", "fwd"):
            ag_copy(kind, 0, layer, whole=True).wait_send()

    def user_part(layer):
        par = (layer - 1) % 2
        upart[...] = jnp.zeros_like(upart)

        def fold(i, carry):
            cols = pl.ds(pl.multiple_of(i * FOLD, FOLD), FOLD)
            upart[...] += jnp.dot(adj[:, cols], panel[par, cols, :], preferred_element_type=F32)
            return carry

        lax.fori_loop(0, items // FOLD, fold, 0)

    def yrows(layer):
        return pl.ds((layer - 1) * own_u, own_u)

    def y_copy(layer):
        return remote(upart.at[oblock], yflat.at[yrows(layer)], y_s.at[0], y_r.at[0], to_col)

    def u_copy(layer):
        return remote(upanel.at[layer, ublock], upanel.at[layer, ublock], u_s.at[0], u_r.at[0], to_col)

    def finish_user(layer):
        y_copy(layer).wait()
        value = (upart[ublock, :] + yflat[yrows(layer), :]).astype(BF16)
        if layer < NUM_LAYERS:
            upanel[layer, ublock, :] = value
            u_copy(layer).start()
        else:
            total = eu_ref[...].astype(F32) + upanel[1, ublock, :].astype(F32)
            total = total + upanel[2, ublock, :].astype(F32)
            total = total + value.astype(F32)
            final = (total / (NUM_LAYERS + 1)).astype(BF16)
            eu_ref[...] = final
            outu_ref[...] = final
            stage[0:own_u, :] = final.astype(F32)
            fu_copy("col").start()
            fu_copy("mate").start()

    def fu_copy(kind):
        src, dst, k, target = {
            "col": (eu_ref, upanel.at[0, pl.ds(0, own_u)], 0, to_col),
            "mate": (eu_ref, upanel.at[0, pl.ds(own_u, own_u)], 1, to_mate),
            "fwd": (upanel.at[0, pl.ds(0, own_u)], upanel.at[1, oblock], 2, to_mate)}[kind]
        return remote(src, dst, agd_r.at[0, k], agd_r.at[1, k], target)

    def gather_users():
        fu_copy("col").wait_recv()
        fu_copy("fwd").start()
        stage[2 * own_u:3 * own_u, :] = upanel[0, 0:own_u, :].astype(F32)
        fu_copy("mate").wait_recv()
        stage[own_u:2 * own_u, :] = upanel[0, own_u:2 * own_u, :].astype(F32)
        fu_copy("fwd").wait_recv()
        stage[3 * own_u:4 * own_u, :] = upanel[1, oblock, :].astype(F32)

    def place_rows(piece):
        def side(r):
            return r // 2

        def step(t, carry):
            for k, owner in ((0, far), (1, row)):
                base = (owner * 2 + col) * share + t
                user = trip_ref[0, base]
                ur = lax.shift_right_logical(user, 10)
                uc = lax.bitwise_and(lax.shift_right_logical(user, 9), 1)
                pos = (jnp.where(uc == col, 0, 2) + jnp.where(ur == row, 0, 1)) * own_u + lax.bitwise_and(user, 511)
                pick_idx[k * 3 * share + t] = jnp.where(lax.shift_right_logical(ur, 1) == side(row), pos, 4 * own_u)
                for which in (1, 2):
                    item = trip_ref[which, base]
                    ic = lax.shift_right_logical(item, 14)
                    ir = lax.bitwise_and(lax.shift_right_logical(item, 12), 3)
                    pos = (jnp.where(ic == col, 0, 2) + jnp.where(ir == row, 0, 1)) * own_i + lax.bitwise_and(item, 4095)
                    pick_idx[(k * 3 + which) * share + t] = jnp.where(
                        lax.shift_right_logical(ir, 1) == side(row), pos, 4 * own_i)
            return carry

        lax.fori_loop(piece * (share // PIECES), (piece + 1) * (share // PIECES), step, 0)

    def pick(src, k, which, dst, lo=0, hi=None):
        def step(t, carry):
            for i in range(8):
                at = t * 8 + i
                dst[pl.ds(which * share + at, 1), :] = src[pl.ds(pick_idx[(k * 3 + which) * share + at], 1), :]
            return carry

        lax.fori_loop(lo // 8, (hi or share) // 8, step, 0)

    def out_rows(lo, size):
        return pl.ds(pl.multiple_of(far * own_i + lo, size), size)

    def pick_copy(k):
        lo, size = ((0, 2 * share), (2 * share, share // 2), (5 * share // 2, share // 2))[k]
        return remote(panel.at[0, out_rows(lo, size)], pick_in.at[pl.ds(lo, size)],
                      agx_r.at[0, k], agx_r.at[1, k], to_far)

    def thirds(k):
        return pl.ds(k * share, share)

    def swap_users():
        pick(stage, 0, 0, yflat)
        pick(stage, 1, 0, drecv)
        panel[0, out_rows(0, share), :] = yflat[thirds(0), :].astype(BF16)
        panel[0, out_rows(share, share), :] = drecv[thirds(0), :].astype(BF16)
        pick_copy(0).start()

    def mark_mixed():
        ids = trip_vec[1:3, pl.ds(pl.multiple_of((far * 2 + col) * share, share), share)]
        sides = lax.bitwise_and(lax.shift_right_logical(ids, 13), 1)
        flag = jnp.where(sides[0:1] == sides[1:2], 0.0, 1.0)
        mixed[...] = jnp.broadcast_to(flag, (128, share)).T

    def loop(lo, hi, body):
        def step(j, carry):
            body(j)
            return carry
        lax.fori_loop(lo, hi, step, 0)

    for layer in range(1, NUM_LAYERS + 1):
        if layer == 1:
            send_far = functools.partial(layer1_step, to_far_chip=True)
            send_near = functools.partial(layer1_step, to_far_chip=False)
            layer1_first()
            loop(1, EARLY, send_far)
            remote(panel.at[0, far_block], panel.at[0, far_block], *head(0), to_far).wait()
            ag0_f.start()
            loop(EARLY, n_chunk, send_far)
            layer1_add(n_chunk - 1, True)
            loop(0, n_chunk, send_near)
            layer1_add(n_chunk - 1, False)
            for slot in range(CORE_SLOTS):
                core_copy(slot, 0).wait_send()
        else:
            loop(0, n_chunk, functools.partial(item_send_step, layer=layer))
            add_mate(n_chunk - 1, layer)
        if layer == 1:
            ag0_d.wait()
            ag0_f.wait()
            u0.wait_send()
        else:
            gather_items(layer - 1)
        finish = functools.partial(finish_item, layer=layer)
        if layer == 1:
            loop(0, n_chunk // 2, finish)
            user_part(layer)
            y_copy(layer).start()
            loop(n_chunk // 2, n_chunk, finish)
            loop(0, 4, place_rows)
            mark_mixed()
            finish_user(layer)
            u_copy(layer).wait()
        elif layer < NUM_LAYERS:
            user_part(layer)
            y_copy(layer).start()
            loop(0, n_chunk // 2, finish)
            finish_user(layer)
            loop(4, PIECES, place_rows)
            loop(n_chunk // 2, n_chunk, finish)
            u_copy(layer).wait()
        else:
            user_part(layer)
            y_copy(layer).start()

    for slot in range(CORE_SLOTS):
        core_copy(slot).wait_send()
    table[pl.ds(4 * own_i, 8), :] = jnp.zeros((8, 128), F32)
    stage[pl.ds(4 * own_u, 8), :] = jnp.zeros((8, 128), F32)

    def last_step(j):
        finish_item(j, NUM_LAYERS)

        @pl.when(j >= LAG)
        def _():
            fin_near(j - LAG)

        @pl.when(j >= LAG + 2)
        def _():
            fin_fwd(j - LAG - 2)

    loop(0, n_chunk // 2, last_step)
    finish_user(NUM_LAYERS)
    loop(n_chunk // 2, 3 * n_chunk // 4, last_step)
    gather_users()
    swap_users()
    loop(3 * n_chunk // 4, n_chunk, last_step)
    loop(n_chunk - LAG, n_chunk, fin_near)
    loop(n_chunk - LAG - 2, n_chunk, fin_fwd)
    for k in (1, 2):
        lo, hi = (k - 1) * share // 2, k * share // 2
        pick(table, 0, 1, yflat, lo, hi)
        pick(table, 0, 2, yflat, lo, hi)
        diff = yflat[share + lo:share + hi, :] - yflat[2 * share + lo:2 * share + hi, :]
        panel[0, out_rows(2 * share + lo, share // 2), :] = jnp.where(mixed[lo:hi, :] > 0.5, diff, 0.0).astype(BF16)
        pick_copy(k).start()
    pick(table, 1, 1, drecv)
    pick(table, 1, 2, drecv)

    def score(user, items_diff):
        return jnp.sum((user * items_diff).T, axis=0, keepdims=True)

    n_dev = len(peers) + 1
    base = (emb * (n_dev // 2) + row * 2 + col) * 2 * share
    pick_copy(0).wait_recv()
    e_far = yflat[thirds(0), :] + pick_in[thirds(1), :].astype(F32)
    diff = jnp.where(mixed[...] > 0.5, 0.0, yflat[thirds(1), :] - yflat[thirds(2), :])
    dots[:, pl.ds(pl.multiple_of(base + share, share), share)] = score(e_far, diff)
    e_own = drecv[thirds(0), :] + pick_in[thirds(0), :].astype(F32)
    diff = drecv[thirds(1), :] - drecv[thirds(2), :]
    pick_copy(1).wait_recv()
    pick_copy(2).wait_recv()
    diff = diff + pick_in[thirds(2), :].astype(F32)
    dots[:, pl.ds(pl.multiple_of(base, share), share)] = score(e_own, diff)
    mine = pl.ds(pl.multiple_of(base, 2 * share), 2 * share)
    for target in peers:
        remote(dots.at[:, mine], dots.at[:, mine], loss_s.at[0], loss_r.at[0], target).start()

    for k in range(3):
        pick_copy(k).wait_send()
    for k, kind in enumerate(("col", "mate", "fwd")):
        fu_copy(kind).wait_send()
        remote(panel.at[1, block], panel.at[1, block], fin_s.at[k], fin_r.at[0, 0], to_mate).wait_send()
    others = dots.at[:, pl.ds(0, len(peers) * 2 * share)]
    remote(others, others, loss_s.at[0], loss_r.at[0], to_far).wait()
    half = n_dev // 2
    def scores(e, owner, k):
        at = ((e * half + owner) * 2 + k) * share
        return dots[:, at:at + share]

    for g in range(half):
        z = -sum(scores(e, g, 0) + scores(e, (g + half // 2) % half, 1) for e in range(2))
        loss_ref[:, g * share:(g + 1) * share] = jnp.maximum(z, 0.0) + jnp.log1p(jnp.exp(-jnp.abs(z)))


def hand_out_kernel(u_in, i_in, l_in, u_out, i_out, l_out, out_s):
    pieces = [pltpu.make_async_copy(src, dst, out_s.at[k])
              for k, (src, dst) in enumerate(((i_in, i_out), (u_in, u_out), (l_in, l_out)))]
    for piece in pieces:
        piece.start()
    for piece in pieces:
        piece.wait()


def hand_out(*arrays):
    return pl.pallas_call(
        hand_out_kernel,
        name="hand_out",
        out_shape=tuple(jax.ShapeDtypeStruct(a.shape, a.dtype) for a in arrays),
        in_specs=[pl.BlockSpec(memory_space=pltpu.VMEM)] * 3,
        out_specs=(pl.BlockSpec(memory_space=pl.ANY),) * 3,
        scratch_shapes=[pltpu.SemaphoreType.DMA((6,))],
        compiler_params=pltpu.CompilerParams(vmem_limit_bytes=2 * 2 ** 20),
    )(*arrays)


def propagate(mask_blk, user_sh, item_sh, triples):
    users, items = mask_blk.shape
    own_u, dim = user_sh.shape
    own_i = item_sh.shape[0]
    n_chunk = own_i // CHUNK
    num_trip = triples.shape[0]
    share = num_trip // 8
    n_group = n_chunk // GROUP
    vmem, dma = pltpu.VMEM, pltpu.SemaphoreType.DMA
    one = dma((1,))
    return pl.pallas_call(
        prop_kernel,
        name="propagate",
        out_shape=(vmem((own_u, dim), BF16), vmem((own_i, dim), BF16), vmem((1, num_trip), F32)),
        in_specs=[pl.BlockSpec(memory_space=pl.ANY)] * 4,
        out_specs=(pl.BlockSpec(memory_space=pltpu.VMEM),) * 3,
        scratch_shapes=[
            vmem((users, items), BF16),
            vmem((MASK_SLOTS, users, CHUNK), jnp.int32),
            vmem((2, items, dim), BF16),
            vmem((4 * own_i + 8, dim), F32),
            vmem((CORE_SLOTS * 2 * CHUNK + 8, dim), F32),
            vmem((CORE_SLOTS * 2 * CHUNK, dim), F32),
            vmem((3, users, dim), BF16),
            vmem((users, dim), F32),
            vmem((3 * own_u, dim), F32),
            vmem((own_u, dim), BF16),
            vmem((own_i, dim), BF16),
            pltpu.SMEM((3, num_trip), jnp.int32),
            vmem((3, num_trip), jnp.int32),
            vmem((1, items), F32),
            vmem((1, items), F32),
            vmem((1, items), F32),
            vmem((1, items), F32),
            vmem((1, users), F32),
            vmem((1, users), F32),
            vmem((1, users), F32),
            pltpu.SMEM((6 * share,), jnp.int32),
            vmem((3 * share, dim), BF16),
            vmem((share, 128), F32),
            vmem((1, 4 * num_trip), F32),
            one, one,
            one, one,
            dma((CORE_SLOTS,)), dma((CORE_SLOTS,)),
            dma((n_group,)), dma((2, n_chunk)),
            one, dma((2, n_group)),
            one, dma((2, n_group)),
            one, dma((2, n_group)),
            dma((3,)), dma((3, n_chunk)),
            one, one,
        ],
        compiler_params=pltpu.CompilerParams(collective_id=0, has_side_effects=True,
                                             vmem_limit_bytes=65_700_000),
    )(mask_blk, user_sh, item_sh, triples.T)


def solution(mesh):
    def local_fn(mask_blk, user_sh, item_sh, triples):
        final_user, final_item, loss = hand_out(*propagate(mask_blk, user_sh, item_sh, triples))
        return final_user, final_item, loss.reshape(-1)

    return jax.shard_map(
        local_fn, mesh=mesh,
        in_specs=(P("row", "col"), P(("row", "col"), "emb"), P(("col", "row"), "emb"), P()),
        out_specs=(P(("row", "col"), "emb"), P(("col", "row"), "emb"), P()),
        check_vma=False)
```

```python
import functools

import jax
import jax.numpy as jnp
from jax import lax
from jax.experimental import pallas as pl
from jax.experimental.pallas import tpu as pltpu
from jax.sharding import PartitionSpec as P

NUM_LAYERS = 3
F32 = jnp.float32
BF16 = jnp.bfloat16
MESH = pl.DeviceIdType.MESH

CHUNK = 256
MASK_SLOTS = 7
GROUP = 4
EARLY = 8
PIECES = 16
CORE_SLOTS = 4
SCALE_ROWS = 256
LAG = 3
FOLD = 2048


def prop_kernel(mask_hbm, eu_hbm, ei_hbm, trip_hbm, outu_ref, outi_ref, loss_ref,
                adj, mbuf, panel, table, stage, drecv, upanel, upart, yflat, eu_ref, ei_ref, trip_ref, trip_vec,
                csum, ccore, cchip, cfar, rdeg, rdfar, rdemb, pick_idx, pick_in, mixed, dots,
                u_s, u_r, y_s, y_r,
                d_s, d_r, x_s, x_r, agx_s, agx_r, agd_s, agd_r, agf_s, agf_r,
                fin_s, fin_r, half_r, loss_s, loss_r):
    users, items = adj.shape
    rsum = rscale = upart
    own_u = eu_ref.shape[0]
    own_i = ei_ref.shape[0]
    n_chunk = own_i // CHUNK
    halves = [(k, CHUNK // 2) for k in (2 * n_chunk - 2, 2 * n_chunk - 1)]
    row = lax.axis_index("row")
    col = lax.axis_index("col")
    mate = row + 1 - 2 * (row % 2)
    far = (row + 2) % 4
    far_mate = (mate + 2) % 4
    other_col = 1 - col
    to_mate = {"row": mate}
    to_far = {"row": far}
    to_col = {"col": other_col}
    emb = lax.axis_index("emb")
    peers = [{"emb": (emb + de) % 2, "row": (row + dr) % 4, "col": (col + dc) % 2}
             for de in range(2) for dr in range(4) for dc in range(2)][1:]
    share = loss_ref.shape[1] // 8

    def remote(src, dst, ssem, rsem, target):
        return pltpu.make_async_remote_copy(src_ref=src, dst_ref=dst, send_sem=ssem, recv_sem=rsem,
                                            device_id=target, device_id_type=MESH)

    def rows_of(owner, j, size=CHUNK):
        return pl.ds(pl.multiple_of(owner * own_i + j * size, size), size)

    block = pl.ds(pl.multiple_of(row * own_i, own_i), own_i)
    far_block = pl.ds(pl.multiple_of(far * own_i, own_i), own_i)
    ublock = pl.ds(pl.multiple_of(col * own_u, own_u), own_u)
    oblock = pl.ds(pl.multiple_of(other_col * own_u, own_u), own_u)
    n_mask = items // CHUNK

    def mask_block(i):
        return (i + emb * (n_mask // 2)) % n_mask

    def mask_copy(i):
        slot = i % MASK_SLOTS
        b = mask_block(i)
        return pltpu.make_async_copy(mask_hbm.at[:, rows_of(b % 4, b // 4)], mbuf.at[slot], fin_r.at[0, slot])

    for i in range(MASK_SLOTS - 1):
        mask_copy(i).start()
    inputs = [pltpu.make_async_copy(src, dst, fin_r.at[0, 8 + k]) for k, (src, dst) in enumerate((
        (eu_hbm, upanel.at[0, ublock]), (ei_hbm, panel.at[0, block]), (eu_hbm, eu_ref), (ei_hbm, ei_ref),
        (trip_hbm, trip_ref), (trip_hbm, trip_vec)))]
    for copy in inputs:
        copy.start()

    barrier = pltpu.get_barrier_semaphore()
    neighbours = (to_mate, to_far, to_col, {"emb": 1 - emb})
    for target in neighbours:
        pl.semaphore_signal(barrier, inc=1, device_id=target, device_id_type=MESH)

    rsum[...] = jnp.zeros_like(rsum)

    def mask_step(i, carry, count):
        mask_copy(i).wait()

        @pl.when(i + MASK_SLOTS - 1 < n_mask)
        def _():
            mask_copy(i + MASK_SLOTS - 1).start()

        b = mask_block(i)
        cols = rows_of(b % 4, b // 4)
        slot = i % MASK_SLOTS

        def tile(t, acc):
            rows = pl.ds(pl.multiple_of(t * 64, 64), 64)
            m = mbuf[slot, rows, :].astype(F32)
            adj[rows, cols] = m.astype(BF16)
            if not count:
                return acc
            part = m[:, 0:128]
            for g in range(1, CHUNK // 128):
                part = part + m[:, g * 128:(g + 1) * 128]
            rsum[rows, :] += part
            return acc + jnp.sum(m.reshape(8, 8, CHUNK), axis=0)

        if count:
            acc = lax.fori_loop(0, users // 64, tile, jnp.zeros((8, CHUNK), F32))
            csum[:, pl.ds(pl.multiple_of(b * CHUNK, CHUNK), CHUNK)] = jnp.sum(acc, axis=0, keepdims=True)
        else:
            lax.fori_loop(0, users // 64, tile, 0)
        return carry

    def stream(lo, hi, count=False):
        lax.fori_loop(lo, hi, functools.partial(mask_step, count=count), 0)

    pl.semaphore_wait(barrier, len(neighbours))

    def head(k):
        return fin_r.at[1, k], fin_r.at[2, k]

    quarter = own_i // 4

    def ag0_x(k):
        return remote(ei_hbm.at[pl.ds(k * quarter, quarter)],
                      panel.at[0, pl.ds(pl.multiple_of(row * own_i + k * quarter, quarter), quarter)],
                      *head(0), to_far)

    ag0_d = remote(ei_hbm, panel.at[0, block], *head(1), to_mate)
    ag0_f = remote(panel.at[0, far_block], panel.at[0, far_block], *head(2), to_mate)
    for k in range(2):
        ag0_x(k).start()
    ag0_d.start()
    u0 = remote(eu_hbm, upanel.at[0, ublock], u_s.at[0], u_r.at[0], to_col)
    u0.start()

    half_cols = pl.ds(pl.multiple_of(emb * (items // 2), items // 2), items // 2)
    to_emb = {"emb": 1 - emb}
    ones = jnp.ones((8, 128), BF16)
    deg_z = remote(rdeg, rdemb, *head(3), to_emb)
    deg_y = remote(rdeg, rdfar, *head(4), to_col)
    deg_d = remote(csum.at[:, half_cols], ccore.at[:, half_cols], *head(5), to_mate)
    deg_x = remote(cchip.at[:, half_cols], cfar.at[:, half_cols], *head(6), to_far)
    deg_e = remote(csum.at[:, half_cols], csum.at[:, half_cols], *head(7), to_emb)
    mid = n_mask // 2

    stream(0, mid, count=True)
    rdeg[...] = lax.dot_general(ones, rsum[...].astype(BF16), (((1,), (1,)), ((), ())),
                                preferred_element_type=F32)[0:1, :]
    deg_z.start()
    deg_d.start()
    stream(mid, mid + 5)
    deg_z.wait()
    rdeg[...] += rdemb[...]
    deg_y.start()
    deg_d.wait()
    cchip[:, half_cols] = csum[:, half_cols] + ccore[:, half_cols]
    deg_x.start()
    ag0_x(2).start()
    ag0_x(3).start()
    stream(mid + 5, mid + 12)
    deg_y.wait()
    deg_u = jnp.maximum(rdeg[...] + rdfar[...], 1.0)
    rscale[...] = lax.rsqrt(jnp.broadcast_to(deg_u, (128, users)).T)
    stream(mid + 12, mid + 18)
    deg_x.wait()
    csum[:, half_cols] = cchip[:, half_cols] + cfar[:, half_cols]
    deg_e.start()
    stream(mid + 18, mid + 26)
    deg_e.wait()
    csum[...] = lax.rsqrt(jnp.maximum(csum[...], 1.0))
    stream(mid + 26, n_mask)
    for copy in inputs:
        copy.wait()
    u0.wait_recv()

    def scale_block(owner, j):
        ci = csum[:, pl.ds(pl.multiple_of((j * 4 + owner) * CHUNK, CHUNK), CHUNK)]

        def tile(t, carry):
            rows = pl.ds(pl.multiple_of(t * SCALE_ROWS, SCALE_ROWS), SCALE_ROWS)
            ru = rscale[rows, :]
            for g in range(CHUNK // 128):
                sub = pl.ds(pl.multiple_of(owner * own_i + j * CHUNK + g * 128, 128), 128)
                m = adj[rows, sub].astype(F32)
                adj[rows, sub] = ((ru * m) * ci[:, g * 128:(g + 1) * 128]).astype(BF16)
            return carry

        lax.fori_loop(0, users // SCALE_ROWS, tile, 0)

    def item_part(owner, j, layer):
        return lax.dot_general(adj[:, rows_of(owner, j)], upanel[layer - 1], (((0,), (0,)), ((), ())),
                               preferred_element_type=F32)

    def core_copy(slot, half=None):
        rows = slot_rows(slot, half)
        return remote(stage.at[rows], drecv.at[rows], d_s.at[slot], d_r.at[slot], to_mate)

    def region(k, j, size=CHUNK):
        return pl.ds(pl.multiple_of(k * own_i + j * size, size), size)

    def near(j, size=CHUNK):
        return region(0, j, size)

    def arrived(j, layer, size=CHUNK):
        return region(1 + layer % 2, j, size)

    def xsend(j, size=CHUNK):
        return region(3, j, size)

    def arrival(pool, row_at, j, size, k):
        if size == CHUNK:
            return pool.at[row_at, j]
        return half_r.at[k] if j % 2 else pool.at[row_at, j // 2]

    def slot_rows(slot, half=None):
        if half is None:
            return pl.ds(pl.multiple_of(slot * 2 * CHUNK, 2 * CHUNK), 2 * CHUNK)
        return pl.ds(pl.multiple_of(slot * 2 * CHUNK + half * CHUNK, CHUNK), CHUNK)

    def x_copy(j, layer, size=CHUNK):
        return remote(table.at[xsend(j, size)], table.at[arrived(j, layer, size)],
                      x_s.at[j * size // (GROUP * CHUNK)], arrival(x_r, layer % 2, j, size, 3), to_far)

    def x_sent(g):
        rows = pl.ds(pl.multiple_of(3 * own_i + g * GROUP * CHUNK, GROUP * CHUNK), GROUP * CHUNK)
        remote(table.at[rows], table.at[rows], x_s.at[g], x_r.at[0, 0], to_far).wait_send()

    def item_send_step(j, layer):
        slot = j % CORE_SLOTS
        if layer == 2:
            pl.when(j >= CORE_SLOTS)(core_copy(slot).wait_send)
        else:
            core_copy(slot).wait_send()

        @pl.when(j % GROUP == 0)
        def _():
            x_sent(j // GROUP)

        stage[slot_rows(slot, 0), :] = item_part(far_mate, j, layer)
        stage[slot_rows(slot, 1), :] = item_part(mate, j, layer)
        core_copy(slot).start()
        table[xsend(j), :] = item_part(far, j, layer)
        table[near(j), :] = item_part(row, j, layer)

        @pl.when(j == 0)
        def _():
            add_mate(0, layer)

        @pl.when(j >= 2)
        def _():
            add_mate(j - 1, layer)

    def add_mate(j, layer, parts=None):
        parts = parts or [(j, CHUNK)]
        slot = j % CORE_SLOTS
        core_copy(slot).wait_recv()
        table[xsend(j), :] += drecv[slot_rows(slot, 0), :]
        table[near(j), :] += drecv[slot_rows(slot, 1), :]
        for part, size in parts:
            x_copy(part, layer, size).start()

    def layer1_step(j, to_far_chip):
        slot = j % CORE_SLOTS
        theirs, ours, here = (far_mate, far, xsend) if to_far_chip else (mate, row, near)
        if to_far_chip:
            pl.when(j >= CORE_SLOTS)(core_copy(slot, 0).wait_send)
        else:
            core_copy(slot, 0).wait_send()
        scale_block(theirs, j)
        scale_block(ours, j)
        stage[slot_rows(slot, 0), :] = item_part(theirs, j, 1)
        table[here(j), :] = item_part(ours, j, 1)
        core_copy(slot, 0).start()
        if not to_far_chip:
            @pl.when(j == 0)
            def _():
                layer1_add(0, to_far_chip)

        @pl.when(j >= 2)
        def _():
            layer1_add(j - 1, to_far_chip)

    def layer1_first():
        scale_block(far_mate, 0)
        stage[slot_rows(0, 0), :] = item_part(far_mate, 0, 1)
        core_copy(0, 0).start()
        scale_block(far, 0)
        table[xsend(0), :] = item_part(far, 0, 1)
        layer1_add(0, True)

    def layer1_add(j, to_far_chip):
        slot = j % CORE_SLOTS
        here = xsend if to_far_chip else near
        core_copy(slot, 0).wait_recv()
        table[here(j), :] += drecv[slot_rows(slot, 0), :]
        if to_far_chip:
            x_copy(j, 1).start()

    def ag_copy(kind, g, layer, whole=False):
        par = layer % 2
        rows = rows_of(far if kind == "fwd" else row, 0 if whole else g, own_i if whole else GROUP * CHUNK)
        piece = panel.at[par, rows]
        ssem, rsem, target = {"x": (agx_s, agx_r, to_far), "mate": (agd_s, agd_r, to_mate),
                              "fwd": (agf_s, agf_r, to_mate)}[kind]
        return remote(piece, piece, ssem.at[0], rsem.at[par, g], target)

    def fin_copy(kind, j, size=CHUNK):
        mine, other = panel.at[1, rows_of(row, j, size)], panel.at[1, rows_of(far, j, size)]
        src, dst, k, target = {"col": (mine, other, 0, to_col), "mate": (mine, mine, 1, to_mate),
                               "fwd": (other, other, 2, to_mate)}[kind]
        return remote(src, dst, fin_s.at[k], arrival(fin_r, k, j, size, k), target)

    def fin_near(j, size=CHUNK):
        fin_copy("col", j, size).wait_recv()
        fin_copy("fwd", j, size).start()
        table[region(2, j, size), :] = panel[1, rows_of(far, j, size), :].astype(F32)
        fin_copy("mate", j, size).wait_recv()
        table[region(1, j, size), :] = panel[1, rows_of(mate, j, size), :].astype(F32)

    def fin_fwd(j, size=CHUNK):
        if size == CHUNK:
            @pl.when(j % GROUP == 0)
            def _():
                x_sent(j // GROUP)

        fin_copy("fwd", j, size).wait_recv()
        table[region(3, j, size), :] = panel[1, rows_of(far_mate, j, size), :].astype(F32)

    def finish_item(j, layer, size=CHUNK):
        x_copy(j, layer, size).wait_recv()
        par = layer % 2
        mine = rows_of(row, j, size)
        here = rows_of(0, j, size)
        value = (table[near(j, size), :] + table[arrived(j, layer, size), :]).astype(BF16)
        if layer < NUM_LAYERS:
            panel[par, mine, :] = value

            @pl.when(j % GROUP == GROUP - 1)
            def _():
                ag_copy("x", j // GROUP, layer).start()
                ag_copy("mate", j // GROUP, layer).start()
        else:
            total = ei_ref[here, :].astype(F32) + panel[1, mine, :].astype(F32)
            total = total + panel[0, mine, :].astype(F32)
            total = total + value.astype(F32)
            final = (total / (NUM_LAYERS + 1)).astype(BF16)
            panel[1, mine, :] = final
            outi_ref[here, :] = final
            table[near(j, size), :] = final.astype(F32)
            fin_copy("col", j, size).start()
            fin_copy("mate", j, size).start()

    def gather_items(layer):
        for g in range(n_chunk // GROUP):
            ag_copy("x", g, layer).wait_recv()
            ag_copy("fwd", g, layer).start()
        for g in range(n_chunk // GROUP):
            ag_copy("mate", g, layer).wait_recv()
            ag_copy("fwd", g, layer).wait_recv()
        for kind in ("x", "mate", "fwd"):
            ag_copy(kind, 0, layer, whole=True).wait_send()

    def user_part(layer):
        par = (layer - 1) % 2
        upart[...] = jnp.zeros_like(upart)

        def fold(i, carry):
            cols = pl.ds(pl.multiple_of(i * FOLD, FOLD), FOLD)
            upart[...] += jnp.dot(adj[:, cols], panel[par, cols, :], preferred_element_type=F32)
            return carry

        lax.fori_loop(0, items // FOLD, fold, 0)

    def yrows(layer):
        return pl.ds((layer - 1) * own_u, own_u)

    def y_copy(layer):
        return remote(upart.at[oblock], yflat.at[yrows(layer)], y_s.at[0], y_r.at[0], to_col)

    def u_copy(layer):
        return remote(upanel.at[layer, ublock], upanel.at[layer, ublock], u_s.at[0], u_r.at[0], to_col)

    def finish_user(layer):
        y_copy(layer).wait()
        value = (upart[ublock, :] + yflat[yrows(layer), :]).astype(BF16)
        if layer < NUM_LAYERS:
            upanel[layer, ublock, :] = value
            u_copy(layer).start()
        else:
            total = eu_ref[...].astype(F32) + upanel[1, ublock, :].astype(F32)
            total = total + upanel[2, ublock, :].astype(F32)
            total = total + value.astype(F32)
            final = (total / (NUM_LAYERS + 1)).astype(BF16)
            eu_ref[...] = final
            outu_ref[...] = final
            stage[0:own_u, :] = final.astype(F32)
            fu_copy("col").start()
            fu_copy("mate").start()

    def fu_copy(kind):
        src, dst, k, target = {
            "col": (eu_ref, upanel.at[0, pl.ds(0, own_u)], 0, to_col),
            "mate": (eu_ref, upanel.at[0, pl.ds(own_u, own_u)], 1, to_mate),
            "fwd": (upanel.at[0, pl.ds(0, own_u)], upanel.at[1, oblock], 2, to_mate)}[kind]
        return remote(src, dst, agd_r.at[0, k], agd_r.at[1, k], target)

    def gather_users():
        fu_copy("col").wait_recv()
        fu_copy("fwd").start()
        stage[2 * own_u:3 * own_u, :] = upanel[0, 0:own_u, :].astype(F32)
        fu_copy("mate").wait_recv()
        stage[own_u:2 * own_u, :] = upanel[0, own_u:2 * own_u, :].astype(F32)
        fu_copy("fwd").wait_recv()
        stage[3 * own_u:4 * own_u, :] = upanel[1, oblock, :].astype(F32)

    def place_rows(piece):
        def side(r):
            return r // 2

        def step(t, carry):
            for k, owner in ((0, far), (1, row)):
                base = (owner * 2 + col) * share + t
                user = trip_ref[0, base]
                ur = lax.shift_right_logical(user, 10)
                uc = lax.bitwise_and(lax.shift_right_logical(user, 9), 1)
                pos = (jnp.where(uc == col, 0, 2) + jnp.where(ur == row, 0, 1)) * own_u + lax.bitwise_and(user, 511)
                pick_idx[k * 3 * share + t] = jnp.where(lax.shift_right_logical(ur, 1) == side(row), pos, 4 * own_u)
                for which in (1, 2):
                    item = trip_ref[which, base]
                    ic = lax.shift_right_logical(item, 14)
                    ir = lax.bitwise_and(lax.shift_right_logical(item, 12), 3)
                    pos = (jnp.where(ic == col, 0, 2) + jnp.where(ir == row, 0, 1)) * own_i + lax.bitwise_and(item, 4095)
                    pick_idx[(k * 3 + which) * share + t] = jnp.where(
                        lax.shift_right_logical(ir, 1) == side(row), pos, 4 * own_i)
            return carry

        lax.fori_loop(piece * (share // PIECES), (piece + 1) * (share // PIECES), step, 0)

    def pick(src, k, which, dst, lo=0, hi=None):
        def step(t, carry):
            for i in range(8):
                at = t * 8 + i
                dst[pl.ds(which * share + at, 1), :] = src[pl.ds(pick_idx[(k * 3 + which) * share + at], 1), :]
            return carry

        lax.fori_loop(lo // 8, (hi or share) // 8, step, 0)

    def out_rows(lo, size):
        return pl.ds(pl.multiple_of(far * own_i + lo, size), size)

    def pick_copy(k):
        lo, size = ((0, 2 * share), (2 * share, share // 2), (5 * share // 2, share // 2))[k]
        return remote(panel.at[0, out_rows(lo, size)], pick_in.at[pl.ds(lo, size)],
                      agx_r.at[0, k], agx_r.at[1, k], to_far)

    def thirds(k):
        return pl.ds(k * share, share)

    def swap_users():
        pick(stage, 0, 0, yflat)
        pick(stage, 1, 0, drecv)
        panel[0, out_rows(0, share), :] = yflat[thirds(0), :].astype(BF16)
        panel[0, out_rows(share, share), :] = drecv[thirds(0), :].astype(BF16)
        pick_copy(0).start()

    def mark_mixed():
        ids = trip_vec[1:3, pl.ds(pl.multiple_of((far * 2 + col) * share, share), share)]
        sides = lax.bitwise_and(lax.shift_right_logical(ids, 13), 1)
        flag = jnp.where(sides[0:1] == sides[1:2], 0.0, 1.0)
        mixed[...] = jnp.broadcast_to(flag, (128, share)).T

    def loop(lo, hi, body):
        def step(j, carry):
            body(j)
            return carry
        lax.fori_loop(lo, hi, step, 0)

    for layer in range(1, NUM_LAYERS + 1):
        if layer == 1:
            send_far = functools.partial(layer1_step, to_far_chip=True)
            send_near = functools.partial(layer1_step, to_far_chip=False)
            layer1_first()
            loop(1, EARLY, send_far)
            remote(panel.at[0, far_block], panel.at[0, far_block], *head(0), to_far).wait()
            ag0_f.start()
            loop(EARLY, n_chunk, send_far)
            layer1_add(n_chunk - 1, True)
            loop(0, n_chunk, send_near)
            layer1_add(n_chunk - 1, False)
            for slot in range(CORE_SLOTS):
                core_copy(slot, 0).wait_send()
        else:
            loop(0, n_chunk, functools.partial(item_send_step, layer=layer))
            add_mate(n_chunk - 1, layer, halves if layer == NUM_LAYERS else None)
        if layer == 1:
            ag0_d.wait()
            ag0_f.wait()
            u0.wait_send()
        else:
            gather_items(layer - 1)
        finish = functools.partial(finish_item, layer=layer)
        if layer == 1:
            loop(0, n_chunk // 2, finish)
            user_part(layer)
            y_copy(layer).start()
            loop(n_chunk // 2, n_chunk, finish)
            loop(0, 4, place_rows)
            mark_mixed()
            finish_user(layer)
            u_copy(layer).wait()
        elif layer < NUM_LAYERS:
            user_part(layer)
            y_copy(layer).start()
            loop(0, n_chunk // 2, finish)
            finish_user(layer)
            loop(4, PIECES, place_rows)
            loop(n_chunk // 2, n_chunk, finish)
            u_copy(layer).wait()
        else:
            user_part(layer)
            y_copy(layer).start()

    for slot in range(CORE_SLOTS):
        core_copy(slot).wait_send()
    table[pl.ds(4 * own_i, 8), :] = jnp.zeros((8, 128), F32)
    stage[pl.ds(4 * own_u, 8), :] = jnp.zeros((8, 128), F32)

    def last_step(j):
        finish_item(j, NUM_LAYERS)

        @pl.when(j >= LAG)
        def _():
            fin_near(j - LAG)

        @pl.when(j >= LAG + 2)
        def _():
            fin_fwd(j - LAG - 2)

    loop(0, n_chunk // 2, last_step)
    finish_user(NUM_LAYERS)
    loop(n_chunk // 2, 3 * n_chunk // 4, last_step)
    gather_users()
    swap_users()
    last = n_chunk - 1
    loop(3 * n_chunk // 4, last, last_step)
    for j, size in halves:
        finish_item(j, NUM_LAYERS, size)
    loop(last - LAG, last, fin_near)
    for j, size in halves:
        fin_near(j, size)
    loop(last - LAG - 2, last, fin_fwd)
    for j, size in halves:
        fin_fwd(j, size)
    for k in (1, 2):
        lo, hi = (k - 1) * share // 2, k * share // 2
        pick(table, 0, 1, yflat, lo, hi)
        pick(table, 0, 2, yflat, lo, hi)
        diff = yflat[share + lo:share + hi, :] - yflat[2 * share + lo:2 * share + hi, :]
        panel[0, out_rows(2 * share + lo, share // 2), :] = jnp.where(mixed[lo:hi, :] > 0.5, diff, 0.0).astype(BF16)
        pick_copy(k).start()
    pick(table, 1, 1, drecv)
    pick(table, 1, 2, drecv)

    def score(user, items_diff):
        return jnp.sum((user * items_diff).T, axis=0, keepdims=True)

    n_dev = len(peers) + 1
    base = (emb * (n_dev // 2) + row * 2 + col) * 2 * share
    pick_copy(0).wait_recv()
    e_far = yflat[thirds(0), :] + pick_in[thirds(1), :].astype(F32)
    diff = jnp.where(mixed[...] > 0.5, 0.0, yflat[thirds(1), :] - yflat[thirds(2), :])
    dots[:, pl.ds(pl.multiple_of(base + share, share), share)] = score(e_far, diff)
    e_own = drecv[thirds(0), :] + pick_in[thirds(0), :].astype(F32)
    diff = drecv[thirds(1), :] - drecv[thirds(2), :]
    pick_copy(1).wait_recv()
    pick_copy(2).wait_recv()
    diff = diff + pick_in[thirds(2), :].astype(F32)
    dots[:, pl.ds(pl.multiple_of(base, share), share)] = score(e_own, diff)
    mine = pl.ds(pl.multiple_of(base, 2 * share), 2 * share)
    for target in peers:
        remote(dots.at[:, mine], dots.at[:, mine], loss_s.at[0], loss_r.at[0], target).start()

    for k in range(3):
        pick_copy(k).wait_send()
    for k, kind in enumerate(("col", "mate", "fwd")):
        fu_copy(kind).wait_send()
        remote(panel.at[1, block], panel.at[1, block], fin_s.at[k], fin_r.at[0, 0], to_mate).wait_send()
    others = dots.at[:, pl.ds(0, len(peers) * 2 * share)]
    remote(others, others, loss_s.at[0], loss_r.at[0], to_far).wait()
    half = n_dev // 2
    def scores(e, owner, k):
        at = ((e * half + owner) * 2 + k) * share
        return dots[:, at:at + share]

    for g in range(half):
        z = -sum(scores(e, g, 0) + scores(e, (g + half // 2) % half, 1) for e in range(2))
        loss_ref[:, g * share:(g + 1) * share] = jnp.maximum(z, 0.0) + jnp.log1p(jnp.exp(-jnp.abs(z)))


def hand_out_kernel(u_in, i_in, l_in, u_out, i_out, l_out, out_s):
    pieces = [pltpu.make_async_copy(src, dst, out_s.at[k])
              for k, (src, dst) in enumerate(((i_in, i_out), (u_in, u_out), (l_in, l_out)))]
    for piece in pieces:
        piece.start()
    for piece in pieces:
        piece.wait()


def hand_out(*arrays):
    return pl.pallas_call(
        hand_out_kernel,
        name="hand_out",
        out_shape=tuple(jax.ShapeDtypeStruct(a.shape, a.dtype) for a in arrays),
        in_specs=[pl.BlockSpec(memory_space=pltpu.VMEM)] * 3,
        out_specs=(pl.BlockSpec(memory_space=pl.ANY),) * 3,
        scratch_shapes=[pltpu.SemaphoreType.DMA((6,))],
        compiler_params=pltpu.CompilerParams(vmem_limit_bytes=2 * 2 ** 20),
    )(*arrays)


def propagate(mask_blk, user_sh, item_sh, triples):
    users, items = mask_blk.shape
    own_u, dim = user_sh.shape
    own_i = item_sh.shape[0]
    n_chunk = own_i // CHUNK
    num_trip = triples.shape[0]
    share = num_trip // 8
    n_group = n_chunk // GROUP
    vmem, dma = pltpu.VMEM, pltpu.SemaphoreType.DMA
    one = dma((1,))
    return pl.pallas_call(
        prop_kernel,
        name="propagate",
        out_shape=(vmem((own_u, dim), BF16), vmem((own_i, dim), BF16), vmem((1, num_trip), F32)),
        in_specs=[pl.BlockSpec(memory_space=pl.ANY)] * 4,
        out_specs=(pl.BlockSpec(memory_space=pltpu.VMEM),) * 3,
        scratch_shapes=[
            vmem((users, items), BF16),
            vmem((MASK_SLOTS, users, CHUNK), jnp.int32),
            vmem((2, items, dim), BF16),
            vmem((4 * own_i + 8, dim), F32),
            vmem((CORE_SLOTS * 2 * CHUNK + 8, dim), F32),
            vmem((CORE_SLOTS * 2 * CHUNK, dim), F32),
            vmem((3, users, dim), BF16),
            vmem((users, dim), F32),
            vmem((3 * own_u, dim), F32),
            vmem((own_u, dim), BF16),
            vmem((own_i, dim), BF16),
            pltpu.SMEM((3, num_trip), jnp.int32),
            vmem((3, num_trip), jnp.int32),
            vmem((1, items), F32),
            vmem((1, items), F32),
            vmem((1, items), F32),
            vmem((1, items), F32),
            vmem((1, users), F32),
            vmem((1, users), F32),
            vmem((1, users), F32),
            pltpu.SMEM((6 * share,), jnp.int32),
            vmem((3 * share, dim), BF16),
            vmem((share, 128), F32),
            vmem((1, 4 * num_trip), F32),
            one, one,
            one, one,
            dma((CORE_SLOTS,)), dma((CORE_SLOTS,)),
            dma((n_group,)), dma((2, n_chunk)),
            one, dma((2, n_group)),
            one, dma((2, n_group)),
            one, dma((2, n_group)),
            dma((3,)), dma((3, n_chunk)), dma((4,)),
            one, one,
        ],
        compiler_params=pltpu.CompilerParams(collective_id=0, has_side_effects=True,
                                             vmem_limit_bytes=65_700_000),
    )(mask_blk, user_sh, item_sh, triples.T)


def solution(mesh):
    def local_fn(mask_blk, user_sh, item_sh, triples):
        final_user, final_item, loss = hand_out(*propagate(mask_blk, user_sh, item_sh, triples))
        return final_user, final_item, loss.reshape(-1)

    return jax.shard_map(
        local_fn, mesh=mesh,
        in_specs=(P("row", "col"), P(("row", "col"), "emb"), P(("col", "row"), "emb"), P()),
        out_specs=(P(("row", "col"), "emb"), P(("col", "row"), "emb"), P()),
        check_vma=False)
```

```python
import functools

import jax
import jax.numpy as jnp
from jax import lax
from jax.experimental import pallas as pl
from jax.experimental.pallas import tpu as pltpu
from jax.sharding import PartitionSpec as P

NUM_LAYERS = 3
F32 = jnp.float32
BF16 = jnp.bfloat16
MESH = pl.DeviceIdType.MESH

CHUNK = 256
MASK_SLOTS = 7
GROUP = 4
EARLY = 8
PIECES = 16
CORE_SLOTS = 4
SCALE_ROWS = 256
LAG = 3
FOLD = 2048


def prop_kernel(mask_hbm, eu_hbm, ei_hbm, trip_hbm, outu_ref, outi_ref, loss_ref,
                adj, mbuf, panel, table, stage, drecv, upanel, upart, yflat, eu_ref, ei_ref, trip_ref, trip_vec,
                csum, ccore, cchip, cfar, rdeg, rdfar, rdemb, pick_idx, pick_in, mixed, dots,
                u_s, u_r, y_s, y_r,
                d_s, d_r, x_s, x_r, agx_s, agx_r, agd_s, agd_r, agf_s, agf_r,
                fin_s, fin_r, half_r, loss_s, loss_r):
    users, items = adj.shape
    rsum = rscale = upart
    own_u = eu_ref.shape[0]
    own_i = ei_ref.shape[0]
    n_chunk = own_i // CHUNK
    halves = [(k, CHUNK // 2) for k in (2 * n_chunk - 2, 2 * n_chunk - 1)]
    row = lax.axis_index("row")
    col = lax.axis_index("col")
    mate = row + 1 - 2 * (row % 2)
    far = (row + 2) % 4
    far_mate = (mate + 2) % 4
    other_col = 1 - col
    to_mate = {"row": mate}
    to_far = {"row": far}
    to_col = {"col": other_col}
    emb = lax.axis_index("emb")
    peers = [{"emb": (emb + de) % 2, "row": (row + dr) % 4, "col": (col + dc) % 2}
             for de in range(2) for dr in range(4) for dc in range(2)][1:]
    share = loss_ref.shape[1] // 8

    def remote(src, dst, ssem, rsem, target):
        return pltpu.make_async_remote_copy(src_ref=src, dst_ref=dst, send_sem=ssem, recv_sem=rsem,
                                            device_id=target, device_id_type=MESH)

    def rows_of(owner, j, size=CHUNK):
        return pl.ds(pl.multiple_of(owner * own_i + j * size, size), size)

    block = pl.ds(pl.multiple_of(row * own_i, own_i), own_i)
    far_block = pl.ds(pl.multiple_of(far * own_i, own_i), own_i)
    ublock = pl.ds(pl.multiple_of(col * own_u, own_u), own_u)
    oblock = pl.ds(pl.multiple_of(other_col * own_u, own_u), own_u)
    n_mask = items // CHUNK

    def mask_block(i):
        return (i + emb * (n_mask // 2)) % n_mask

    def mask_copy(i):
        slot = i % MASK_SLOTS
        b = mask_block(i)
        return pltpu.make_async_copy(mask_hbm.at[:, rows_of(b % 4, b // 4)], mbuf.at[slot], fin_r.at[0, slot])

    for i in range(MASK_SLOTS - 1):
        mask_copy(i).start()
    inputs = [pltpu.make_async_copy(src, dst, fin_r.at[0, 8 + k]) for k, (src, dst) in enumerate((
        (eu_hbm, upanel.at[0, ublock]), (ei_hbm, panel.at[0, block]), (eu_hbm, eu_ref), (ei_hbm, ei_ref),
        (trip_hbm, trip_ref), (trip_hbm, trip_vec)))]
    for copy in inputs:
        copy.start()

    barrier = pltpu.get_barrier_semaphore()
    neighbours = (to_mate, to_far, to_col, {"emb": 1 - emb})
    for target in neighbours:
        pl.semaphore_signal(barrier, inc=1, device_id=target, device_id_type=MESH)

    rsum[...] = jnp.zeros_like(rsum)

    def mask_step(i, carry, count):
        mask_copy(i).wait()

        @pl.when(i + MASK_SLOTS - 1 < n_mask)
        def _():
            mask_copy(i + MASK_SLOTS - 1).start()

        b = mask_block(i)
        cols = rows_of(b % 4, b // 4)
        slot = i % MASK_SLOTS

        def tile(t, acc):
            rows = pl.ds(pl.multiple_of(t * 64, 64), 64)
            m = mbuf[slot, rows, :].astype(F32)
            adj[rows, cols] = m.astype(BF16)
            if not count:
                return acc
            part = m[:, 0:128]
            for g in range(1, CHUNK // 128):
                part = part + m[:, g * 128:(g + 1) * 128]
            rsum[rows, :] += part
            return acc + jnp.sum(m.reshape(8, 8, CHUNK), axis=0)

        if count:
            acc = lax.fori_loop(0, users // 64, tile, jnp.zeros((8, CHUNK), F32))
            csum[:, pl.ds(pl.multiple_of(b * CHUNK, CHUNK), CHUNK)] = jnp.sum(acc, axis=0, keepdims=True)
        else:
            lax.fori_loop(0, users // 64, tile, 0)
        return carry

    def stream(lo, hi, count=False):
        lax.fori_loop(lo, hi, functools.partial(mask_step, count=count), 0)

    pl.semaphore_wait(barrier, len(neighbours))

    def head(k):
        return fin_r.at[1, k], fin_r.at[2, k]

    quarter = own_i // 4

    def ag0_x(k):
        return remote(ei_hbm.at[pl.ds(k * quarter, quarter)],
                      panel.at[0, pl.ds(pl.multiple_of(row * own_i + k * quarter, quarter), quarter)],
                      *head(0), to_far)

    ag0_d = remote(ei_hbm, panel.at[0, block], *head(1), to_mate)
    ag0_f = remote(panel.at[0, far_block], panel.at[0, far_block], *head(2), to_mate)
    for k in range(2):
        ag0_x(k).start()
    ag0_d.start()
    u0 = remote(eu_hbm, upanel.at[0, ublock], u_s.at[0], u_r.at[0], to_col)
    u0.start()

    half_cols = pl.ds(pl.multiple_of(emb * (items // 2), items // 2), items // 2)
    to_emb = {"emb": 1 - emb}
    ones = jnp.ones((8, 128), BF16)
    deg_z = remote(rdeg, rdemb, *head(3), to_emb)
    deg_y = remote(rdeg, rdfar, *head(4), to_col)
    deg_d = remote(csum.at[:, half_cols], ccore.at[:, half_cols], *head(5), to_mate)
    deg_x = remote(cchip.at[:, half_cols], cfar.at[:, half_cols], *head(6), to_far)
    deg_e = remote(csum.at[:, half_cols], csum.at[:, half_cols], *head(7), to_emb)
    mid = n_mask // 2

    stream(0, mid, count=True)
    rdeg[...] = lax.dot_general(ones, rsum[...].astype(BF16), (((1,), (1,)), ((), ())),
                                preferred_element_type=F32)[0:1, :]
    deg_z.start()
    deg_d.start()
    stream(mid, mid + 5)
    deg_z.wait()
    rdeg[...] += rdemb[...]
    deg_y.start()
    deg_d.wait()
    cchip[:, half_cols] = csum[:, half_cols] + ccore[:, half_cols]
    deg_x.start()
    ag0_x(2).start()
    ag0_x(3).start()
    stream(mid + 5, mid + 12)
    deg_y.wait()
    deg_u = jnp.maximum(rdeg[...] + rdfar[...], 1.0)
    rscale[...] = lax.rsqrt(jnp.broadcast_to(deg_u, (128, users)).T)
    stream(mid + 12, mid + 18)
    deg_x.wait()
    csum[:, half_cols] = cchip[:, half_cols] + cfar[:, half_cols]
    deg_e.start()
    stream(mid + 18, mid + 26)
    deg_e.wait()
    csum[...] = lax.rsqrt(jnp.maximum(csum[...], 1.0))
    stream(mid + 26, n_mask)
    for copy in inputs:
        copy.wait()
    u0.wait_recv()

    def scale_block(owner, j):
        ci = csum[:, pl.ds(pl.multiple_of((j * 4 + owner) * CHUNK, CHUNK), CHUNK)]

        def tile(t, carry):
            rows = pl.ds(pl.multiple_of(t * SCALE_ROWS, SCALE_ROWS), SCALE_ROWS)
            ru = rscale[rows, :]
            for g in range(CHUNK // 128):
                sub = pl.ds(pl.multiple_of(owner * own_i + j * CHUNK + g * 128, 128), 128)
                m = adj[rows, sub].astype(F32)
                adj[rows, sub] = ((ru * m) * ci[:, g * 128:(g + 1) * 128]).astype(BF16)
            return carry

        lax.fori_loop(0, users // SCALE_ROWS, tile, 0)

    def item_part(owner, j, layer):
        return lax.dot_general(adj[:, rows_of(owner, j)], upanel[layer - 1], (((0,), (0,)), ((), ())),
                               preferred_element_type=F32)

    def core_copy(slot, half=None):
        rows = slot_rows(slot, half)
        return remote(stage.at[rows], drecv.at[rows], d_s.at[slot], d_r.at[slot], to_mate)

    def region(k, j, size=CHUNK):
        return pl.ds(pl.multiple_of(k * own_i + j * size, size), size)

    def near(j, size=CHUNK):
        return region(0, j, size)

    def arrived(j, layer, size=CHUNK):
        return region(1 + layer % 2, j, size)

    def xsend(j, size=CHUNK):
        return region(3, j, size)

    def arrival(pool, row_at, j, size, k):
        if size == CHUNK:
            return pool.at[row_at, j]
        return half_r.at[k] if j % 2 else pool.at[row_at, j // 2]

    def slot_rows(slot, half=None):
        if half is None:
            return pl.ds(pl.multiple_of(slot * 2 * CHUNK, 2 * CHUNK), 2 * CHUNK)
        return pl.ds(pl.multiple_of(slot * 2 * CHUNK + half * CHUNK, CHUNK), CHUNK)

    def x_copy(j, layer, size=CHUNK):
        return remote(table.at[xsend(j, size)], table.at[arrived(j, layer, size)],
                      x_s.at[j * size // (GROUP * CHUNK)], arrival(x_r, layer % 2, j, size, 3), to_far)

    def x_sent(g):
        rows = pl.ds(pl.multiple_of(3 * own_i + g * GROUP * CHUNK, GROUP * CHUNK), GROUP * CHUNK)
        remote(table.at[rows], table.at[rows], x_s.at[g], x_r.at[0, 0], to_far).wait_send()

    def item_send_step(j, layer):
        slot = j % CORE_SLOTS
        if layer == 2:
            pl.when(j >= CORE_SLOTS)(core_copy(slot).wait_send)
        else:
            core_copy(slot).wait_send()

        @pl.when(j % GROUP == 0)
        def _():
            x_sent(j // GROUP)

        stage[slot_rows(slot, 0), :] = item_part(far_mate, j, layer)
        stage[slot_rows(slot, 1), :] = item_part(mate, j, layer)
        core_copy(slot).start()
        table[xsend(j), :] = item_part(far, j, layer)
        table[near(j), :] = item_part(row, j, layer)

        @pl.when(j == 0)
        def _():
            add_mate(0, layer)

        @pl.when(j >= 2)
        def _():
            add_mate(j - 1, layer)

    def add_mate(j, layer, parts=None):
        parts = parts or [(j, CHUNK)]
        slot = j % CORE_SLOTS
        core_copy(slot).wait_recv()
        table[xsend(j), :] += drecv[slot_rows(slot, 0), :]
        table[near(j), :] += drecv[slot_rows(slot, 1), :]
        for part, size in parts:
            x_copy(part, layer, size).start()

    def layer1_step(j, to_far_chip):
        slot = j % CORE_SLOTS
        theirs, ours, here = (far_mate, far, xsend) if to_far_chip else (mate, row, near)
        if to_far_chip:
            pl.when(j >= CORE_SLOTS)(core_copy(slot, 0).wait_send)
        else:
            core_copy(slot, 0).wait_send()
        scale_block(theirs, j)
        scale_block(ours, j)
        stage[slot_rows(slot, 0), :] = item_part(theirs, j, 1)
        table[here(j), :] = item_part(ours, j, 1)
        core_copy(slot, 0).start()
        if not to_far_chip:
            @pl.when(j == 0)
            def _():
                layer1_add(0, to_far_chip)

        @pl.when(j >= 2)
        def _():
            layer1_add(j - 1, to_far_chip)

    def layer1_first():
        scale_block(far_mate, 0)
        stage[slot_rows(0, 0), :] = item_part(far_mate, 0, 1)
        core_copy(0, 0).start()
        scale_block(far, 0)
        table[xsend(0), :] = item_part(far, 0, 1)
        layer1_add(0, True)

    def layer1_add(j, to_far_chip):
        slot = j % CORE_SLOTS
        here = xsend if to_far_chip else near
        core_copy(slot, 0).wait_recv()
        table[here(j), :] += drecv[slot_rows(slot, 0), :]
        if to_far_chip:
            x_copy(j, 1).start()

    def ag_copy(kind, g, layer, whole=False):
        par = layer % 2
        rows = rows_of(far if kind == "fwd" else row, 0 if whole else g, own_i if whole else GROUP * CHUNK)
        piece = panel.at[par, rows]
        ssem, rsem, target = {"x": (agx_s, agx_r, to_far), "mate": (agd_s, agd_r, to_mate),
                              "fwd": (agf_s, agf_r, to_mate)}[kind]
        return remote(piece, piece, ssem.at[0], rsem.at[par, g], target)

    def fin_copy(kind, j, size=CHUNK):
        mine, other = panel.at[1, rows_of(row, j, size)], panel.at[1, rows_of(far, j, size)]
        src, dst, k, target = {"col": (mine, other, 0, to_col), "mate": (mine, mine, 1, to_mate),
                               "fwd": (other, other, 2, to_mate)}[kind]
        return remote(src, dst, fin_s.at[k], arrival(fin_r, k, j, size, k), target)

    def fin_near(j, size=CHUNK):
        fin_copy("col", j, size).wait_recv()
        fin_copy("fwd", j, size).start()
        table[region(2, j, size), :] = panel[1, rows_of(far, j, size), :].astype(F32)
        fin_copy("mate", j, size).wait_recv()
        table[region(1, j, size), :] = panel[1, rows_of(mate, j, size), :].astype(F32)

    def fin_fwd(j, size=CHUNK):
        if size == CHUNK:
            @pl.when(j % GROUP == 0)
            def _():
                x_sent(j // GROUP)

        fin_copy("fwd", j, size).wait_recv()
        table[region(3, j, size), :] = panel[1, rows_of(far_mate, j, size), :].astype(F32)

    def finish_item(j, layer, size=CHUNK):
        x_copy(j, layer, size).wait_recv()
        par = layer % 2
        mine = rows_of(row, j, size)
        here = rows_of(0, j, size)
        value = (table[near(j, size), :] + table[arrived(j, layer, size), :]).astype(BF16)
        if layer < NUM_LAYERS:
            panel[par, mine, :] = value

            @pl.when(j % GROUP == GROUP - 1)
            def _():
                ag_copy("x", j // GROUP, layer).start()
                ag_copy("mate", j // GROUP, layer).start()
        else:
            total = ei_ref[here, :].astype(F32) + panel[1, mine, :].astype(F32)
            total = total + panel[0, mine, :].astype(F32)
            total = total + value.astype(F32)
            final = (total / (NUM_LAYERS + 1)).astype(BF16)
            panel[1, mine, :] = final
            outi_ref[here, :] = final
            table[near(j, size), :] = final.astype(F32)
            fin_copy("col", j, size).start()
            fin_copy("mate", j, size).start()

    def gather_items(layer):
        for g in range(n_chunk // GROUP):
            ag_copy("x", g, layer).wait_recv()
            ag_copy("fwd", g, layer).start()
        for g in range(n_chunk // GROUP):
            ag_copy("mate", g, layer).wait_recv()
            ag_copy("fwd", g, layer).wait_recv()
        for kind in ("x", "mate", "fwd"):
            ag_copy(kind, 0, layer, whole=True).wait_send()

    def user_part(layer):
        par = (layer - 1) % 2
        upart[...] = jnp.zeros_like(upart)

        def fold(i, carry):
            cols = pl.ds(pl.multiple_of(i * FOLD, FOLD), FOLD)
            upart[...] += jnp.dot(adj[:, cols], panel[par, cols, :], preferred_element_type=F32)
            return carry

        lax.fori_loop(0, items // FOLD, fold, 0)

    def yrows(layer):
        return pl.ds((layer - 1) * own_u, own_u)

    def y_copy(layer):
        return remote(upart.at[oblock], yflat.at[yrows(layer)], y_s.at[0], y_r.at[0], to_col)

    def u_copy(layer):
        return remote(upanel.at[layer, ublock], upanel.at[layer, ublock], u_s.at[0], u_r.at[0], to_col)

    def finish_user(layer):
        y_copy(layer).wait()
        value = (upart[ublock, :] + yflat[yrows(layer), :]).astype(BF16)
        if layer < NUM_LAYERS:
            upanel[layer, ublock, :] = value
            u_copy(layer).start()
        else:
            total = eu_ref[...].astype(F32) + upanel[1, ublock, :].astype(F32)
            total = total + upanel[2, ublock, :].astype(F32)
            total = total + value.astype(F32)
            final = (total / (NUM_LAYERS + 1)).astype(BF16)
            eu_ref[...] = final
            outu_ref[...] = final
            stage[0:own_u, :] = final.astype(F32)
            fu_copy("col").start()
            fu_copy("mate").start()

    def fu_copy(kind):
        src, dst, k, target = {
            "col": (eu_ref, upanel.at[0, pl.ds(0, own_u)], 0, to_col),
            "mate": (eu_ref, upanel.at[0, pl.ds(own_u, own_u)], 1, to_mate),
            "fwd": (upanel.at[0, pl.ds(0, own_u)], upanel.at[1, oblock], 2, to_mate)}[kind]
        return remote(src, dst, agd_r.at[0, k], agd_r.at[1, k], target)

    def gather_users():
        fu_copy("col").wait_recv()
        fu_copy("fwd").start()
        stage[2 * own_u:3 * own_u, :] = upanel[0, 0:own_u, :].astype(F32)
        fu_copy("mate").wait_recv()
        stage[own_u:2 * own_u, :] = upanel[0, own_u:2 * own_u, :].astype(F32)
        fu_copy("fwd").wait_recv()
        stage[3 * own_u:4 * own_u, :] = upanel[1, oblock, :].astype(F32)

    def place_rows(piece):
        def side(r):
            return r // 2

        def step(t, carry):
            for k, owner in ((0, far), (1, row)):
                base = (owner * 2 + col) * share + t
                user = trip_ref[0, base]
                ur = lax.shift_right_logical(user, 10)
                uc = lax.bitwise_and(lax.shift_right_logical(user, 9), 1)
                pos = (jnp.where(uc == col, 0, 2) + jnp.where(ur == row, 0, 1)) * own_u + lax.bitwise_and(user, 511)
                pick_idx[k * 3 * share + t] = jnp.where(lax.shift_right_logical(ur, 1) == side(row), pos, 4 * own_u)
                for which in (1, 2):
                    item = trip_ref[which, base]
                    ic = lax.shift_right_logical(item, 14)
                    ir = lax.bitwise_and(lax.shift_right_logical(item, 12), 3)
                    pos = (jnp.where(ic == col, 0, 2) + jnp.where(ir == row, 0, 1)) * own_i + lax.bitwise_and(item, 4095)
                    pick_idx[(k * 3 + which) * share + t] = jnp.where(
                        lax.shift_right_logical(ir, 1) == side(row), pos, 4 * own_i)
            return carry

        lax.fori_loop(piece * (share // PIECES), (piece + 1) * (share // PIECES), step, 0)

    def pick(src, k, which, dst, lo=0, hi=None):
        def step(t, carry):
            for i in range(8):
                at = t * 8 + i
                dst[pl.ds(which * share + at, 1), :] = src[pl.ds(pick_idx[(k * 3 + which) * share + at], 1), :]
            return carry

        lax.fori_loop(lo // 8, (hi or share) // 8, step, 0)

    def out_rows(lo, size):
        return pl.ds(pl.multiple_of(far * own_i + lo, size), size)

    piece = share // GROUP

    def pick_copy(k):
        lo, size = (2 * share + (k - 1) * piece, piece) if k else (0, 2 * share)
        pool, at = (agx_r, k - 1) if k else (agf_r, 0)
        return remote(panel.at[0, out_rows(lo, size)], pick_in.at[pl.ds(lo, size)],
                      pool.at[0, at], pool.at[1, at], to_far)

    def thirds(k):
        return pl.ds(k * share, share)

    def swap_users():
        pick(stage, 0, 0, yflat)
        pick(stage, 1, 0, drecv)
        panel[0, out_rows(0, share), :] = yflat[thirds(0), :].astype(BF16)
        panel[0, out_rows(share, share), :] = drecv[thirds(0), :].astype(BF16)
        pick_copy(0).start()

    def mark_mixed():
        ids = trip_vec[1:3, pl.ds(pl.multiple_of((far * 2 + col) * share, share), share)]
        sides = lax.bitwise_and(lax.shift_right_logical(ids, 13), 1)
        flag = jnp.where(sides[0:1] == sides[1:2], 0.0, 1.0)
        mixed[...] = jnp.broadcast_to(flag, (128, share)).T

    def loop(lo, hi, body):
        def step(j, carry):
            body(j)
            return carry
        lax.fori_loop(lo, hi, step, 0)

    for layer in range(1, NUM_LAYERS + 1):
        if layer == 1:
            send_far = functools.partial(layer1_step, to_far_chip=True)
            send_near = functools.partial(layer1_step, to_far_chip=False)
            layer1_first()
            loop(1, EARLY, send_far)
            remote(panel.at[0, far_block], panel.at[0, far_block], *head(0), to_far).wait()
            ag0_f.start()
            loop(EARLY, n_chunk, send_far)
            layer1_add(n_chunk - 1, True)
            loop(0, n_chunk, send_near)
            layer1_add(n_chunk - 1, False)
            for slot in range(CORE_SLOTS):
                core_copy(slot, 0).wait_send()
        else:
            loop(0, n_chunk, functools.partial(item_send_step, layer=layer))
            add_mate(n_chunk - 1, layer, halves if layer == NUM_LAYERS else None)
        if layer == 1:
            ag0_d.wait()
            ag0_f.wait()
            u0.wait_send()
        else:
            gather_items(layer - 1)
        finish = functools.partial(finish_item, layer=layer)
        if layer == 1:
            loop(0, n_chunk // 2, finish)
            user_part(layer)
            y_copy(layer).start()
            loop(n_chunk // 2, n_chunk, finish)
            loop(0, 4, place_rows)
            mark_mixed()
            finish_user(layer)
            u_copy(layer).wait()
        elif layer < NUM_LAYERS:
            user_part(layer)
            y_copy(layer).start()
            loop(0, n_chunk // 2, finish)
            finish_user(layer)
            loop(4, PIECES, place_rows)
            loop(n_chunk // 2, n_chunk, finish)
            u_copy(layer).wait()
        else:
            user_part(layer)
            y_copy(layer).start()

    for slot in range(CORE_SLOTS):
        core_copy(slot).wait_send()
    table[pl.ds(4 * own_i, 8), :] = jnp.zeros((8, 128), F32)
    stage[pl.ds(4 * own_u, 8), :] = jnp.zeros((8, 128), F32)

    def last_step(j):
        finish_item(j, NUM_LAYERS)

        @pl.when(j >= LAG)
        def _():
            fin_near(j - LAG)

        @pl.when(j >= LAG + 2)
        def _():
            fin_fwd(j - LAG - 2)

    loop(0, n_chunk // 2, last_step)
    finish_user(NUM_LAYERS)
    loop(n_chunk // 2, 3 * n_chunk // 4, last_step)
    gather_users()
    swap_users()
    last = n_chunk - 1
    loop(3 * n_chunk // 4, last, last_step)
    for j, size in halves:
        finish_item(j, NUM_LAYERS, size)
    loop(last - LAG, last, fin_near)
    for j, size in halves:
        fin_near(j, size)
    loop(last - LAG - 2, last, fin_fwd)
    for j, size in halves:
        fin_fwd(j, size)
    for k in range(1, GROUP + 1):
        lo, hi = (k - 1) * piece, k * piece
        pick(table, 0, 1, yflat, lo, hi)
        pick(table, 0, 2, yflat, lo, hi)
        diff = yflat[share + lo:share + hi, :] - yflat[2 * share + lo:2 * share + hi, :]
        panel[0, out_rows(2 * share + lo, piece), :] = jnp.where(mixed[lo:hi, :] > 0.5, diff, 0.0).astype(BF16)
        pick_copy(k).start()
    pick(table, 1, 1, drecv)
    pick(table, 1, 2, drecv)

    def score(user, items_diff):
        return jnp.sum((user * items_diff).T, axis=0, keepdims=True)

    n_dev = len(peers) + 1
    base = (emb * (n_dev // 2) + row * 2 + col) * 2 * share
    pick_copy(0).wait_recv()
    e_far = yflat[thirds(0), :] + pick_in[thirds(1), :].astype(F32)
    diff = jnp.where(mixed[...] > 0.5, 0.0, yflat[thirds(1), :] - yflat[thirds(2), :])
    dots[:, pl.ds(pl.multiple_of(base + share, share), share)] = score(e_far, diff)
    e_own = drecv[thirds(0), :] + pick_in[thirds(0), :].astype(F32)
    diff = drecv[thirds(1), :] - drecv[thirds(2), :]
    for k in range(1, GROUP + 1):
        pick_copy(k).wait_recv()
    diff = diff + pick_in[thirds(2), :].astype(F32)
    dots[:, pl.ds(pl.multiple_of(base, share), share)] = score(e_own, diff)
    mine = pl.ds(pl.multiple_of(base, 2 * share), 2 * share)
    for target in peers:
        remote(dots.at[:, mine], dots.at[:, mine], loss_s.at[0], loss_r.at[0], target).start()

    for k in range(GROUP + 1):
        pick_copy(k).wait_send()
    for k, kind in enumerate(("col", "mate", "fwd")):
        fu_copy(kind).wait_send()
        remote(panel.at[1, block], panel.at[1, block], fin_s.at[k], fin_r.at[0, 0], to_mate).wait_send()
    others = dots.at[:, pl.ds(0, len(peers) * 2 * share)]
    remote(others, others, loss_s.at[0], loss_r.at[0], to_far).wait()
    half = n_dev // 2
    def scores(e, owner, k):
        at = ((e * half + owner) * 2 + k) * share
        return dots[:, at:at + share]

    for g in range(half):
        z = -sum(scores(e, g, 0) + scores(e, (g + half // 2) % half, 1) for e in range(2))
        loss_ref[:, g * share:(g + 1) * share] = jnp.maximum(z, 0.0) + jnp.log1p(jnp.exp(-jnp.abs(z)))


def hand_out_kernel(u_in, i_in, l_in, u_out, i_out, l_out, out_s):
    pieces = [pltpu.make_async_copy(src, dst, out_s.at[k])
              for k, (src, dst) in enumerate(((i_in, i_out), (u_in, u_out), (l_in, l_out)))]
    for piece in pieces:
        piece.start()
    for piece in pieces:
        piece.wait()


def hand_out(*arrays):
    return pl.pallas_call(
        hand_out_kernel,
        name="hand_out",
        out_shape=tuple(jax.ShapeDtypeStruct(a.shape, a.dtype) for a in arrays),
        in_specs=[pl.BlockSpec(memory_space=pltpu.VMEM)] * 3,
        out_specs=(pl.BlockSpec(memory_space=pl.ANY),) * 3,
        scratch_shapes=[pltpu.SemaphoreType.DMA((6,))],
        compiler_params=pltpu.CompilerParams(vmem_limit_bytes=2 * 2 ** 20),
    )(*arrays)


def propagate(mask_blk, user_sh, item_sh, triples):
    users, items = mask_blk.shape
    own_u, dim = user_sh.shape
    own_i = item_sh.shape[0]
    n_chunk = own_i // CHUNK
    num_trip = triples.shape[0]
    share = num_trip // 8
    n_group = n_chunk // GROUP
    vmem, dma = pltpu.VMEM, pltpu.SemaphoreType.DMA
    one = dma((1,))
    return pl.pallas_call(
        prop_kernel,
        name="propagate",
        out_shape=(vmem((own_u, dim), BF16), vmem((own_i, dim), BF16), vmem((1, num_trip), F32)),
        in_specs=[pl.BlockSpec(memory_space=pl.ANY)] * 4,
        out_specs=(pl.BlockSpec(memory_space=pltpu.VMEM),) * 3,
        scratch_shapes=[
            vmem((users, items), BF16),
            vmem((MASK_SLOTS, users, CHUNK), jnp.int32),
            vmem((2, items, dim), BF16),
            vmem((4 * own_i + 8, dim), F32),
            vmem((CORE_SLOTS * 2 * CHUNK + 8, dim), F32),
            vmem((CORE_SLOTS * 2 * CHUNK, dim), F32),
            vmem((3, users, dim), BF16),
            vmem((users, dim), F32),
            vmem((3 * own_u, dim), F32),
            vmem((own_u, dim), BF16),
            vmem((own_i, dim), BF16),
            pltpu.SMEM((3, num_trip), jnp.int32),
            vmem((3, num_trip), jnp.int32),
            vmem((1, items), F32),
            vmem((1, items), F32),
            vmem((1, items), F32),
            vmem((1, items), F32),
            vmem((1, users), F32),
            vmem((1, users), F32),
            vmem((1, users), F32),
            pltpu.SMEM((6 * share,), jnp.int32),
            vmem((3 * share, dim), BF16),
            vmem((share, 128), F32),
            vmem((1, 4 * num_trip), F32),
            one, one,
            one, one,
            dma((CORE_SLOTS,)), dma((CORE_SLOTS,)),
            dma((n_group,)), dma((2, n_chunk)),
            one, dma((2, n_group)),
            one, dma((2, n_group)),
            one, dma((2, n_group)),
            dma((3,)), dma((3, n_chunk)), dma((4,)),
            one, one,
        ],
        compiler_params=pltpu.CompilerParams(collective_id=0, has_side_effects=True,
                                             vmem_limit_bytes=65_700_000),
    )(mask_blk, user_sh, item_sh, triples.T)


def solution(mesh):
    def local_fn(mask_blk, user_sh, item_sh, triples):
        final_user, final_item, loss = hand_out(*propagate(mask_blk, user_sh, item_sh, triples))
        return final_user, final_item, loss.reshape(-1)

    return jax.shard_map(
        local_fn, mesh=mesh,
        in_specs=(P("row", "col"), P(("row", "col"), "emb"), P(("col", "row"), "emb"), P()),
        out_specs=(P(("row", "col"), "emb"), P(("col", "row"), "emb"), P()),
        check_vma=False)
```
